32 devices in a mesh: seq: 2 (over y), dp: 16 (over z, x, core).
Axes of the slice: x: 2, y: 2, z: 4, core: 2. Of those that a mesh axis runs over, the one named last changes fastest.
Arguments:
- inputs: bfloat16 [32, 128, 2304], P('dp', 'seq'), may hold values from -6 to 6
- lengths: int32 [32], P('dp'), may hold values from 32 to 128, as said below
- query_weight: bfloat16 [2304, 2304], P(('seq', 'dp')), may hold values from -0.1875 to 0.1875
- key_weight: bfloat16 [2304, 2304], P(('seq', 'dp')), may hold values from -0.1875 to 0.1875
- value_weight: bfloat16 [2304, 2304], P(('seq', 'dp')), may hold values from -0.125 to 0.125
- out_weight: bfloat16 [2304, 2304], P(('seq', 'dp')), may hold values from -2 to 2
- gate_weight: bfloat16 [2304, 5760], P(('seq', 'dp')), may hold values from -0.125 to 0.125
- up_weight: bfloat16 [2304, 5760], P(('seq', 'dp')), may hold values from -0.125 to 0.125
- down_weight: bfloat16 [5760, 2304], P(('seq', 'dp')), may hold values from -0.3125 to 0.3125
- attn_gain: bfloat16 [2304], P(('seq', 'dp')), may hold values from 0.5 to 1.5
- ffn_gain: bfloat16 [2304], P(('seq', 'dp')), may hold values from 0.5 to 1.5
- cotangent: bfloat16 [32, 128, 2304], P('dp', 'seq'), may hold values from -6 to 6
Outputs:
- output: bfloat16 [32, 128, 2304], P('dp', 'seq')
- input_grad: bfloat16 [32, 128, 2304], P('dp', 'seq')
- query_grad: float32 [2304, 2304], P(('seq', 'dp'))
- key_grad: float32 [2304, 2304], P(('seq', 'dp'))
- value_grad: float32 [2304, 2304], P(('seq', 'dp'))
- out_grad: float32 [2304, 2304], P(('seq', 'dp'))
- gate_grad: float32 [2304, 5760], P(('seq', 'dp'))
- up_grad: float32 [2304, 5760], P(('seq', 'dp'))
- down_grad: float32 [5760, 2304], P(('seq', 'dp'))
- attn_gain_grad: float32 [2304], P(('seq', 'dp'))
- ffn_gain_grad: float32 [2304], P(('seq', 'dp'))
The draws below stay inside these ranges and needn't reach their ends.
Inputs may be any that keep to these rules, and one draw needn't show every extreme that they name: `lengths`: every sequence's valid tokens come first; one sequence has 128 valid tokens and one has 32.
All inputs are finite; a program needn't handle non-finite values.
Results may differ from the reference program's by a relative error of at most 0.015.
Values may be sent and summed in bfloat16 or wider, within the bound.
A program may use at most 576 MiB of HBM per device.

```python
import math
import jax
import jax.numpy as jnp
from jax import lax

D = 2304
HEADS = 36
HEAD_DIM = 64
FF = 5760
SEQ_LEN = 128
SEQS = 32


def draw_lengths(key, part):
    first_key, second_key, third_key = jax.random.split(key, 3)
    drawn = jax.random.randint(first_key, (SEQS,), SEQ_LEN // 4, SEQ_LEN + 1)
    full_slot = jax.random.randint(second_key, (), 0, SEQS)
    short_slot = (full_slot + 1 + jax.random.randint(third_key, (), 0, SEQS - 1)) % SEQS
    drawn = drawn.at[full_slot].set(SEQ_LEN)
    drawn = drawn.at[short_slot].set(SEQ_LEN // 4)
    return drawn.astype(jnp.int32)


def with_spikes(array, rng, source, target, blocks, factor):
    owner, partner = [(jnp.arange(array.shape[dim]) // (array.shape[dim] // blocks)).reshape([-1 if axis == dim else 1 for axis in range(array.ndim)]) for dim in (source, target)]
    chosen = jax.random.permutation(rng, blocks)[partner]
    strong = (owner == chosen) | (owner == (partner + blocks // 2) % blocks)
    return jnp.where(strong, factor * array, array)


def levels(own_key, dims, cuts, least, top_value):
    factor_of, own = 1.0, jax.random.fold_in(own_key, 6)
    for position, shards_of in cuts:
        draws = jnp.exp(jax.random.uniform(jax.random.fold_in(own, position), (shards_of,), jnp.float32, least / len(cuts), top_value / len(cuts)))
        factor_of = factor_of * jnp.repeat(draws, dims[position] // shards_of).reshape([-1 if axis == position else 1 for axis in range(len(dims))])
    return factor_of


def noise(rng, extent, scale, limit, shards=(), kind=jnp.bfloat16):
    entries = jax.random.normal(rng, extent, jnp.float32) * scale
    if len(shards) > 0:
        entries = levels(rng, extent, shards, -0.22, 0.18) * entries
    return jnp.clip(entries, min=-limit, max=limit).astype(kind)


def gaussian_with(own_key, extent, deviation, most, shards, heavy, kind=jnp.bfloat16):
    entries = deviation * jax.random.normal(own_key, extent, jnp.float32)
    if shards:
        entries = entries * levels(own_key, extent, shards, -0.22, 0.18)
    return jnp.clip(with_spikes(entries, jax.random.fold_in(own_key, 3), *heavy), -most, most).astype(kind)


def setup_inputs(seed: int = 0) -> dict:
    key_of = jax.random.split(jax.random.key(seed), 13)
    return {
        "inputs": noise(key_of[0], (SEQS, SEQ_LEN, D), 1.0, 6.0, ((0, 16), (1, 2))),
        "lengths": draw_lengths(jax.random.fold_in(key_of[12], 71), 0),
        "query_weight": noise(key_of[2], (D, D), (D // 2) ** -0.5, 0.1875, ((0, 32),)),
        "key_weight": noise(key_of[3], (D, D), (D // 2) ** -0.5, 0.1875, ((0, 32),)),
        "value_weight": noise(key_of[4], (D, D), D ** -0.5, 0.125, ((0, 32),)),
        "out_weight": noise(key_of[5], (D, D), (max(D // 256, 8)) ** -0.5, 2.0, ((0, 32),)),
        "gate_weight": noise(key_of[6], (D, FF), D ** -0.5, 0.125, ((0, 32),)),
        "up_weight": noise(key_of[7], (D, FF), D ** -0.5, 0.125, ((0, 32),)),
        "down_weight": noise(key_of[8], (FF, D), (FF // 16) ** -0.5, 0.3125, ((0, 32),)),
        "attn_gain": jnp.clip(1.0 + 0.1 * jax.random.normal(key_of[9], (D,), jnp.float32), 0.5, 1.5).astype(jnp.bfloat16),
        "ffn_gain": jnp.clip(1.0 + 0.1 * jax.random.normal(key_of[10], (D,), jnp.float32), 0.5, 1.5).astype(jnp.bfloat16),
        "cotangent": gaussian_with(key_of[11], (SEQS, SEQ_LEN, D), 1.0, 6.0, ((0, 16), (1, 2)), (0, 2, 16, 2.0)),
    }


NORM_EPS = 1e-05
BRANCH_SCALE = 1.4 / math.sqrt(40.0)
SCORE_SCALE = 0.125
MASK_FILL = -1e+30
HIGHEST = lax.Precision.HIGHEST

@jax.custom_vjp
def low(v):
    return lax.optimization_barrier(v.astype(jnp.bfloat16)).astype(jnp.float32)

@jax.custom_vjp
def low_back(v):
    return v

def low_keep(v):
    return (low(v), None)

def low_pass(kept, grad):
    return (grad,)

def back_keep(v):
    return (v, None)

def back_low(kept, grad):
    return (low(grad),)
low.defvjp(low_keep, low_pass)
low_back.defvjp(back_keep, back_low)

def angles(positions):
    inverse = 10000.0 ** (-jnp.arange(32, dtype=jnp.float32) / 32.0)
    phase = positions[:, None] * inverse[None, :]
    phase = jnp.concatenate([phase, phase], axis=-1)
    return (jnp.cos(phase), jnp.sin(phase))

def rotate(tensor, cosine, sine_tab):
    half_dim = tensor.shape[-1] // 2
    first = tensor[..., :half_dim]
    second = tensor[..., half_dim:]
    turned = jnp.concatenate([-second, first], axis=-1)
    return tensor * cosine[:, None, :] + turned * sine_tab[:, None, :]

def rms_scale(values, gain):
    factor = lax.rsqrt(lax.optimization_barrier(jnp.mean(values * values, axis=-1, keepdims=True)) + NORM_EPS)
    return values * factor * gain

def block_fn(weights, block_x, block_len):
    w_query, w_key, w_value, w_out, w_gate, w_up, w_down, gain_one, gain_two = weights
    group_n = block_x.shape[0]
    cosine, sine_tab = angles(jnp.arange(SEQ_LEN).astype(jnp.float32))
    normed = low(rms_scale(block_x, gain_one))

    def project(left, right):
        return jnp.einsum('gld,de->gle', left, right, precision=HIGHEST)

    def split_heads(tensor):
        return tensor.reshape(group_n, SEQ_LEN, HEADS, HEAD_DIM)
    queries = low(rotate(split_heads(low_back(project(normed, w_query))), cosine, sine_tab))
    keys_all = low(rotate(split_heads(low_back(project(normed, w_key))), cosine, sine_tab))
    values_all = low(split_heads(low_back(project(normed, w_value))))
    scores = low_back(jnp.einsum('gqhe,gkhe->ghqk', queries, keys_all, precision=HIGHEST) * SCORE_SCALE)
    slots = jnp.arange(SEQ_LEN)
    causal = slots[None, :] <= slots[:, None]
    visible = causal[None, None, :, :] & (slots[None, None, None, :] < block_len[:, None, None, None])
    scores = jnp.where(visible, scores, MASK_FILL)
    peak_val = lax.optimization_barrier(jnp.max(scores, axis=-1, keepdims=True))
    expo = jnp.exp(scores - peak_val)
    probs = expo / lax.optimization_barrier(jnp.sum(expo, axis=-1, keepdims=True))
    attended = jnp.einsum('ghqk,gkhe->gqhe', low(probs), values_all, precision=HIGHEST)
    attended = low(low_back(attended.reshape(group_n, SEQ_LEN, HEADS * HEAD_DIM)))
    mid_state = block_x + BRANCH_SCALE * low_back(project(attended, w_out))
    normed_ffn = low(rms_scale(mid_state, gain_two))
    gate_pre = low_back(project(normed_ffn, w_gate))
    up_pre = low_back(project(normed_ffn, w_up))
    mixed = low(gate_pre / (1.0 + jnp.exp(-gate_pre)) * up_pre)
    return mid_state + BRANCH_SCALE * low_back(project(mixed, w_down))

def reference(inputs, lengths, query_weight, key_weight, value_weight, out_weight, gate_weight, up_weight, down_weight, attn_gain, ffn_gain, cotangent):
    group_n = math.gcd(SEQS, max(1, 4096 // SEQ_LEN))
    block_count = SEQS // group_n
    checked = jax.checkpoint(block_fn)

    def layer_fn(x_in, w_query, w_key, w_value, w_out, w_gate, w_up, w_down, gain_one, gain_two):
        weights = (w_query, w_key, w_value, w_out, w_gate, w_up, w_down, gain_one, gain_two)
        blocks_x = x_in.reshape(block_count, group_n, SEQ_LEN, D)
        blocks_len = lengths.reshape(block_count, group_n)

        def one_block(pair):
            return checked(weights, pair[0], pair[1])
        results = lax.map(one_block, (blocks_x, blocks_len))
        return results.reshape(SEQS, SEQ_LEN, D)
    floats = [item.astype(jnp.float32) for item in (inputs, query_weight, key_weight, value_weight, out_weight, gate_weight, up_weight, down_weight, attn_gain, ffn_gain)]
    result, pull_back = jax.vjp(layer_fn, *floats)
    live_rows = (jnp.arange(SEQ_LEN)[None, :] < lengths[:, None]).astype(jnp.float32)
    grads = pull_back(cotangent.astype(jnp.float32) * live_rows[:, :, None])
    return (result.astype(jnp.bfloat16), grads[0].astype(jnp.bfloat16), grads[1], grads[2], grads[3], grads[4], grads[5], grads[6], grads[7], grads[8], grads[9])
```

```python
import math

import jax
import jax.numpy as jnp
from jax import lax
from jax.sharding import Mesh
from jax.sharding import PartitionSpec as P

HEADS = 36
HEAD_DIM = 64

NORM_EPS = 1e-05
BRANCH_SCALE = 1.4 / math.sqrt(40.0)
SCORE_SCALE = 0.125
MASK_FILL = -1e30

BF16 = jnp.bfloat16
F32 = jnp.float32


PLANE = ("y", "x")
LINE = ("z", "c")
FLIPS = (0, 2, 1, 3)


def dot(left, right, contract=((1,), (0,))):
    return lax.dot_general(left, right, (contract, ((), ())), preferred_element_type=F32)


NT = ((1,), (1,))
TN = ((0,), (0,))


def flip_send(block, flip):
    return lax.ppermute(block, PLANE, [(p, p ^ flip) for p in range(4)])


def plane_gather(block):
    return jnp.concatenate([block] + [flip_send(block, f) for f in FLIPS[1:]], axis=0)


def plane_scatter(partial):
    rows = partial.shape[0] // 4
    total = partial[:rows].astype(F32)
    for k, f in enumerate(FLIPS[1:], 1):
        total = total + flip_send(partial[k * rows : (k + 1) * rows].astype(BF16), f).astype(F32)
    return total


def reorder(blocks):
    pairs = blocks.reshape((2, 2) + blocks.shape[1:])
    pairs = jnp.where(lax.axis_index("y") == 1, pairs[::-1], pairs)
    pairs = jnp.where(lax.axis_index("x") == 1, pairs[:, ::-1], pairs)
    return pairs.reshape(blocks.shape)


def plane_exchange(blocks):
    mine = reorder(blocks)
    got = [mine[0]] + [flip_send(mine[f], f) for f in (1, 2, 3)]
    return reorder(jnp.stack(got))


def line_gather(block):
    return lax.all_gather(block, LINE, axis=0, tiled=True)


def line_scatter(partial):
    return lax.psum_scatter(partial, LINE, scatter_dimension=0, tiled=True)


def column_weight(blocks):
    four, rows, n = blocks.shape
    z = lax.axis_size("z")
    whole = line_gather(plane_exchange(blocks).reshape(four * rows, n))
    whole = whole.reshape(z, 2, 2, 2, rows, n).transpose(2, 0, 3, 1, 4, 5)
    return whole.reshape(z * 8 * rows, n)


def column_grad(partial):
    z = lax.axis_size("z")
    n = partial.shape[1]
    rows = partial.shape[0] // (z * 8)
    lined = partial.reshape(2, z, 2, 2, rows, n).transpose(1, 3, 0, 2, 4, 5)
    mine = line_scatter(lined.reshape(z * 8 * rows, n))
    return plane_exchange(mine.reshape(4, rows, n))


def head_order():
    z = lax.axis_size("z")
    pairs = []
    for zi in range(z):
        for xi in range(2):
            for ci in range(2):
                pairs.append((xi * 2 * z + 2 * zi + ci, (zi * 2 + xi) * 2 + ci))
    return pairs


def angle_tables(positions):
    inverse = 10000.0 ** (-jnp.arange(32, dtype=F32) / 32.0)
    phase = positions[:, None] * inverse[None, :]
    phase = jnp.concatenate([phase, phase], axis=-1)
    return jnp.cos(phase), jnp.sin(phase)


def rotate(tensor, cosine, sine):
    half = HEAD_DIM // 2
    turned = jnp.concatenate([-tensor[..., half:], tensor[..., :half]], axis=-1)
    return tensor * cosine[:, None, :] + turned * sine[:, None, :]


def rotate_back(grad, cosine, sine):
    half = HEAD_DIM // 2
    scaled = grad * sine[:, None, :]
    turned = jnp.concatenate([scaled[..., half:], -scaled[..., :half]], axis=-1)
    return grad * cosine[:, None, :] + turned


def norm_factor(values):
    return lax.rsqrt(jnp.mean(values * values, axis=-1, keepdims=True) + NORM_EPS)


def norm_back(values, factor, grad):
    mean = jnp.mean(values * grad, axis=-1, keepdims=True)
    return factor * (grad - values * (factor * factor) * mean)


def einsum(spec, left, right):
    return jnp.einsum(spec, left, right, preferred_element_type=F32)


def body(
    inputs,
    lengths,
    query_weight,
    key_weight,
    value_weight,
    out_weight,
    gate_weight,
    up_weight,
    down_weight,
    attn_gain,
    ffn_gain,
    cotangent,
):
    count, tokens, width = inputs.shape
    rows = query_weight.shape[0]
    units = down_weight.shape[0]
    z = lax.axis_size("z")
    heads = HEADS // 4
    part = heads * HEAD_DIM
    hidden = units * 2 * z
    y = lax.axis_index("y")

    gain_one = attn_gain.astype(F32)[:, None]
    gain_two = ffn_gain.astype(F32)[:, None]

    def split_heads(weight):
        return (weight.astype(F32) * gain_one).astype(BF16).reshape(rows, 4, part)

    def split_units(weight):
        scaled = (weight.astype(F32) * gain_two).astype(BF16)
        return scaled.reshape(rows, 2, z, 2, 2 * units).transpose(1, 3, 0, 2, 4).reshape(4, rows, hidden)

    def join_units(blocks):
        return blocks.reshape(2, 2, rows, z, 2 * units).transpose(2, 0, 3, 1, 4).reshape(rows, 4 * hidden)

    out_pairs = head_order()
    w_out = line_gather(lax.ppermute(out_weight, ("z", "x", "c"), out_pairs))
    qkv_blocks = jnp.concatenate(
        [split_heads(w) for w in (query_weight, key_weight, value_weight)], axis=2
    ).transpose(1, 0, 2)
    w_qkv = column_weight(qkv_blocks)
    w_gu = column_weight(
        jnp.concatenate([split_units(gate_weight), split_units(up_weight)], axis=2)
    )
    w_down = line_gather(down_weight)

    own = jnp.arange(tokens, dtype=jnp.int32)
    place = jnp.concatenate([y * tokens + own, (1 - y) * tokens + own])
    local_place = place[:tokens]
    cosine, sine = angle_tables(place.astype(F32))
    lengths_two = jnp.stack(
        [lengths, lax.ppermute(lengths, "x", [(0, 1), (1, 0)])], axis=1
    )

    x_float = [inputs[s].astype(F32) for s in range(count)]
    factor_one = [norm_factor(v) for v in x_float]
    normed = [plane_gather((v * f).astype(BF16)) for v, f in zip(x_float, factor_one)]
    grad_y = []
    branch2 = []
    for s in range(count):
        live = (local_place < lengths[s]).astype(F32)
        grad_y.append(cotangent[s].astype(F32) * live[:, None])
        branch2.append(plane_gather((BRANCH_SCALE * grad_y[s]).astype(BF16)))

    kept = []
    mids = []
    for s in range(count):
        visible = (place[None, :] <= place[:, None])[None] & (
            place[None, None, :] < lengths_two[s][:, None, None]
        )
        visible = visible[:, None, :, :]
        lin = dot(normed[s], w_qkv).reshape(2, 2 * tokens, 3, heads, HEAD_DIM)
        queries = rotate(lin[:, :, 0], cosine, sine).astype(BF16)
        keys = rotate(lin[:, :, 1], cosine, sine).astype(BF16)
        values = lin[:, :, 2].astype(BF16)
        scores = einsum("bqhe,bkhe->bhqk", queries, keys) * SCORE_SCALE
        scores = jnp.where(visible, scores, MASK_FILL)
        expo = jnp.exp(scores - jnp.max(scores, axis=-1, keepdims=True))
        probs = expo / jnp.sum(expo, axis=-1, keepdims=True)
        attended = einsum("bhqk,bkhe->bqhe", probs.astype(BF16), values)
        attended = attended.astype(BF16).reshape(4 * tokens, part)
        mid = x_float[s] + BRANCH_SCALE * plane_scatter(dot(attended, w_out))
        kept.append((queries, keys, values, probs, attended))
        mids.append(mid)

    factor_two = [norm_factor(v) for v in mids]
    normed_ffn = [plane_gather((v * f).astype(BF16)) for v, f in zip(mids, factor_two)]
    mixes = []
    acts = []
    for s in range(count):
        both = dot(normed_ffn[s], w_gu)
        gate_pre, up_pre = both[:, :hidden], both[:, hidden:]
        sigmoid = 1.0 / (1.0 + jnp.exp(-gate_pre))
        mixes.append((gate_pre * sigmoid * up_pre).astype(BF16))
        acts.append((gate_pre, up_pre, sigmoid))
    all_mixed = jnp.concatenate(mixes, axis=0)
    all_branch2 = jnp.concatenate(branch2, axis=0)
    down_terms = dot(all_mixed, all_branch2, TN).astype(BF16).reshape(2 * z, units, width)
    padded = -(-units // 8) * 8
    down_terms = jnp.pad(down_terms, ((0, 0), (0, padded - units), (0, 0)))
    down_grad = line_scatter(down_terms.reshape(2 * z * padded, width))[:units].astype(F32)

    grad_gates = []
    grad_ups = []
    for s in range(count):
        gate_pre, up_pre, sigmoid = acts[s]
        grad_mixed = dot(branch2[s], w_down, NT)
        grad_gates.append(
            (grad_mixed * up_pre * (sigmoid + gate_pre * sigmoid * (1.0 - sigmoid))).astype(BF16)
        )
        grad_ups.append((grad_mixed * gate_pre * sigmoid).astype(BF16))
    all_ffn = jnp.concatenate(normed_ffn, axis=0)
    gate_raw = column_grad(dot(all_ffn, jnp.concatenate(grad_gates, axis=0), TN).astype(BF16))
    up_raw = column_grad(dot(all_ffn, jnp.concatenate(grad_ups, axis=0), TN).astype(BF16))

    outputs = [
        (mids[s] + BRANCH_SCALE * plane_scatter(dot(mixes[s], w_down))).astype(BF16)
        for s in range(count)
    ]

    grad_mids = []
    branch1 = []
    for s in range(count):
        both = jnp.concatenate([grad_gates[s], grad_ups[s]], axis=1)
        grad_norm = plane_scatter(dot(both, w_gu, NT))
        grad_mid = grad_y[s] + norm_back(mids[s], factor_two[s], grad_norm)
        grad_mids.append(grad_mid)
        branch1.append(plane_gather((BRANCH_SCALE * grad_mid).astype(BF16)))

    all_attended = jnp.concatenate([k[4] for k in kept], axis=0)
    all_branch1 = jnp.concatenate(branch1, axis=0)
    out_part = line_scatter(dot(all_attended, all_branch1, TN).astype(BF16))
    out_grad = lax.ppermute(out_part, ("z", "x", "c"), [(b, a) for a, b in out_pairs]).astype(F32)

    grad_qkv = []
    input_grads = []
    for s in range(count):
        queries, keys, values, probs, attended = kept[s]
        grad_att = dot(branch1[s], w_out, NT).astype(BF16).reshape(2, 2 * tokens, heads, HEAD_DIM)
        grad_probs = einsum("bqhe,bkhe->bhqk", grad_att, values)
        delta = jnp.sum(probs * grad_probs, axis=-1, keepdims=True)
        grad_scores = (probs * (grad_probs - delta)).astype(BF16)
        grad_q = einsum("bhqk,bkhe->bqhe", grad_scores, keys) * SCORE_SCALE
        grad_k = einsum("bhqk,bqhe->bkhe", grad_scores, queries) * SCORE_SCALE
        grad_v = einsum("bhqk,bqhe->bkhe", probs.astype(BF16), grad_att)
        grads = jnp.stack(
            [
                rotate_back(grad_q, cosine, sine).astype(BF16),
                rotate_back(grad_k, cosine, sine).astype(BF16),
                grad_v.astype(BF16),
            ],
            axis=2,
        ).reshape(4 * tokens, 3 * part)
        grad_qkv.append(grads)
    qkv_raw = column_grad(
        dot(jnp.concatenate(normed, axis=0), jnp.concatenate(grad_qkv, axis=0), TN).astype(BF16)
    )
    for s in range(count):
        grad_norm = plane_scatter(dot(grad_qkv[s], w_qkv, NT))
        input_grads.append(
            (grad_mids[s] + norm_back(x_float[s], factor_one[s], grad_norm)).astype(BF16)
        )

    gate_raw = join_units(gate_raw).astype(F32)
    up_raw = join_units(up_raw).astype(F32)
    ffn_gain_grad = jnp.sum(
        gate_raw * gate_weight.astype(F32) + up_raw * up_weight.astype(F32), axis=1
    )
    raws = [
        qkv_raw[:, :, i * part : (i + 1) * part].transpose(1, 0, 2).reshape(rows, width).astype(F32)
        for i in range(3)
    ]
    attn_gain_grad = jnp.sum(
        raws[0] * query_weight.astype(F32)
        + raws[1] * key_weight.astype(F32)
        + raws[2] * value_weight.astype(F32),
        axis=1,
    )
    return (
        jnp.stack(outputs, axis=0),
        jnp.stack(input_grads, axis=0),
        raws[0] * gain_one,
        raws[1] * gain_one,
        raws[2] * gain_one,
        out_grad,
        gate_raw * gain_two,
        up_raw * gain_two,
        down_grad,
        attn_gain_grad,
        ffn_gain_grad,
    )


def solution(mesh):
    seq, dp = mesh.devices.shape
    fine = Mesh(mesh.devices.reshape(seq, dp // 4, 2, 2), ("y", "z", "x", "c"))
    acts = P(("z", "x", "c"), "y", None)
    weight = P(("y", "z", "x", "c"), None)
    gain = P(("y", "z", "x", "c"))
    return jax.shard_map(
        body,
        mesh=fine,
        in_specs=(acts, P(("z", "x", "c"))) + (weight,) * 7 + (gain, gain, acts),
        out_specs=(acts, acts) + (weight,) * 7 + (gain, gain),
        check_vma=False,
    )
```

```python
import math

import jax
import jax.numpy as jnp
from jax import lax
from jax.sharding import Mesh
from jax.sharding import PartitionSpec as P


HEADS = 36
HEAD_DIM = 64

NORM_EPS = 1e-05
BRANCH_SCALE = 1.4 / math.sqrt(40.0)
SCORE_SCALE = 0.125
MASK_FILL = -1e30

BF16 = jnp.bfloat16
F32 = jnp.float32


PLANE = ("y", "l")
LINE = ("x", "c")
FLIPS = (0, 2, 1, 3)


def dot(left, right, contract=((1,), (0,))):
    return lax.dot_general(left, right, (contract, ((), ())), preferred_element_type=F32)


NT = ((1,), (1,))
TN = ((0,), (0,))


def flip_send(block, flip):
    return lax.ppermute(block, PLANE, [(p, p ^ flip) for p in range(4)])


def plane_gather(block):
    return jnp.concatenate([block] + [flip_send(block, f) for f in FLIPS[1:]], axis=0)


def plane_scatter(partial):
    rows = partial.shape[0] // 4
    total = partial[:rows].astype(F32)
    for k, f in enumerate(FLIPS[1:], 1):
        total = total + flip_send(partial[k * rows : (k + 1) * rows].astype(BF16), f).astype(F32)
    return total


def reorder(blocks):
    pairs = blocks.reshape((2, 2) + blocks.shape[1:])
    pairs = jnp.where(lax.axis_index("y") == 1, pairs[::-1], pairs)
    pairs = jnp.where(lax.axis_index("l") == 1, pairs[:, ::-1], pairs)
    return pairs.reshape(blocks.shape)


def plane_exchange(blocks):
    mine = reorder(blocks)
    got = [mine[0]] + [flip_send(mine[f], f) for f in (1, 2, 3)]
    return reorder(jnp.stack(got))


def after(value, *others):
    return lax.optimization_barrier((value,) + others)[0]


def line_gather(block):
    return lax.all_gather(block, LINE, axis=0, tiled=True)


def in_order(own, other):
    return jnp.where(
        lax.axis_index("h") == 0,
        jnp.concatenate([own, other], axis=0),
        jnp.concatenate([other, own], axis=0),
    )


def half_gather(block):
    if lax.axis_size("h") == 2:
        return in_order(block, lax.ppermute(block, "h", [(0, 1), (1, 0)]))
    return lax.all_gather(block, "h", axis=0, tiled=True)


def line_scatter(partial):
    return lax.psum_scatter(partial, LINE, scatter_dimension=0, tiled=True)


def half_scatter(partial):
    if lax.axis_size("h") == 2:
        rows = partial.shape[0] // 2
        h = lax.axis_index("h")
        other = lax.dynamic_slice_in_dim(partial, (1 - h) * rows, rows)
        own = lax.dynamic_slice_in_dim(partial, h * rows, rows)
        return own.astype(F32) + lax.ppermute(other, "h", [(0, 1), (1, 0)]).astype(F32)
    return lax.psum_scatter(partial, "h", scatter_dimension=0, tiled=True).astype(F32)


def column_block(blocks):
    four, rows, n = blocks.shape
    return half_gather(plane_exchange(blocks).reshape(four * rows, n))


def column_grad(scattered, rows):
    mine = half_scatter(scattered).astype(BF16)
    return plane_exchange(mine.reshape(4, rows, mine.shape[1]))


def to_line(tokens, rows):
    count = tokens.shape[0]
    blocks = tokens.reshape(count, 2, -1, 2, 2, 2, rows)
    return blocks.transpose(0, 4, 5, 2, 1, 3, 6).reshape(tokens.shape)


def from_line(tokens, rows):
    count = tokens.shape[0]
    blocks = tokens.reshape(count, 2, 2, -1, 2, 2, rows)
    return blocks.transpose(0, 4, 3, 5, 1, 2, 6).reshape(tokens.shape)


def head_order(flip):
    h = lax.axis_size("h")
    pairs = []
    for hi in range(h):
        for li in range(2):
            for xc in range(4):
                source = li * 4 * h + xc * h + hi
                pairs.append((source, ((hi ^ flip) * 2 + li) * 4 + xc))
    return pairs


def angle_tables(positions):
    inverse = 10000.0 ** (-jnp.arange(32, dtype=F32) / 32.0)
    phase = positions[:, None] * inverse[None, :]
    phase = jnp.concatenate([phase, phase], axis=-1)
    return jnp.cos(phase), jnp.sin(phase)


def rotate(tensor, cosine, sine):
    half = HEAD_DIM // 2
    turned = jnp.concatenate([-tensor[..., half:], tensor[..., :half]], axis=-1)
    return tensor * cosine[:, None, :] + turned * sine[:, None, :]


def rotate_back(grad, cosine, sine):
    half = HEAD_DIM // 2
    scaled = grad * sine[:, None, :]
    turned = jnp.concatenate([scaled[..., half:], -scaled[..., :half]], axis=-1)
    return grad * cosine[:, None, :] + turned


def norm_factor(values):
    return lax.rsqrt(jnp.mean(values * values, axis=-1, keepdims=True) + NORM_EPS)


def norm_back(values, factor, grad):
    mean = jnp.mean(values * grad, axis=-1, keepdims=True)
    return factor * (grad - values * (factor * factor) * mean)


def einsum(spec, left, right):
    return jnp.einsum(spec, left, right, preferred_element_type=F32)


def body(
    inputs,
    lengths,
    query_weight,
    key_weight,
    value_weight,
    out_weight,
    gate_weight,
    up_weight,
    down_weight,
    attn_gain,
    ffn_gain,
    cotangent,
):
    count, tokens, width = inputs.shape
    rows = query_weight.shape[0]
    units = down_weight.shape[0]
    halves = lax.axis_size("h")
    heads = HEADS // 4
    part = heads * HEAD_DIM
    padded = -(-units // 8) * 8
    hidden = padded * 4 * halves
    y = lax.axis_index("y")

    spare = -3 * part % 128
    spare = spare if spare >= 2 else spare + 128
    extra = jnp.concatenate(
        [attn_gain[:, None], ffn_gain[:, None], jnp.zeros((rows, spare - 2), BF16)], axis=1
    )
    extra = jnp.broadcast_to(extra[None], (4, rows, spare))

    def split_heads(weight):
        return weight.reshape(rows, 4, part).transpose(1, 0, 2)

    def split_units(weight):
        blocks = weight.reshape(rows, 2, halves, 2, 2, 2, units)
        blocks = jnp.pad(blocks, ((0, 0),) * 6 + ((0, padded - units),))
        return blocks.transpose(1, 3, 0, 4, 5, 2, 6).reshape(4, rows, hidden)

    def join_units(blocks):
        blocks = blocks.reshape(2, 2, rows, 2, 2, halves, padded)[..., :units]
        return blocks.transpose(2, 0, 5, 1, 3, 4, 6).reshape(rows, 16 * halves * units)

    HLXC = ("h", "l", "x", "c")
    if halves == 2:
        out_block = in_order(
            lax.ppermute(out_weight, HLXC, head_order(0)),
            lax.ppermute(out_weight, HLXC, head_order(1)),
        )
    else:
        out_block = half_gather(lax.ppermute(out_weight, HLXC, head_order(0)))
    qkv_columns = jnp.concatenate(
        [split_heads(w) for w in (query_weight, key_weight, value_weight)] + [extra], axis=2
    )
    qkv_block = column_block(qkv_columns)
    late_gate, late_up, late_down, qkv_columns = lax.optimization_barrier(
        (gate_weight, up_weight, down_weight, qkv_columns)
    )
    gu_block = column_block(
        jnp.concatenate([split_units(late_gate), split_units(late_up)], axis=2)
    )
    down_block = half_gather(jnp.pad(late_down, ((0, padded - units), (0, 0))))
    w_out = line_gather(out_block)
    w_qkv = line_gather(qkv_block)
    w_gu = line_gather(gu_block)
    w_down = line_gather(down_block)

    own = jnp.arange(tokens, dtype=jnp.int32)
    place = jnp.concatenate([y * tokens + own, (1 - y) * tokens + own])
    local_place = place[:tokens]
    cosine, sine = angle_tables(place.astype(F32))
    lengths_two = jnp.stack(
        [lengths, lax.ppermute(lengths, "l", [(0, 1), (1, 0)])], axis=1
    )

    x_float = [inputs[s].astype(F32) for s in range(count)]
    gathered = [plane_gather(to_line(inputs[s], rows)) for s in range(count)]
    grad_y = []
    branch2 = []
    for s in range(count):
        live = (local_place < lengths[s]).astype(F32)
        grad_y.append(cotangent[s].astype(F32) * live[:, None])
        branch2.append(plane_gather((BRANCH_SCALE * grad_y[s]).astype(BF16)))

    pick = (
        lax.broadcasted_iota(jnp.int32, (8, spare), 0)
        == lax.broadcasted_iota(jnp.int32, (8, spare), 1)
    ).astype(BF16)
    gains = dot(pick, w_qkv[:, 3 * part :], NT)
    gain_one_line = gains[0:1]
    gain_one = from_line(gain_one_line, rows)
    gain_two = from_line(gains[1:2], rows)

    kept = []
    mids = []
    normed = []
    for s in range(count):
        whole = gathered[s].astype(F32)
        normed.append((whole * norm_factor(whole) * gain_one_line).astype(BF16))
        visible = (place[None, :] <= place[:, None])[None] & (
            place[None, None, :] < lengths_two[s][:, None, None]
        )
        visible = visible[:, None, :, :]
        lin = dot(normed[s], w_qkv)[:, : 3 * part].reshape(2, 2 * tokens, 3, heads, HEAD_DIM)
        queries = rotate(lin[:, :, 0], cosine, sine).astype(BF16)
        keys = rotate(lin[:, :, 1], cosine, sine).astype(BF16)
        values = lin[:, :, 2].astype(BF16)
        scores = einsum("bqhe,bkhe->bhqk", queries, keys) * SCORE_SCALE
        scores = jnp.where(visible, scores, MASK_FILL)
        expo = jnp.exp(scores - jnp.max(scores, axis=-1, keepdims=True))
        probs = expo / jnp.sum(expo, axis=-1, keepdims=True)
        attended = einsum("bhqk,bkhe->bqhe", probs.astype(BF16), values)
        attended = attended.astype(BF16).reshape(4 * tokens, part)
        mid = x_float[s] + BRANCH_SCALE * plane_scatter(dot(attended, w_out))
        kept.append((queries, keys, values, probs, attended))
        mids.append(mid)

    factor_two = [norm_factor(v) for v in mids]
    normed_ffn = [
        plane_gather(to_line((v * f * gain_two).astype(BF16), rows))
        for v, f in zip(mids, factor_two)
    ]
    mixes = []
    acts = []
    for s in range(count):
        both = dot(normed_ffn[s], w_gu)
        gate_pre, up_pre = both[:, :hidden], both[:, hidden:]
        sigmoid = 1.0 / (1.0 + jnp.exp(-gate_pre))
        mixes.append((gate_pre * sigmoid * up_pre).astype(BF16))
        acts.append((gate_pre, up_pre, sigmoid))
    all_mixed = jnp.concatenate(mixes, axis=0)
    all_branch2 = jnp.concatenate(branch2, axis=0)
    down_terms = dot(all_mixed, all_branch2, TN).astype(BF16)
    down_part = line_scatter(down_terms)

    grad_boths = []
    for s in range(count):
        gate_pre, up_pre, sigmoid = acts[s]
        grad_mixed = dot(after(branch2[s], down_terms), w_down, NT)
        grad_gate = grad_mixed * up_pre * (sigmoid + gate_pre * sigmoid * (1.0 - sigmoid))
        grad_up = grad_mixed * gate_pre * sigmoid
        grad_boths.append(jnp.concatenate([grad_gate.astype(BF16), grad_up.astype(BF16)], axis=1))
    norm_terms = [dot(g, w_gu, NT).astype(BF16) for g in grad_boths]
    all_ffn = after(jnp.concatenate(normed_ffn, axis=0), *norm_terms)
    gu_terms = dot(all_ffn, jnp.concatenate(grad_boths, axis=0), TN).astype(BF16)
    gu_part = line_scatter(gu_terms)

    grad_mids = []
    branch1 = []
    for s in range(count):
        grad_norm = from_line(plane_scatter(norm_terms[s]), rows) * gain_two
        grad_mid = grad_y[s] + norm_back(mids[s], factor_two[s], grad_norm)
        grad_mids.append(grad_mid)
        branch1.append(plane_gather((BRANCH_SCALE * grad_mid).astype(BF16)))

    outputs = [
        (mids[s] + BRANCH_SCALE * plane_scatter(dot(after(mixes[s], gu_terms), w_down))).astype(BF16)
        for s in range(count)
    ]

    grad_qkv = []
    input_grads = []
    for s in range(count):
        queries, keys, values, probs, attended = kept[s]
        grad_att = dot(branch1[s], w_out, NT).astype(BF16).reshape(2, 2 * tokens, heads, HEAD_DIM)
        grad_probs = einsum("bqhe,bkhe->bhqk", grad_att, values)
        delta = jnp.sum(probs * grad_probs, axis=-1, keepdims=True)
        grad_scores = (probs * (grad_probs - delta)).astype(BF16)
        grad_q = einsum("bhqk,bkhe->bqhe", grad_scores, keys) * SCORE_SCALE
        grad_k = einsum("bhqk,bqhe->bkhe", grad_scores, queries) * SCORE_SCALE
        grad_v = einsum("bhqk,bqhe->bkhe", probs.astype(BF16), grad_att)
        grads = jnp.stack(
            [
                rotate_back(grad_q, cosine, sine).astype(BF16),
                rotate_back(grad_k, cosine, sine).astype(BF16),
                grad_v.astype(BF16),
            ],
            axis=2,
        ).reshape(4 * tokens, 3 * part)
        grad_qkv.append(jnp.pad(grads, ((0, 0), (0, spare))))
    qkv_terms = dot(
        jnp.concatenate(normed, axis=0), jnp.concatenate(grad_qkv, axis=0), TN
    ).astype(BF16)
    qkv_part = line_scatter(qkv_terms)
    all_attended = after(jnp.concatenate([k[4] for k in kept], axis=0), qkv_terms)
    out_terms = dot(all_attended, jnp.concatenate(branch1, axis=0), TN).astype(BF16)
    out_part = line_scatter(out_terms)
    out_grad = lax.ppermute(
        half_scatter(out_part).astype(BF16), HLXC, [(b, a) for a, b in head_order(0)]
    ).astype(F32)
    gu_raw = column_grad(gu_part, rows)
    qkv_raw = column_grad(qkv_part, rows)
    factor_one = [norm_factor(v) for v in x_float]
    for s in range(count):
        grad_norm = from_line(plane_scatter(dot(grad_qkv[s], w_qkv, NT)), rows) * gain_one
        input_grads.append(
            (grad_mids[s] + norm_back(x_float[s], factor_one[s], grad_norm)).astype(BF16)
        )

    gate_grad = join_units(gu_raw[:, :, :hidden]).astype(F32)
    up_grad = join_units(gu_raw[:, :, hidden:]).astype(F32)
    ffn_gain_grad = jnp.sum(
        gate_grad * gate_weight.astype(F32) + up_grad * up_weight.astype(F32), axis=1
    ) / ffn_gain.astype(F32)
    qkv_grads = [
        qkv_raw[:, :, i * part : (i + 1) * part].transpose(1, 0, 2).reshape(rows, width).astype(F32)
        for i in range(3)
    ]
    attn_gain_grad = jnp.sum(
        qkv_grads[0] * query_weight.astype(F32)
        + qkv_grads[1] * key_weight.astype(F32)
        + qkv_grads[2] * value_weight.astype(F32),
        axis=1,
    ) / attn_gain.astype(F32)
    return (
        jnp.stack(outputs, axis=0),
        jnp.stack(input_grads, axis=0),
        *qkv_grads,
        out_grad,
        gate_grad,
        up_grad,
        half_scatter(down_part)[:units],
        attn_gain_grad,
        ffn_gain_grad,
    )


def solution(mesh):
    seq, dp = mesh.devices.shape
    fine = Mesh(mesh.devices.reshape(seq, dp // 8, 2, 2, 2), ("y", "h", "l", "x", "c"))
    owners = ("y", "h", "l", "x", "c")
    acts = P(owners[1:], "y", None)
    weight = P(owners, None)
    gain = P(owners)
    return jax.shard_map(
        body,
        mesh=fine,
        in_specs=(acts, P(owners[1:])) + (weight,) * 7 + (gain, gain, acts),
        out_specs=(acts, acts) + (weight,) * 7 + (gain, gain),
        check_vma=False,
    )
```

```python
import math

import jax
import jax.numpy as jnp
from jax import lax
from jax.sharding import Mesh
from jax.sharding import PartitionSpec as P


HEADS = 36
HEAD_DIM = 64

NORM_EPS = 1e-05
BRANCH_SCALE = 1.4 / math.sqrt(40.0)
SCORE_SCALE = 0.125
MASK_FILL = -1e30

BF16 = jnp.bfloat16
F32 = jnp.float32


PLANE = ("y", "l")
LINE = ("x", "c")
FLIPS = (0, 2, 1, 3)


def dot(left, right, contract=((1,), (0,))):
    return lax.dot_general(left, right, (contract, ((), ())), preferred_element_type=F32)


NT = ((1,), (1,))
TN = ((0,), (0,))


def flip_send(block, flip):
    return lax.ppermute(block, PLANE, [(p, p ^ flip) for p in range(4)])


def plane_gather(block):
    return jnp.concatenate([block] + [flip_send(block, f) for f in FLIPS[1:]], axis=0)


def plane_scatter(partial):
    rows = partial.shape[0] // 4
    total = partial[:rows].astype(F32)
    for k, f in enumerate(FLIPS[1:], 1):
        total = total + flip_send(partial[k * rows : (k + 1) * rows].astype(BF16), f).astype(F32)
    return total


def reorder(blocks):
    pairs = blocks.reshape((2, 2) + blocks.shape[1:])
    pairs = jnp.where(lax.axis_index("y") == 1, pairs[::-1], pairs)
    pairs = jnp.where(lax.axis_index("l") == 1, pairs[:, ::-1], pairs)
    return pairs.reshape(blocks.shape)


def plane_exchange(blocks):
    mine = reorder(blocks)
    got = [mine[0]] + [flip_send(mine[f], f) for f in (1, 2, 3)]
    return reorder(jnp.stack(got))


def after(value, *others):
    return lax.optimization_barrier((value,) + others)[0]


def line_gather(block):
    return lax.all_gather(block, LINE, axis=0, tiled=True)


def in_order(own, other):
    return jnp.where(
        lax.axis_index("h") == 0,
        jnp.concatenate([own, other], axis=0),
        jnp.concatenate([other, own], axis=0),
    )


def half_gather(block):
    if lax.axis_size("h") == 2:
        other = lax.ppermute(block, "h", [(0, 1), (1, 0)])
        return in_order(block, other)
    return lax.all_gather(block, "h", axis=0, tiled=True)


def line_scatter(partial):
    return lax.psum_scatter(partial, LINE, scatter_dimension=0, tiled=True)


def half_scatter(partial):
    if lax.axis_size("h") == 2:
        rows = partial.shape[0] // 2
        h = lax.axis_index("h")
        other = lax.dynamic_slice_in_dim(partial, (1 - h) * rows, rows)
        own = lax.dynamic_slice_in_dim(partial, h * rows, rows)
        other = lax.ppermute(other, "h", [(0, 1), (1, 0)])
        return own.astype(F32) + other.astype(F32)
    return lax.psum_scatter(partial, "h", scatter_dimension=0, tiled=True).astype(F32)


def column_block(blocks):
    four, rows, n = blocks.shape
    mine = plane_exchange(blocks)
    return half_gather(mine.reshape(four * rows, n))


def column_grad(scattered, rows):
    mine = half_scatter(scattered).astype(BF16)
    return plane_exchange(mine.reshape(4, rows, mine.shape[1]))


def to_line(tokens, rows):
    count = tokens.shape[0]
    blocks = tokens.reshape(count, 2, -1, 2, 2, 2, rows)
    return blocks.transpose(0, 4, 5, 2, 1, 3, 6).reshape(tokens.shape)


def from_line(tokens, rows):
    count = tokens.shape[0]
    blocks = tokens.reshape(count, 2, 2, -1, 2, 2, rows)
    return blocks.transpose(0, 4, 3, 5, 1, 2, 6).reshape(tokens.shape)


def head_order(flip):
    h = lax.axis_size("h")
    pairs = []
    for hi in range(h):
        for li in range(2):
            for xc in range(4):
                source = li * 4 * h + xc * h + hi
                pairs.append((source, ((hi ^ flip) * 2 + li) * 4 + xc))
    return pairs


def angle_tables(positions):
    inverse = 10000.0 ** (-jnp.arange(32, dtype=F32) / 32.0)
    phase = positions[:, None] * inverse[None, :]
    phase = jnp.concatenate([phase, phase], axis=-1)
    return jnp.cos(phase), jnp.sin(phase)


def rotate(tensor, cosine, sine):
    half = HEAD_DIM // 2
    turned = jnp.concatenate([-tensor[..., half:], tensor[..., :half]], axis=-1)
    return tensor * cosine[:, None, :] + turned * sine[:, None, :]


def rotate_back(grad, cosine, sine):
    half = HEAD_DIM // 2
    scaled = grad * sine[:, None, :]
    turned = jnp.concatenate([scaled[..., half:], -scaled[..., :half]], axis=-1)
    return grad * cosine[:, None, :] + turned


def norm_factor(values):
    return lax.rsqrt(jnp.mean(values * values, axis=-1, keepdims=True) + NORM_EPS)


def norm_back(values, factor, grad):
    mean = jnp.mean(values * grad, axis=-1, keepdims=True)
    return factor * (grad - values * (factor * factor) * mean)


def einsum(spec, left, right):
    return jnp.einsum(spec, left, right, preferred_element_type=F32)


def body(
    inputs,
    lengths,
    query_weight,
    key_weight,
    value_weight,
    out_weight,
    gate_weight,
    up_weight,
    down_weight,
    attn_gain,
    ffn_gain,
    cotangent,
):
    count, tokens, width = inputs.shape
    rows = query_weight.shape[0]
    units = down_weight.shape[0]
    halves = lax.axis_size("h")
    heads = HEADS // 4
    part = heads * HEAD_DIM
    padded = -(-units // 8) * 8
    hidden = padded * 4 * halves
    y = lax.axis_index("y")

    spare = -3 * part % 128
    spare = spare if spare >= 2 else spare + 128
    extra = jnp.concatenate(
        [attn_gain[:, None], ffn_gain[:, None], jnp.zeros((rows, spare - 2), BF16)], axis=1
    )
    extra = jnp.broadcast_to(extra[None], (4, rows, spare))

    def split_heads(weight):
        return weight.reshape(rows, 4, part).transpose(1, 0, 2)

    def split_units(weight):
        blocks = weight.reshape(rows, 2, halves, 2, 2, 2, units)
        blocks = jnp.pad(blocks, ((0, 0),) * 6 + ((0, padded - units),))
        return blocks.transpose(1, 3, 0, 4, 5, 2, 6).reshape(4, rows, hidden)

    def join_units(blocks):
        blocks = blocks.reshape(2, 2, rows, 2, 2, halves, padded)[..., :units]
        return blocks.transpose(2, 0, 5, 1, 3, 4, 6).reshape(rows, 16 * halves * units)

    HLXC = ("h", "l", "x", "c")
    if halves == 2:
        pair = [lax.ppermute(out_weight, HLXC, head_order(flip)) for flip in (0, 1)]
        out_block = in_order(*pair)
    else:
        out_block = half_gather(lax.ppermute(out_weight, HLXC, head_order(0)))
    other_lengths = lax.ppermute(lengths, "l", [(0, 1), (1, 0)])
    gathered = [plane_gather(to_line(inputs[s], rows)) for s in range(count)]
    down_block = half_gather(jnp.pad(down_weight, ((0, padded - units), (0, 0))))
    qkv_block = column_block(
        jnp.concatenate(
            [split_heads(w) for w in (query_weight, key_weight, value_weight)] + [extra], axis=2
        ),
    )
    gu_block = column_block(
        jnp.concatenate([split_units(gate_weight), split_units(up_weight)], axis=2)
    )
    w_out = line_gather(out_block)
    w_qkv = line_gather(qkv_block)
    w_gu = line_gather(gu_block)
    w_down = line_gather(down_block)

    step = jnp.arange(tokens, dtype=jnp.int32)
    place = jnp.concatenate([y * tokens + step, (1 - y) * tokens + step])
    local_place = place[:tokens]
    cosine, sine = angle_tables(place.astype(F32))
    lengths_two = jnp.stack([lengths, other_lengths], axis=1)

    x_float = [inputs[s].astype(F32) for s in range(count)]
    grad_y = []
    branch2 = []
    for s in range(count):
        live = (local_place < lengths[s]).astype(F32)
        grad_y.append(cotangent[s].astype(F32) * live[:, None])
        branch2.append(plane_gather((BRANCH_SCALE * grad_y[s]).astype(BF16)))

    pick = (
        lax.broadcasted_iota(jnp.int32, (8, spare), 0)
        == lax.broadcasted_iota(jnp.int32, (8, spare), 1)
    ).astype(BF16)
    gains = dot(pick, w_qkv[:, 3 * part :], NT)
    gain_one_line = gains[0:1]
    gain_one = from_line(gain_one_line, rows)
    gain_two = from_line(gains[1:2], rows)

    kept = []
    mids = []
    normed = []
    for s in range(count):
        whole = gathered[s].astype(F32)
        normed.append((whole * norm_factor(whole) * gain_one_line).astype(BF16))
        visible = (place[None, :] <= place[:, None])[None] & (
            place[None, None, :] < lengths_two[s][:, None, None]
        )
        visible = visible[:, None, :, :]
        lin = dot(normed[s], w_qkv)[:, : 3 * part].reshape(2, 2 * tokens, 3, heads, HEAD_DIM)
        queries = rotate(lin[:, :, 0], cosine, sine).astype(BF16)
        keys = rotate(lin[:, :, 1], cosine, sine).astype(BF16)
        values = lin[:, :, 2].astype(BF16)
        scores = einsum("bqhe,bkhe->bhqk", queries, keys) * SCORE_SCALE
        scores = jnp.where(visible, scores, MASK_FILL)
        expo = jnp.exp(scores - jnp.max(scores, axis=-1, keepdims=True))
        probs = expo / jnp.sum(expo, axis=-1, keepdims=True)
        attended = einsum("bhqk,bkhe->bqhe", probs.astype(BF16), values)
        attended = attended.astype(BF16).reshape(4 * tokens, part)
        mid = x_float[s] + BRANCH_SCALE * plane_scatter(dot(attended, w_out))
        kept.append((queries, keys, values, probs, attended))
        mids.append(mid)

    factor_two = [norm_factor(v) for v in mids]
    normed_ffn = [
        plane_gather(to_line((v * f * gain_two).astype(BF16), rows))
        for v, f in zip(mids, factor_two)
    ]
    mixes = []
    acts = []
    for s in range(count):
        both = dot(normed_ffn[s], w_gu)
        gate_pre, up_pre = both[:, :hidden], both[:, hidden:]
        sigmoid = 1.0 / (1.0 + jnp.exp(-gate_pre))
        mixes.append((gate_pre * sigmoid * up_pre).astype(BF16))
        acts.append((gate_pre, up_pre, sigmoid))
    all_mixed = jnp.concatenate(mixes, axis=0)
    all_branch2 = jnp.concatenate(branch2, axis=0)
    down_terms = dot(all_mixed, all_branch2, TN).astype(BF16)
    down_part = line_scatter(down_terms)

    grad_boths = []
    for s in range(count):
        gate_pre, up_pre, sigmoid = acts[s]
        grad_mixed = dot(after(branch2[s], down_terms), w_down, NT)
        grad_gate = grad_mixed * up_pre * (sigmoid + gate_pre * sigmoid * (1.0 - sigmoid))
        grad_up = grad_mixed * gate_pre * sigmoid
        grad_boths.append(jnp.concatenate([grad_gate.astype(BF16), grad_up.astype(BF16)], axis=1))
    norm_terms = [dot(g, w_gu, NT).astype(BF16) for g in grad_boths]
    all_ffn = after(jnp.concatenate(normed_ffn, axis=0), *norm_terms)
    gu_terms = dot(all_ffn, jnp.concatenate(grad_boths, axis=0), TN).astype(BF16)
    gu_part = line_scatter(gu_terms)

    grad_mids = []
    branch1 = []
    for s in range(count):
        grad_norm = from_line(plane_scatter(norm_terms[s]), rows) * gain_two
        grad_mid = grad_y[s] + norm_back(mids[s], factor_two[s], grad_norm)
        grad_mids.append(grad_mid)
        branch1.append(plane_gather((BRANCH_SCALE * grad_mid).astype(BF16)))

    outputs = [
        (mids[s] + BRANCH_SCALE * plane_scatter(dot(after(mixes[s], gu_terms), w_down))).astype(BF16)
        for s in range(count)
    ]

    grad_qkv = []
    input_grads = []
    for s in range(count):
        queries, keys, values, probs, attended = kept[s]
        grad_att = dot(after(branch1[s], down_part), w_out, NT).astype(BF16).reshape(2, 2 * tokens, heads, HEAD_DIM)
        grad_probs = einsum("bqhe,bkhe->bhqk", grad_att, values)
        delta = jnp.sum(probs * grad_probs, axis=-1, keepdims=True)
        grad_scores = (probs * (grad_probs - delta)).astype(BF16)
        grad_q = einsum("bhqk,bkhe->bqhe", grad_scores, keys) * SCORE_SCALE
        grad_k = einsum("bhqk,bqhe->bkhe", grad_scores, queries) * SCORE_SCALE
        grad_v = einsum("bhqk,bqhe->bkhe", probs.astype(BF16), grad_att)
        grads = jnp.stack(
            [
                rotate_back(grad_q, cosine, sine).astype(BF16),
                rotate_back(grad_k, cosine, sine).astype(BF16),
                grad_v.astype(BF16),
            ],
            axis=2,
        ).reshape(4 * tokens, 3 * part)
        grad_qkv.append(jnp.pad(grads, ((0, 0), (0, spare))))
    qkv_terms = dot(
        jnp.concatenate(normed, axis=0), jnp.concatenate(grad_qkv, axis=0), TN
    ).astype(BF16)
    qkv_part = line_scatter(qkv_terms)
    all_attended = after(jnp.concatenate([k[4] for k in kept], axis=0), qkv_terms)
    out_terms = dot(all_attended, jnp.concatenate(branch1, axis=0), TN).astype(BF16)
    out_part = line_scatter(out_terms)
    own = out_part.shape[0] // halves
    if halves == 2:
        h = lax.axis_index("h")
        out_grad = sum(
            lax.ppermute(
                lax.dynamic_slice_in_dim(out_part, (h ^ flip) * own, own),
                HLXC,
                [(b, a) for a, b in head_order(flip)],
            ).astype(F32)
            for flip in (0, 1)
        )
    else:
        out_grad = lax.ppermute(half_scatter(out_part), HLXC, [(b, a) for a, b in head_order(0)])
    gu_raw = column_grad(gu_part, rows)
    qkv_raw = column_grad(qkv_part, rows)
    factor_one = [norm_factor(v) for v in x_float]
    for s in range(count):
        in_terms = dot(after(grad_qkv[s], gu_part, out_terms), w_qkv, NT)
        grad_norm = plane_scatter(in_terms)
        grad_norm = from_line(grad_norm, rows) * gain_one
        input_grads.append(
            (grad_mids[s] + norm_back(x_float[s], factor_one[s], grad_norm)).astype(BF16)
        )

    gate_grad = join_units(gu_raw[:, :, :hidden]).astype(F32)
    up_grad = join_units(gu_raw[:, :, hidden:]).astype(F32)
    ffn_gain_grad = jnp.sum(
        gate_grad * gate_weight.astype(F32) + up_grad * up_weight.astype(F32), axis=1
    ) / ffn_gain.astype(F32)
    qkv_grads = [
        qkv_raw[:, :, i * part : (i + 1) * part].transpose(1, 0, 2).reshape(rows, width).astype(F32)
        for i in range(3)
    ]
    attn_gain_grad = jnp.sum(
        qkv_grads[0] * query_weight.astype(F32)
        + qkv_grads[1] * key_weight.astype(F32)
        + qkv_grads[2] * value_weight.astype(F32),
        axis=1,
    ) / attn_gain.astype(F32)
    return (
        jnp.stack(outputs, axis=0),
        jnp.stack(input_grads, axis=0),
        *qkv_grads,
        out_grad,
        gate_grad,
        up_grad,
        half_scatter(down_part)[:units],
        attn_gain_grad,
        ffn_gain_grad,
    )


def solution(mesh):
    seq, dp = mesh.devices.shape
    fine = Mesh(mesh.devices.reshape(seq, dp // 8, 2, 2, 2), ("y", "h", "l", "x", "c"))
    owners = ("y", "h", "l", "x", "c")
    acts = P(owners[1:], "y", None)
    weight = P(owners, None)
    gain = P(owners)
    return jax.shard_map(
        body,
        mesh=fine,
        in_specs=(acts, P(owners[1:])) + (weight,) * 7 + (gain, gain, acts),
        out_specs=(acts, acts) + (weight,) * 7 + (gain, gain),
        check_vma=False,
    )
```

```python
import math

import jax
import jax.numpy as jnp
from jax import lax
from jax.sharding import Mesh
from jax.sharding import PartitionSpec as P


HEADS = 36
HEAD_DIM = 64

NORM_EPS = 1e-05
BRANCH_SCALE = 1.4 / math.sqrt(40.0)
SCORE_SCALE = 0.125
MASK_FILL = -1e30

BF16 = jnp.bfloat16
F32 = jnp.float32


PLANE = ("y", "l")
LINE = ("x", "c")
FLIPS = (0, 2, 1, 3)


def dot(left, right, contract=((1,), (0,))):
    return lax.dot_general(left, right, (contract, ((), ())), preferred_element_type=F32)


NT = ((1,), (1,))
TN = ((0,), (0,))


def flip_send(block, flip):
    return lax.ppermute(block, PLANE, [(p, p ^ flip) for p in range(4)])


def plane_gather(block):
    return jnp.concatenate([block] + [flip_send(block, f) for f in FLIPS[1:]], axis=0)


def plane_scatter(partial):
    rows = partial.shape[0] // 4
    total = partial[:rows].astype(F32)
    for k, f in enumerate(FLIPS[1:], 1):
        total = total + flip_send(partial[k * rows : (k + 1) * rows].astype(BF16), f).astype(F32)
    return total


def reorder(blocks):
    pairs = blocks.reshape((2, 2) + blocks.shape[1:])
    pairs = jnp.where(lax.axis_index("y") == 1, pairs[::-1], pairs)
    pairs = jnp.where(lax.axis_index("l") == 1, pairs[:, ::-1], pairs)
    return pairs.reshape(blocks.shape)


def plane_exchange(blocks):
    mine = reorder(blocks)
    got = [mine[0]] + [flip_send(mine[f], f) for f in (1, 2, 3)]
    return reorder(jnp.stack(got))


def after(value, *others):
    return lax.optimization_barrier((value,) + others)[0]


def line_gather(block):
    return lax.all_gather(block, LINE, axis=0, tiled=True)


def in_order(own, other):
    return jnp.where(
        lax.axis_index("h") == 0,
        jnp.concatenate([own, other], axis=0),
        jnp.concatenate([other, own], axis=0),
    )


def half_gather(block):
    if lax.axis_size("h") == 2:
        other = lax.ppermute(block, "h", [(0, 1), (1, 0)])
        return in_order(block, other)
    return lax.all_gather(block, "h", axis=0, tiled=True)


def line_scatter(partial):
    return lax.psum_scatter(partial, LINE, scatter_dimension=0, tiled=True)


def half_scatter(partial, *late):
    if lax.axis_size("h") == 2:
        rows = partial.shape[0] // 2
        h = lax.axis_index("h")
        other = lax.dynamic_slice_in_dim(partial, (1 - h) * rows, rows)
        own = lax.dynamic_slice_in_dim(partial, h * rows, rows)
        other = lax.ppermute(other, "h", [(0, 1), (1, 0)])
        if late:
            own = after(own, *late)
        return own.astype(F32) + other.astype(F32)
    return lax.psum_scatter(partial, "h", scatter_dimension=0, tiled=True).astype(F32)


def column_block(blocks):
    four, rows, n = blocks.shape
    mine = plane_exchange(blocks)
    return half_gather(mine.reshape(four * rows, n))


def column_grad(scattered, rows, *late):
    mine = half_scatter(scattered, *late).astype(BF16)
    return plane_exchange(mine.reshape(4, rows, mine.shape[1]))


def to_line(tokens, rows):
    count = tokens.shape[0]
    blocks = tokens.reshape(count, 2, -1, 2, 2, 2, rows)
    return blocks.transpose(0, 4, 5, 2, 1, 3, 6).reshape(tokens.shape)


def from_line(tokens, rows):
    count = tokens.shape[0]
    blocks = tokens.reshape(count, 2, 2, -1, 2, 2, rows)
    return blocks.transpose(0, 4, 3, 5, 1, 2, 6).reshape(tokens.shape)


def head_order(flip):
    h = lax.axis_size("h")
    pairs = []
    for hi in range(h):
        for li in range(2):
            for xc in range(4):
                source = li * 4 * h + xc * h + hi
                pairs.append((source, ((hi ^ flip) * 2 + li) * 4 + xc))
    return pairs


def angle_tables(positions):
    inverse = 10000.0 ** (-jnp.arange(32, dtype=F32) / 32.0)
    phase = positions[:, None] * inverse[None, :]
    phase = jnp.concatenate([phase, phase], axis=-1)
    return jnp.cos(phase), jnp.sin(phase)


def rotate(tensor, cosine, sine):
    half = HEAD_DIM // 2
    turned = jnp.concatenate([-tensor[..., half:], tensor[..., :half]], axis=-1)
    return tensor * cosine[:, None, :] + turned * sine[:, None, :]


def rotate_back(grad, cosine, sine):
    half = HEAD_DIM // 2
    scaled = grad * sine[:, None, :]
    turned = jnp.concatenate([scaled[..., half:], -scaled[..., :half]], axis=-1)
    return grad * cosine[:, None, :] + turned


def norm_factor(values):
    return lax.rsqrt(jnp.mean(values * values, axis=-1, keepdims=True) + NORM_EPS)


def norm_back(values, factor, grad):
    mean = jnp.mean(values * grad, axis=-1, keepdims=True)
    return factor * (grad - values * (factor * factor) * mean)


def einsum(spec, left, right):
    return jnp.einsum(spec, left, right, preferred_element_type=F32)


def body(
    inputs,
    lengths,
    query_weight,
    key_weight,
    value_weight,
    out_weight,
    gate_weight,
    up_weight,
    down_weight,
    attn_gain,
    ffn_gain,
    cotangent,
):
    count, tokens, width = inputs.shape
    rows = query_weight.shape[0]
    units = down_weight.shape[0]
    halves = lax.axis_size("h")
    heads = HEADS // 4
    part = heads * HEAD_DIM
    padded = -(-units // 8) * 8
    hidden = padded * 4 * halves
    y = lax.axis_index("y")

    spare = -3 * part % 128
    spare = spare if spare >= 2 else spare + 128
    extra = jnp.concatenate(
        [attn_gain[:, None], ffn_gain[:, None], jnp.zeros((rows, spare - 2), BF16)], axis=1
    )
    extra = jnp.broadcast_to(extra[None], (4, rows, spare))

    def split_heads(weight):
        return weight.reshape(rows, 4, part).transpose(1, 0, 2)

    def split_units(weight):
        blocks = weight.reshape(rows, 2, halves, 2, 2, 2, units)
        blocks = jnp.pad(blocks, ((0, 0),) * 6 + ((0, padded - units),))
        return blocks.transpose(1, 3, 0, 4, 5, 2, 6).reshape(4, rows, hidden)

    def join_units(blocks):
        blocks = blocks.reshape(2, 2, rows, 2, 2, halves, padded)[..., :units]
        return blocks.transpose(2, 0, 5, 1, 3, 4, 6).reshape(rows, 16 * halves * units)

    HLXC = ("h", "l", "x", "c")
    if halves == 2:
        pair = [lax.ppermute(out_weight, HLXC, head_order(flip)) for flip in (0, 1)]
        out_block = in_order(*pair)
    else:
        out_block = half_gather(lax.ppermute(out_weight, HLXC, head_order(0)))
    other_lengths = lax.ppermute(lengths, "l", [(0, 1), (1, 0)])
    down_block = half_gather(jnp.pad(down_weight, ((0, padded - units), (0, 0))))
    qkv_block = column_block(
        jnp.concatenate(
            [split_heads(w) for w in (query_weight, key_weight, value_weight)] + [extra], axis=2
        ),
    )
    gu_block = column_block(
        jnp.concatenate([split_units(gate_weight), split_units(up_weight)], axis=2)
    )
    gathered = [plane_gather(to_line(inputs[s], rows)) for s in range(count)]
    w_out = line_gather(out_block)
    w_qkv = line_gather(qkv_block)
    w_gu = line_gather(gu_block)
    w_down = line_gather(down_block)

    step = jnp.arange(tokens, dtype=jnp.int32)
    place = jnp.concatenate([y * tokens + step, (1 - y) * tokens + step])
    local_place = place[:tokens]
    cosine, sine = angle_tables(place.astype(F32))
    lengths_two = jnp.stack([lengths, other_lengths], axis=1)

    x_float = [inputs[s].astype(F32) for s in range(count)]
    grad_y = []
    branch2 = []
    for s in range(count):
        live = (local_place < lengths[s]).astype(F32)
        grad_y.append(cotangent[s].astype(F32) * live[:, None])
        branch2.append(plane_gather((BRANCH_SCALE * grad_y[s]).astype(BF16)))

    pick = (
        lax.broadcasted_iota(jnp.int32, (8, spare), 0)
        == lax.broadcasted_iota(jnp.int32, (8, spare), 1)
    ).astype(BF16)
    gains = dot(pick, w_qkv[:, 3 * part :], NT)
    gain_one_line = gains[0:1]
    gain_one = from_line(gain_one_line, rows)
    gain_two = from_line(gains[1:2], rows)

    kept = []
    mids = []
    normed = []
    for s in range(count):
        whole = gathered[s].astype(F32)
        normed.append((whole * norm_factor(whole) * gain_one_line).astype(BF16))
        visible = (place[None, :] <= place[:, None])[None] & (
            place[None, None, :] < lengths_two[s][:, None, None]
        )
        visible = visible[:, None, :, :]
        lin = dot(normed[s], w_qkv)[:, : 3 * part].reshape(2, 2 * tokens, 3, heads, HEAD_DIM)
        queries = rotate(lin[:, :, 0], cosine, sine).astype(BF16)
        keys = rotate(lin[:, :, 1], cosine, sine).astype(BF16)
        values = lin[:, :, 2].astype(BF16)
        scores = einsum("bqhe,bkhe->bhqk", queries, keys) * SCORE_SCALE
        scores = jnp.where(visible, scores, MASK_FILL)
        expo = jnp.exp(scores - jnp.max(scores, axis=-1, keepdims=True))
        probs = expo / jnp.sum(expo, axis=-1, keepdims=True)
        attended = einsum("bhqk,bkhe->bqhe", probs.astype(BF16), values)
        attended = attended.astype(BF16).reshape(4 * tokens, part)
        mid = x_float[s] + BRANCH_SCALE * plane_scatter(dot(attended, w_out))
        kept.append((queries, keys, values, probs, attended))
        mids.append(mid)

    factor_two = [norm_factor(v) for v in mids]
    normed_ffn = [
        plane_gather(to_line((v * f * gain_two).astype(BF16), rows))
        for v, f in zip(mids, factor_two)
    ]
    mixes = []
    acts = []
    for s in range(count):
        both = dot(normed_ffn[s], w_gu)
        gate_pre, up_pre = both[:, :hidden], both[:, hidden:]
        sigmoid = 1.0 / (1.0 + jnp.exp(-gate_pre))
        mixes.append((gate_pre * sigmoid * up_pre).astype(BF16))
        acts.append((gate_pre, up_pre, sigmoid))
    all_mixed = jnp.concatenate(mixes, axis=0)
    all_branch2 = jnp.concatenate(branch2, axis=0)
    down_terms = dot(all_mixed, all_branch2, TN).astype(BF16)
    down_part = line_scatter(down_terms)

    grad_boths = []
    for s in range(count):
        gate_pre, up_pre, sigmoid = acts[s]
        grad_mixed = dot(after(branch2[s], down_terms), w_down, NT)
        grad_gate = grad_mixed * up_pre * (sigmoid + gate_pre * sigmoid * (1.0 - sigmoid))
        grad_up = grad_mixed * gate_pre * sigmoid
        grad_boths.append(jnp.concatenate([grad_gate.astype(BF16), grad_up.astype(BF16)], axis=1))
    norm_terms = [dot(g, w_gu, NT).astype(BF16) for g in grad_boths]
    all_ffn = after(jnp.concatenate(normed_ffn, axis=0), *norm_terms)
    gu_terms = dot(all_ffn, jnp.concatenate(grad_boths, axis=0), TN).astype(BF16)
    gu_part = line_scatter(gu_terms)

    grad_mids = []
    branch1 = []
    for s in range(count):
        grad_norm = from_line(plane_scatter(norm_terms[s]), rows) * gain_two
        grad_mid = grad_y[s] + norm_back(mids[s], factor_two[s], grad_norm)
        grad_mids.append(grad_mid)
        branch1.append(plane_gather((BRANCH_SCALE * grad_mid).astype(BF16)))

    outputs = [
        (mids[s] + BRANCH_SCALE * plane_scatter(dot(after(mixes[s], gu_terms), w_down))).astype(BF16)
        for s in range(count)
    ]

    grad_qkv = []
    input_grads = []
    for s in range(count):
        queries, keys, values, probs, attended = kept[s]
        grad_att = dot(after(branch1[s], down_part), w_out, NT).astype(BF16)
        grad_att = grad_att.reshape(2, 2 * tokens, heads, HEAD_DIM)
        grad_probs = einsum("bqhe,bkhe->bhqk", grad_att, values)
        delta = jnp.sum(probs * grad_probs, axis=-1, keepdims=True)
        grad_scores = (probs * (grad_probs - delta)).astype(BF16)
        grad_q = einsum("bhqk,bkhe->bqhe", grad_scores, keys) * SCORE_SCALE
        grad_k = einsum("bhqk,bqhe->bkhe", grad_scores, queries) * SCORE_SCALE
        grad_v = einsum("bhqk,bqhe->bkhe", probs.astype(BF16), grad_att)
        grads = jnp.stack(
            [
                rotate_back(grad_q, cosine, sine).astype(BF16),
                rotate_back(grad_k, cosine, sine).astype(BF16),
                grad_v.astype(BF16),
            ],
            axis=2,
        ).reshape(4 * tokens, 3 * part)
        grad_qkv.append(jnp.pad(grads, ((0, 0), (0, spare))))
    qkv_terms = dot(
        jnp.concatenate(normed, axis=0), jnp.concatenate(grad_qkv, axis=0), TN
    ).astype(BF16)
    qkv_part = line_scatter(qkv_terms)
    all_attended = after(jnp.concatenate([k[4] for k in kept], axis=0), qkv_terms, gu_part)
    out_terms = dot(all_attended, jnp.concatenate(branch1, axis=0), TN).astype(BF16)
    out_part = line_scatter(out_terms)
    own = out_part.shape[0] // halves
    if halves == 2:
        h = lax.axis_index("h")
        out_grad = sum(
            lax.ppermute(
                lax.dynamic_slice_in_dim(out_part, (h ^ flip) * own, own),
                HLXC,
                [(b, a) for a, b in head_order(flip)],
            ).astype(F32)
            for flip in (0, 1)
        )
    else:
        out_grad = lax.ppermute(half_scatter(out_part), HLXC, [(b, a) for a, b in head_order(0)])
    all_in_terms = [dot(after(g, out_terms), w_qkv, NT).astype(BF16) for g in grad_qkv]
    gu_raw = column_grad(gu_part, rows, *all_in_terms)
    qkv_raw = column_grad(qkv_part, rows)
    factor_one = [norm_factor(v) for v in x_float]
    for s in range(count):
        grad_norm = plane_scatter(all_in_terms[s])
        grad_norm = from_line(grad_norm, rows) * gain_one
        input_grads.append(
            (grad_mids[s] + norm_back(x_float[s], factor_one[s], grad_norm)).astype(BF16)
        )

    gate_grad = join_units(gu_raw[:, :, :hidden]).astype(F32)
    up_grad = join_units(gu_raw[:, :, hidden:]).astype(F32)
    ffn_gain_grad = jnp.sum(
        gate_grad * gate_weight.astype(F32) + up_grad * up_weight.astype(F32), axis=1
    ) / ffn_gain.astype(F32)
    qkv_grads = [
        qkv_raw[:, :, i * part : (i + 1) * part].transpose(1, 0, 2).reshape(rows, width).astype(F32)
        for i in range(3)
    ]
    attn_gain_grad = jnp.sum(
        qkv_grads[0] * query_weight.astype(F32)
        + qkv_grads[1] * key_weight.astype(F32)
        + qkv_grads[2] * value_weight.astype(F32),
        axis=1,
    ) / attn_gain.astype(F32)
    return (
        jnp.stack(outputs, axis=0),
        jnp.stack(input_grads, axis=0),
        *qkv_grads,
        out_grad,
        gate_grad,
        up_grad,
        half_scatter(down_part, qkv_part)[:units],
        attn_gain_grad,
        ffn_gain_grad,
    )


def solution(mesh):
    seq, dp = mesh.devices.shape
    fine = Mesh(mesh.devices.reshape(seq, dp // 8, 2, 2, 2), ("y", "h", "l", "x", "c"))
    owners = ("y", "h", "l", "x", "c")
    acts = P(owners[1:], "y", None)
    weight = P(owners, None)
    gain = P(owners)
    return jax.shard_map(
        body,
        mesh=fine,
        in_specs=(acts, P(owners[1:])) + (weight,) * 7 + (gain, gain, acts),
        out_specs=(acts, acts) + (weight,) * 7 + (gain, gain),
        check_vma=False,
    )
```

```python
import math

import jax
import jax.numpy as jnp
from jax import lax
from jax.sharding import Mesh
from jax.sharding import PartitionSpec as P


HEADS = 36
HEAD_DIM = 64

NORM_EPS = 1e-05
BRANCH_SCALE = 1.4 / math.sqrt(40.0)
SCORE_SCALE = 0.125
MASK_FILL = -1e30

BF16 = jnp.bfloat16
F32 = jnp.float32


PLANE = ("y", "l")
LINE = ("x", "c")
FLIPS = (0, 2, 1, 3)


def dot(left, right, contract=((1,), (0,))):
    return lax.dot_general(left, right, (contract, ((), ())), preferred_element_type=F32)


NT = ((1,), (1,))
TN = ((0,), (0,))


def flip_send(block, flip):
    return lax.ppermute(block, PLANE, [(p, p ^ flip) for p in range(4)])


def plane_gather(block):
    return jnp.concatenate([block] + [flip_send(block, f) for f in FLIPS[1:]], axis=0)


def plane_scatter(partial):
    rows = partial.shape[0] // 4
    total = partial[:rows].astype(F32)
    for k, f in enumerate(FLIPS[1:], 1):
        total = total + flip_send(partial[k * rows : (k + 1) * rows].astype(BF16), f).astype(F32)
    return total


def reorder(blocks):
    pairs = blocks.reshape((2, 2) + blocks.shape[1:])
    pairs = jnp.where(lax.axis_index("y") == 1, pairs[::-1], pairs)
    pairs = jnp.where(lax.axis_index("l") == 1, pairs[:, ::-1], pairs)
    return pairs.reshape(blocks.shape)


def plane_exchange(blocks):
    mine = reorder(blocks)
    got = [mine[0]] + [flip_send(mine[f], f) for f in (1, 2, 3)]
    return reorder(jnp.stack(got))


def after(value, *others):
    return lax.optimization_barrier((value,) + others)[0]


def line_gather(block):
    return lax.all_gather(block, LINE, axis=0, tiled=True)


def in_order(own, other):
    return jnp.where(
        lax.axis_index("h") == 0,
        jnp.concatenate([own, other], axis=0),
        jnp.concatenate([other, own], axis=0),
    )


def half_gather(block):
    if lax.axis_size("h") == 2:
        other = lax.ppermute(block, "h", [(0, 1), (1, 0)])
        return in_order(block, other)
    return lax.all_gather(block, "h", axis=0, tiled=True)


def line_scatter(partial):
    return lax.psum_scatter(partial, LINE, scatter_dimension=0, tiled=True)


def half_scatter(partial, *late):
    if lax.axis_size("h") == 2:
        rows = partial.shape[0] // 2
        h = lax.axis_index("h")
        other = lax.dynamic_slice_in_dim(partial, (1 - h) * rows, rows)
        own = lax.dynamic_slice_in_dim(partial, h * rows, rows)
        other = lax.ppermute(other, "h", [(0, 1), (1, 0)])
        if late:
            own = after(own, *late)
        return own.astype(F32) + other.astype(F32)
    return lax.psum_scatter(partial, "h", scatter_dimension=0, tiled=True).astype(F32)


def column_block(blocks):
    four, rows, n = blocks.shape
    mine = plane_exchange(blocks)
    return half_gather(mine.reshape(four * rows, n))


def column_grad(scattered, rows, *late):
    mine = half_scatter(scattered, *late).astype(BF16)
    return plane_exchange(mine.reshape(4, rows, mine.shape[1]))


def to_line(tokens, rows):
    count = tokens.shape[0]
    blocks = tokens.reshape(count, 2, -1, 2, 2, 2, rows)
    return blocks.transpose(0, 4, 5, 2, 1, 3, 6).reshape(tokens.shape)


def from_line(tokens, rows):
    count = tokens.shape[0]
    blocks = tokens.reshape(count, 2, 2, -1, 2, 2, rows)
    return blocks.transpose(0, 4, 3, 5, 1, 2, 6).reshape(tokens.shape)


def head_order(flip):
    h = lax.axis_size("h")
    pairs = []
    for hi in range(h):
        for li in range(2):
            for xc in range(4):
                source = li * 4 * h + xc * h + hi
                pairs.append((source, ((hi ^ flip) * 2 + li) * 4 + xc))
    return pairs


def angle_tables(positions):
    inverse = 10000.0 ** (-jnp.arange(32, dtype=F32) / 32.0)
    phase = positions[:, None] * inverse[None, :]
    phase = jnp.concatenate([phase, phase], axis=-1)
    return jnp.cos(phase), jnp.sin(phase)


def rotate(tensor, cosine, sine):
    half = HEAD_DIM // 2
    turned = jnp.concatenate([-tensor[..., half:], tensor[..., :half]], axis=-1)
    return tensor * cosine[:, None, :] + turned * sine[:, None, :]


def rotate_back(grad, cosine, sine):
    half = HEAD_DIM // 2
    scaled = grad * sine[:, None, :]
    turned = jnp.concatenate([scaled[..., half:], -scaled[..., :half]], axis=-1)
    return grad * cosine[:, None, :] + turned


def norm_factor(values):
    return lax.rsqrt(jnp.mean(values * values, axis=-1, keepdims=True) + NORM_EPS)


def norm_back(values, factor, grad):
    mean = jnp.mean(values * grad, axis=-1, keepdims=True)
    return factor * (grad - values * (factor * factor) * mean)


def einsum(spec, left, right):
    return jnp.einsum(spec, left, right, preferred_element_type=F32)


def body(
    inputs,
    lengths,
    query_weight,
    key_weight,
    value_weight,
    out_weight,
    gate_weight,
    up_weight,
    down_weight,
    attn_gain,
    ffn_gain,
    cotangent,
):
    count, tokens, width = inputs.shape
    rows = query_weight.shape[0]
    units = down_weight.shape[0]
    halves = lax.axis_size("h")
    heads = HEADS // 4
    part = heads * HEAD_DIM
    padded = -(-units // 8) * 8
    hidden = padded * 4 * halves
    y = lax.axis_index("y")

    spare = -3 * part % 128
    spare = spare if spare >= 2 else spare + 128
    extra = jnp.concatenate(
        [attn_gain[:, None], ffn_gain[:, None], jnp.zeros((rows, spare - 2), BF16)], axis=1
    )
    extra = jnp.broadcast_to(extra[None], (4, rows, spare))

    def split_heads(weight):
        return weight.reshape(rows, 4, part).transpose(1, 0, 2)

    def split_units(weight):
        blocks = weight.reshape(rows, 2, halves, 2, 2, 2, units)
        blocks = jnp.pad(blocks, ((0, 0),) * 6 + ((0, padded - units),))
        return blocks.transpose(1, 3, 0, 4, 5, 2, 6).reshape(4, rows, hidden)

    def join_units(blocks):
        blocks = blocks.reshape(2, 2, rows, 2, 2, halves, padded)[..., :units]
        return blocks.transpose(2, 0, 5, 1, 3, 4, 6).reshape(rows, 16 * halves * units)

    HLXC = ("h", "l", "x", "c")
    if halves == 2:
        pair = [lax.ppermute(out_weight, HLXC, head_order(flip)) for flip in (0, 1)]
        out_block = in_order(*pair)
    else:
        out_block = half_gather(lax.ppermute(out_weight, HLXC, head_order(0)))
    other_lengths = lax.ppermute(lengths, "l", [(0, 1), (1, 0)])
    qkv_block = column_block(
        jnp.concatenate(
            [split_heads(w) for w in (query_weight, key_weight, value_weight)] + [extra], axis=2
        ),
    )
    gu_block = column_block(
        jnp.concatenate([split_units(gate_weight), split_units(up_weight)], axis=2)
    )
    down_own = jnp.pad(down_weight, ((0, padded - units), (0, 0)))
    if halves == 2:
        down_other = lax.ppermute(down_own, "h", [(0, 1), (1, 0)])
    gathered = [plane_gather(to_line(inputs[s], rows)) for s in range(count)]
    w_out = line_gather(out_block)
    w_qkv = line_gather(qkv_block)
    w_gu = line_gather(gu_block)
    step = jnp.arange(tokens, dtype=jnp.int32)
    place = jnp.concatenate([y * tokens + step, (1 - y) * tokens + step])
    local_place = place[:tokens]
    cosine, sine = angle_tables(place.astype(F32))
    lengths_two = jnp.stack([lengths, other_lengths], axis=1)

    x_float = [inputs[s].astype(F32) for s in range(count)]
    grad_y = []
    branch2 = []
    for s in range(count):
        live = (local_place < lengths[s]).astype(F32)
        grad_y.append(cotangent[s].astype(F32) * live[:, None])
        branch2.append(plane_gather((BRANCH_SCALE * grad_y[s]).astype(BF16)))

    pick = (
        lax.broadcasted_iota(jnp.int32, (8, spare), 0)
        == lax.broadcasted_iota(jnp.int32, (8, spare), 1)
    ).astype(BF16)
    gains = dot(pick, w_qkv[:, 3 * part :], NT)
    gain_one_line = gains[0:1]
    gain_one = from_line(gain_one_line, rows)
    gain_two = from_line(gains[1:2], rows)

    kept = []
    mids = []
    normed = []
    for s in range(count):
        whole = after(gathered[s], gu_block).astype(F32)
        normed.append((whole * norm_factor(whole) * gain_one_line).astype(BF16))
        visible = (place[None, :] <= place[:, None])[None] & (
            place[None, None, :] < lengths_two[s][:, None, None]
        )
        visible = visible[:, None, :, :]
        lin = dot(normed[s], w_qkv)[:, : 3 * part].reshape(2, 2 * tokens, 3, heads, HEAD_DIM)
        queries = rotate(lin[:, :, 0], cosine, sine).astype(BF16)
        keys = rotate(lin[:, :, 1], cosine, sine).astype(BF16)
        values = lin[:, :, 2].astype(BF16)
        scores = einsum("bqhe,bkhe->bhqk", queries, keys) * SCORE_SCALE
        scores = jnp.where(visible, scores, MASK_FILL)
        expo = jnp.exp(scores - jnp.max(scores, axis=-1, keepdims=True))
        probs = expo / jnp.sum(expo, axis=-1, keepdims=True)
        attended = einsum("bhqk,bkhe->bqhe", probs.astype(BF16), values)
        attended = attended.astype(BF16).reshape(4 * tokens, part)
        if s == 0:
            if halves == 2:
                down_block = in_order(down_own, after(down_other, attended))
            else:
                down_block = half_gather(down_own)
            w_down = line_gather(down_block)
        mid = x_float[s] + BRANCH_SCALE * plane_scatter(dot(attended, w_out))
        kept.append((queries, keys, values, probs, attended))
        mids.append(mid)

    factor_two = [norm_factor(v) for v in mids]
    normed_ffn = [
        plane_gather(to_line((v * f * gain_two).astype(BF16), rows))
        for v, f in zip(mids, factor_two)
    ]
    mixes = []
    acts = []
    for s in range(count):
        both = dot(normed_ffn[s], w_gu)
        gate_pre, up_pre = both[:, :hidden], both[:, hidden:]
        sigmoid = 1.0 / (1.0 + jnp.exp(-gate_pre))
        mixes.append((gate_pre * sigmoid * up_pre).astype(BF16))
        acts.append((gate_pre, up_pre, sigmoid))
    all_mixed = jnp.concatenate(mixes, axis=0)
    all_branch2 = jnp.concatenate(branch2, axis=0)
    down_terms = dot(all_mixed, all_branch2, TN).astype(BF16)
    down_part = line_scatter(down_terms)

    grad_boths = []
    for s in range(count):
        gate_pre, up_pre, sigmoid = acts[s]
        grad_mixed = dot(after(branch2[s], down_terms), w_down, NT)
        grad_gate = grad_mixed * up_pre * (sigmoid + gate_pre * sigmoid * (1.0 - sigmoid))
        grad_up = grad_mixed * gate_pre * sigmoid
        grad_boths.append(jnp.concatenate([grad_gate.astype(BF16), grad_up.astype(BF16)], axis=1))
    norm_terms = [dot(g, w_gu, NT).astype(BF16) for g in grad_boths]
    all_ffn = after(jnp.concatenate(normed_ffn, axis=0), *norm_terms)
    gu_terms = dot(all_ffn, jnp.concatenate(grad_boths, axis=0), TN).astype(BF16)
    gu_part = line_scatter(gu_terms)

    grad_mids = []
    branch1 = []
    own_branch1 = []
    for s in range(count):
        grad_norm = plane_scatter(norm_terms[s])
        grad_norm = from_line(grad_norm, rows) * gain_two
        grad_mid = grad_y[s] + norm_back(mids[s], factor_two[s], grad_norm)
        grad_mids.append(grad_mid)
        own_branch1.append((BRANCH_SCALE * grad_mid).astype(BF16))
        branch1.append(plane_gather(own_branch1[s]))

    outputs = []
    for s in range(count):
        terms = dot(after(mixes[s], gu_terms, *own_branch1), w_down)
        outputs.append((mids[s] + BRANCH_SCALE * plane_scatter(terms)).astype(BF16))

    grad_qkv = []
    input_grads = []
    for s in range(count):
        queries, keys, values, probs, attended = kept[s]
        grad_att = dot(after(branch1[s], down_part), w_out, NT).astype(BF16)
        grad_att = grad_att.reshape(2, 2 * tokens, heads, HEAD_DIM)
        grad_probs = einsum("bqhe,bkhe->bhqk", grad_att, values)
        delta = jnp.sum(probs * grad_probs, axis=-1, keepdims=True)
        grad_scores = (probs * (grad_probs - delta)).astype(BF16)
        grad_q = einsum("bhqk,bkhe->bqhe", grad_scores, keys) * SCORE_SCALE
        grad_k = einsum("bhqk,bqhe->bkhe", grad_scores, queries) * SCORE_SCALE
        grad_v = einsum("bhqk,bqhe->bkhe", probs.astype(BF16), grad_att)
        grads = jnp.stack(
            [
                rotate_back(grad_q, cosine, sine).astype(BF16),
                rotate_back(grad_k, cosine, sine).astype(BF16),
                grad_v.astype(BF16),
            ],
            axis=2,
        ).reshape(4 * tokens, 3 * part)
        grad_qkv.append(jnp.pad(grads, ((0, 0), (0, spare))))
    qkv_terms = dot(
        jnp.concatenate(normed, axis=0), jnp.concatenate(grad_qkv, axis=0), TN
    ).astype(BF16)
    qkv_part = line_scatter(qkv_terms)
    all_attended = after(jnp.concatenate([k[4] for k in kept], axis=0), qkv_terms, gu_part)
    out_terms = dot(all_attended, jnp.concatenate(branch1, axis=0), TN).astype(BF16)
    out_part = line_scatter(out_terms)
    own = out_part.shape[0] // halves
    if halves == 2:
        h = lax.axis_index("h")
        out_grad = sum(
            lax.ppermute(
                lax.dynamic_slice_in_dim(out_part, (h ^ flip) * own, own),
                HLXC,
                [(b, a) for a, b in head_order(flip)],
            ).astype(F32)
            for flip in (0, 1)
        )
    else:
        out_grad = lax.ppermute(half_scatter(out_part), HLXC, [(b, a) for a, b in head_order(0)])
    all_in_terms = [dot(after(g, out_terms), w_qkv, NT).astype(BF16) for g in grad_qkv]
    gu_raw = column_grad(gu_part, rows, *all_in_terms)
    qkv_raw = column_grad(qkv_part, rows)
    factor_one = [norm_factor(v) for v in x_float]
    for s in range(count):
        grad_norm = plane_scatter(all_in_terms[s])
        grad_norm = from_line(grad_norm, rows) * gain_one
        input_grads.append(
            (grad_mids[s] + norm_back(x_float[s], factor_one[s], grad_norm)).astype(BF16)
        )

    gate_grad, up_grad = lax.optimization_barrier(
        (join_units(gu_raw[:, :, :hidden]), join_units(gu_raw[:, :, hidden:]))
    )
    gate_grad, up_grad = gate_grad.astype(F32), up_grad.astype(F32)
    ffn_gain_grad = jnp.sum(
        gate_grad * gate_weight.astype(F32) + up_grad * up_weight.astype(F32), axis=1
    ) / ffn_gain.astype(F32)
    qkv_grads = [
        qkv_raw[:, :, i * part : (i + 1) * part].transpose(1, 0, 2).reshape(rows, width).astype(F32)
        for i in range(3)
    ]
    attn_gain_grad = jnp.sum(
        qkv_grads[0] * query_weight.astype(F32)
        + qkv_grads[1] * key_weight.astype(F32)
        + qkv_grads[2] * value_weight.astype(F32),
        axis=1,
    ) / attn_gain.astype(F32)
    return (
        jnp.stack(outputs, axis=0),
        jnp.stack(input_grads, axis=0),
        *qkv_grads,
        out_grad,
        gate_grad,
        up_grad,
        half_scatter(down_part, qkv_part)[:units],
        attn_gain_grad,
        ffn_gain_grad,
    )


def solution(mesh):
    seq, dp = mesh.devices.shape
    fine = Mesh(mesh.devices.reshape(seq, dp // 8, 2, 2, 2), ("y", "h", "l", "x", "c"))
    owners = ("y", "h", "l", "x", "c")
    acts = P(owners[1:], "y", None)
    weight = P(owners, None)
    gain = P(owners)
    return jax.shard_map(
        body,
        mesh=fine,
        in_specs=(acts, P(owners[1:])) + (weight,) * 7 + (gain, gain, acts),
        out_specs=(acts, acts) + (weight,) * 7 + (gain, gain),
        check_vma=False,
    )
```

```python
import math

import jax
import jax.numpy as jnp
from jax import lax
from jax.sharding import Mesh
from jax.sharding import PartitionSpec as P


HEADS = 36
HEAD_DIM = 64

NORM_EPS = 1e-05
BRANCH_SCALE = 1.4 / math.sqrt(40.0)
SCORE_SCALE = 0.125
MASK_FILL = -1e30

BF16 = jnp.bfloat16
F32 = jnp.float32


PLANE = ("y", "l")
LINE = ("x", "c")
FLIPS = (0, 2, 1, 3)


def dot(left, right, contract=((1,), (0,))):
    return lax.dot_general(left, right, (contract, ((), ())), preferred_element_type=F32)


NT = ((1,), (1,))
TN = ((0,), (0,))


def flip_send(block, flip):
    return lax.ppermute(block, PLANE, [(p, p ^ flip) for p in range(4)])


def plane_gather(block, *late):
    got = [flip_send(block, f) for f in FLIPS[1:]]
    if late:
        got = [after(g, *late) for g in got]
    return jnp.concatenate([block] + got, axis=0)


def plane_scatter(partial):
    rows = partial.shape[0] // 4
    total = partial[:rows].astype(F32)
    for k, f in enumerate(FLIPS[1:], 1):
        total = total + flip_send(partial[k * rows : (k + 1) * rows].astype(BF16), f).astype(F32)
    return total


def reorder(blocks):
    pairs = blocks.reshape((2, 2) + blocks.shape[1:])
    pairs = jnp.where(lax.axis_index("y") == 1, pairs[::-1], pairs)
    pairs = jnp.where(lax.axis_index("l") == 1, pairs[:, ::-1], pairs)
    return pairs.reshape(blocks.shape)


def plane_exchange(blocks):
    mine = reorder(blocks)
    got = [mine[0]] + [flip_send(mine[f], f) for f in (1, 2, 3)]
    return reorder(jnp.stack(got))


def after(value, *others):
    return lax.optimization_barrier((value,) + others)[0]


def line_gather(block):
    return lax.all_gather(block, LINE, axis=0, tiled=True)


def in_order(own, other):
    return jnp.where(
        lax.axis_index("h") == 0,
        jnp.concatenate([own, other], axis=0),
        jnp.concatenate([other, own], axis=0),
    )


def half_gather(block):
    if lax.axis_size("h") == 2:
        other = lax.ppermute(block, "h", [(0, 1), (1, 0)])
        return in_order(block, other)
    return lax.all_gather(block, "h", axis=0, tiled=True)


def line_scatter(partial):
    return lax.psum_scatter(partial, LINE, scatter_dimension=0, tiled=True)


def half_scatter(partial, *late):
    if lax.axis_size("h") == 2:
        rows = partial.shape[0] // 2
        h = lax.axis_index("h")
        other = lax.dynamic_slice_in_dim(partial, (1 - h) * rows, rows)
        own = lax.dynamic_slice_in_dim(partial, h * rows, rows)
        other = lax.ppermute(other, "h", [(0, 1), (1, 0)])
        if late:
            own = after(own, *late)
        return own.astype(F32) + other.astype(F32)
    return lax.psum_scatter(partial, "h", scatter_dimension=0, tiled=True).astype(F32)


def column_block(blocks):
    four, rows, n = blocks.shape
    mine = plane_exchange(blocks)
    return half_gather(mine.reshape(four * rows, n))


def column_grad(scattered, rows, *late):
    mine = half_scatter(scattered, *late).astype(BF16)
    return plane_exchange(mine.reshape(4, rows, mine.shape[1]))


def to_line(tokens, rows):
    count = tokens.shape[0]
    blocks = tokens.reshape(count, 2, -1, 2, 2, 2, rows)
    return blocks.transpose(0, 4, 5, 2, 1, 3, 6).reshape(tokens.shape)


def from_line(tokens, rows):
    count = tokens.shape[0]
    blocks = tokens.reshape(count, 2, 2, -1, 2, 2, rows)
    return blocks.transpose(0, 4, 3, 5, 1, 2, 6).reshape(tokens.shape)


def head_order(flip):
    h = lax.axis_size("h")
    pairs = []
    for hi in range(h):
        for li in range(2):
            for xc in range(4):
                source = li * 4 * h + xc * h + hi
                pairs.append((source, ((hi ^ flip) * 2 + li) * 4 + xc))
    return pairs


def angle_tables(positions):
    inverse = 10000.0 ** (-jnp.arange(32, dtype=F32) / 32.0)
    phase = positions[:, None] * inverse[None, :]
    phase = jnp.concatenate([phase, phase], axis=-1)
    return jnp.cos(phase), jnp.sin(phase)


def rotate(tensor, cosine, sine):
    half = HEAD_DIM // 2
    turned = jnp.concatenate([-tensor[..., half:], tensor[..., :half]], axis=-1)
    return tensor * cosine[:, None, :] + turned * sine[:, None, :]


def rotate_back(grad, cosine, sine):
    half = HEAD_DIM // 2
    scaled = grad * sine[:, None, :]
    turned = jnp.concatenate([scaled[..., half:], -scaled[..., :half]], axis=-1)
    return grad * cosine[:, None, :] + turned


def norm_factor(values):
    return lax.rsqrt(jnp.mean(values * values, axis=-1, keepdims=True) + NORM_EPS)


def norm_back(values, factor, grad):
    mean = jnp.mean(values * grad, axis=-1, keepdims=True)
    return factor * (grad - values * (factor * factor) * mean)


def einsum(spec, left, right):
    return jnp.einsum(spec, left, right, preferred_element_type=F32)


def body(
    inputs,
    lengths,
    query_weight,
    key_weight,
    value_weight,
    out_weight,
    gate_weight,
    up_weight,
    down_weight,
    attn_gain,
    ffn_gain,
    cotangent,
):
    count, tokens, width = inputs.shape
    rows = query_weight.shape[0]
    units = down_weight.shape[0]
    halves = lax.axis_size("h")
    heads = HEADS // 4
    part = heads * HEAD_DIM
    padded = -(-units // 8) * 8
    hidden = padded * 4 * halves
    y = lax.axis_index("y")

    spare = -3 * part % 128
    spare = spare if spare >= 2 else spare + 128
    extra = jnp.concatenate(
        [attn_gain[:, None], ffn_gain[:, None], jnp.zeros((rows, spare - 2), BF16)], axis=1
    )
    extra = jnp.broadcast_to(extra[None], (4, rows, spare))

    def split_heads(weight):
        return weight.reshape(rows, 4, part).transpose(1, 0, 2)

    def split_units(weight):
        blocks = weight.reshape(rows, 2, halves, 2, 2, 2, units)
        blocks = jnp.pad(blocks, ((0, 0),) * 6 + ((0, padded - units),))
        return blocks.transpose(1, 3, 0, 4, 5, 2, 6).reshape(4, rows, hidden)

    def join_units(blocks):
        blocks = blocks.reshape(2, 2, rows, 2, 2, halves, padded)[..., :units]
        return blocks.transpose(2, 0, 5, 1, 3, 4, 6).reshape(rows, 16 * halves * units)

    HLXC = ("h", "l", "x", "c")
    if halves == 2:
        pair = [lax.ppermute(out_weight, HLXC, head_order(flip)) for flip in (0, 1)]
        out_block = in_order(*pair)
    else:
        out_block = half_gather(lax.ppermute(out_weight, HLXC, head_order(0)))
    other_lengths = lax.ppermute(lengths, "l", [(0, 1), (1, 0)])
    qkv_block = column_block(
        jnp.concatenate(
            [split_heads(w) for w in (query_weight, key_weight, value_weight)] + [extra], axis=2
        ),
    )
    gu_block = column_block(
        jnp.concatenate([split_units(gate_weight), split_units(up_weight)], axis=2)
    )
    down_own = jnp.pad(down_weight, ((0, padded - units), (0, 0)))
    if halves == 2:
        down_other = lax.ppermute(down_own, "h", [(0, 1), (1, 0)])
    gathered = [plane_gather(to_line(inputs[s], rows)) for s in range(count)]
    w_out = line_gather(out_block)
    w_qkv = line_gather(qkv_block)
    w_gu = line_gather(gu_block)
    step = jnp.arange(tokens, dtype=jnp.int32)
    place = jnp.concatenate([y * tokens + step, (1 - y) * tokens + step])
    local_place = place[:tokens]
    cosine, sine = angle_tables(place.astype(F32))
    lengths_two = jnp.stack([lengths, other_lengths], axis=1)

    x_float = [inputs[s].astype(F32) for s in range(count)]
    grad_y = []
    branch2 = []
    for s in range(count):
        live = (local_place < lengths[s]).astype(F32)
        grad_y.append(cotangent[s].astype(F32) * live[:, None])

    pick = (
        lax.broadcasted_iota(jnp.int32, (8, spare), 0)
        == lax.broadcasted_iota(jnp.int32, (8, spare), 1)
    ).astype(BF16)
    gains = dot(pick, w_qkv[:, 3 * part :], NT)
    gain_one_line = gains[0:1]
    gain_one = from_line(gain_one_line, rows)
    gain_two = from_line(gains[1:2], rows)

    kept = []
    mids = []
    normed = []
    for s in range(count):
        whole = after(gathered[s], gu_block).astype(F32)
        normed.append((whole * norm_factor(whole) * gain_one_line).astype(BF16))
        visible = (place[None, :] <= place[:, None])[None] & (
            place[None, None, :] < lengths_two[s][:, None, None]
        )
        visible = visible[:, None, :, :]
        lin = dot(normed[s], w_qkv)[:, : 3 * part].reshape(2, 2 * tokens, 3, heads, HEAD_DIM)
        queries = rotate(lin[:, :, 0], cosine, sine).astype(BF16)
        keys = rotate(lin[:, :, 1], cosine, sine).astype(BF16)
        values = lin[:, :, 2].astype(BF16)
        scores = einsum("bqhe,bkhe->bhqk", queries, keys) * SCORE_SCALE
        scores = jnp.where(visible, scores, MASK_FILL)
        expo = jnp.exp(scores - jnp.max(scores, axis=-1, keepdims=True))
        probs = expo / jnp.sum(expo, axis=-1, keepdims=True)
        attended = einsum("bhqk,bkhe->bqhe", probs.astype(BF16), values)
        attended = attended.astype(BF16).reshape(4 * tokens, part)
        if s == 0:
            if halves == 2:
                down_block = in_order(down_own, after(down_other, attended))
            else:
                down_block = half_gather(down_own)
            w_down = line_gather(down_block)
        mid = x_float[s] + BRANCH_SCALE * plane_scatter(dot(attended, w_out))
        kept.append((queries, keys, values, probs, attended))
        mids.append(mid)

    factor_two = [norm_factor(v) for v in mids]
    own_ffn = [
        to_line((v * f * gain_two).astype(BF16), rows) for v, f in zip(mids, factor_two)
    ]
    normed_ffn = [plane_gather(v) for v in own_ffn]
    for s in range(count):
        branch2.append(plane_gather((BRANCH_SCALE * grad_y[s]).astype(BF16), *own_ffn))
    mixes = []
    acts = []
    for s in range(count):
        both = dot(normed_ffn[s], w_gu)
        gate_pre, up_pre = both[:, :hidden], both[:, hidden:]
        sigmoid = 1.0 / (1.0 + jnp.exp(-gate_pre))
        mixes.append((gate_pre * sigmoid * up_pre).astype(BF16))
        acts.append((gate_pre, up_pre, sigmoid))
    all_mixed = jnp.concatenate(mixes, axis=0)
    all_branch2 = jnp.concatenate(branch2, axis=0)
    down_terms = dot(all_mixed, all_branch2, TN).astype(BF16)
    down_part = line_scatter(down_terms)

    grad_boths = []
    for s in range(count):
        gate_pre, up_pre, sigmoid = acts[s]
        grad_mixed = dot(after(branch2[s], down_terms), w_down, NT)
        grad_gate = grad_mixed * up_pre * (sigmoid + gate_pre * sigmoid * (1.0 - sigmoid))
        grad_up = grad_mixed * gate_pre * sigmoid
        grad_boths.append(jnp.concatenate([grad_gate.astype(BF16), grad_up.astype(BF16)], axis=1))
    norm_terms = [dot(g, w_gu, NT).astype(BF16) for g in grad_boths]
    all_ffn = after(jnp.concatenate(normed_ffn, axis=0), *norm_terms)
    all_boths = jnp.concatenate(grad_boths, axis=0)
    cut = -(-hidden // 128) * 128
    one_terms = dot(all_ffn, all_boths[:, :cut], TN).astype(BF16)
    one_part = line_scatter(one_terms)
    two_terms = dot(after(all_ffn, one_terms), all_boths[:, cut:], TN).astype(BF16)
    two_part = line_scatter(two_terms)

    grad_mids = []
    branch1 = []
    own_branch1 = []
    for s in range(count):
        grad_norm = plane_scatter(norm_terms[s])
        grad_norm = from_line(grad_norm, rows) * gain_two
        grad_mid = grad_y[s] + norm_back(mids[s], factor_two[s], grad_norm)
        grad_mids.append(grad_mid)
        own_branch1.append((BRANCH_SCALE * grad_mid).astype(BF16))
        branch1.append(plane_gather(own_branch1[s]))

    outputs = []
    for s in range(count):
        terms = dot(after(mixes[s], two_terms, *own_branch1), w_down)
        outputs.append((mids[s] + BRANCH_SCALE * plane_scatter(terms)).astype(BF16))

    grad_qkv = []
    input_grads = []
    for s in range(count):
        queries, keys, values, probs, attended = kept[s]
        grad_att = dot(after(branch1[s], down_part), w_out, NT).astype(BF16)
        grad_att = grad_att.reshape(2, 2 * tokens, heads, HEAD_DIM)
        grad_probs = einsum("bqhe,bkhe->bhqk", grad_att, values)
        delta = jnp.sum(probs * grad_probs, axis=-1, keepdims=True)
        grad_scores = (probs * (grad_probs - delta)).astype(BF16)
        grad_q = einsum("bhqk,bkhe->bqhe", grad_scores, keys) * SCORE_SCALE
        grad_k = einsum("bhqk,bqhe->bkhe", grad_scores, queries) * SCORE_SCALE
        grad_v = einsum("bhqk,bqhe->bkhe", probs.astype(BF16), grad_att)
        grads = jnp.stack(
            [
                rotate_back(grad_q, cosine, sine).astype(BF16),
                rotate_back(grad_k, cosine, sine).astype(BF16),
                grad_v.astype(BF16),
            ],
            axis=2,
        ).reshape(4 * tokens, 3 * part)
        grad_qkv.append(jnp.pad(grads, ((0, 0), (0, spare))))
    qkv_terms = dot(
        jnp.concatenate(normed, axis=0), jnp.concatenate(grad_qkv, axis=0), TN
    ).astype(BF16)
    qkv_part = line_scatter(qkv_terms)
    all_attended = after(jnp.concatenate([k[4] for k in kept], axis=0), qkv_terms, two_part)
    out_terms = dot(all_attended, jnp.concatenate(branch1, axis=0), TN).astype(BF16)
    out_part = line_scatter(out_terms)
    own = out_part.shape[0] // halves
    if halves == 2:
        h = lax.axis_index("h")
        out_grad = sum(
            lax.ppermute(
                lax.dynamic_slice_in_dim(out_part, (h ^ flip) * own, own),
                HLXC,
                [(b, a) for a, b in head_order(flip)],
            ).astype(F32)
            for flip in (0, 1)
        )
    else:
        out_grad = lax.ppermute(half_scatter(out_part), HLXC, [(b, a) for a, b in head_order(0)])
    all_in_terms = [dot(after(g, out_terms), w_qkv, NT).astype(BF16) for g in grad_qkv]
    qkv_raw = column_grad(qkv_part, rows)
    factor_one = [norm_factor(v) for v in x_float]
    for s in range(count):
        grad_norm = plane_scatter(all_in_terms[s])
        grad_norm = from_line(grad_norm, rows) * gain_one
        input_grads.append(
            (grad_mids[s] + norm_back(x_float[s], factor_one[s], grad_norm)).astype(BF16)
        )

    gu_raw = jnp.concatenate(
        [column_grad(one_part, rows, qkv_terms), column_grad(two_part, rows, *input_grads)],
        axis=2,
    )

    gate_grad, up_grad = lax.optimization_barrier(
        (join_units(gu_raw[:, :, :hidden]), join_units(gu_raw[:, :, hidden:]))
    )
    gate_grad, up_grad = gate_grad.astype(F32), up_grad.astype(F32)
    ffn_gain_grad = jnp.sum(
        gate_grad * gate_weight.astype(F32) + up_grad * up_weight.astype(F32), axis=1
    ) / ffn_gain.astype(F32)
    qkv_grads = [
        qkv_raw[:, :, i * part : (i + 1) * part].transpose(1, 0, 2).reshape(rows, width).astype(F32)
        for i in range(3)
    ]
    attn_gain_grad = jnp.sum(
        qkv_grads[0] * query_weight.astype(F32)
        + qkv_grads[1] * key_weight.astype(F32)
        + qkv_grads[2] * value_weight.astype(F32),
        axis=1,
    ) / attn_gain.astype(F32)
    return (
        jnp.stack(outputs, axis=0),
        jnp.stack(input_grads, axis=0),
        *qkv_grads,
        out_grad,
        gate_grad,
        up_grad,
        half_scatter(down_part, qkv_part)[:units],
        attn_gain_grad,
        ffn_gain_grad,
    )


def solution(mesh):
    seq, dp = mesh.devices.shape
    fine = Mesh(mesh.devices.reshape(seq, dp // 8, 2, 2, 2), ("y", "h", "l", "x", "c"))
    owners = ("y", "h", "l", "x", "c")
    acts = P(owners[1:], "y", None)
    weight = P(owners, None)
    gain = P(owners)
    return jax.shard_map(
        body,
        mesh=fine,
        in_specs=(acts, P(owners[1:])) + (weight,) * 7 + (gain, gain, acts),
        out_specs=(acts, acts) + (weight,) * 7 + (gain, gain),
        check_vma=False,
    )
```

```python
import math

import jax
import jax.numpy as jnp
from jax import lax
from jax.sharding import Mesh
from jax.sharding import PartitionSpec as P


HEADS = 36
HEAD_DIM = 64

NORM_EPS = 1e-05
BRANCH_SCALE = 1.4 / math.sqrt(40.0)
SCORE_SCALE = 0.125
MASK_FILL = -1e30

BF16 = jnp.bfloat16
F32 = jnp.float32


PLANE = ("y", "l")
LINE = ("x", "c")
FLIPS = (0, 2, 1, 3)


def dot(left, right, contract=((1,), (0,))):
    return lax.dot_general(left, right, (contract, ((), ())), preferred_element_type=F32)


NT = ((1,), (1,))
TN = ((0,), (0,))


def flip_send(block, flip):
    return lax.ppermute(block, PLANE, [(p, p ^ flip) for p in range(4)])


def plane_gather(block, *late):
    got = [flip_send(block, f) for f in FLIPS[1:]]
    if late:
        got = [after(g, *late) for g in got]
    return lax.optimization_barrier(jnp.concatenate([block] + got, axis=0))


def plane_scatter(partial):
    rows = partial.shape[0] // 4
    total = partial[:rows].astype(F32)
    for k, f in enumerate(FLIPS[1:], 1):
        total = total + flip_send(partial[k * rows : (k + 1) * rows].astype(BF16), f).astype(F32)
    return total


def reorder(blocks):
    pairs = blocks.reshape((2, 2) + blocks.shape[1:])
    pairs = jnp.where(lax.axis_index("y") == 1, pairs[::-1], pairs)
    pairs = jnp.where(lax.axis_index("l") == 1, pairs[:, ::-1], pairs)
    return pairs.reshape(blocks.shape)


def plane_exchange(blocks):
    mine = reorder(blocks)
    got = [mine[0]] + [flip_send(mine[f], f) for f in (1, 2, 3)]
    return reorder(jnp.stack(got))


def after(value, *others):
    return lax.optimization_barrier((value,) + others)[0]


def line_gather(block):
    return lax.all_gather(block, LINE, axis=0, tiled=True)


def in_order(own, other):
    return jnp.where(
        lax.axis_index("h") == 0,
        jnp.concatenate([own, other], axis=0),
        jnp.concatenate([other, own], axis=0),
    )


def half_gather(block):
    if lax.axis_size("h") == 2:
        other = lax.ppermute(block, "h", [(0, 1), (1, 0)])
        return in_order(block, other)
    return lax.all_gather(block, "h", axis=0, tiled=True)


def line_scatter(partial):
    return lax.psum_scatter(partial, LINE, scatter_dimension=0, tiled=True)


def half_scatter(partial, *late):
    if lax.axis_size("h") == 2:
        rows = partial.shape[0] // 2
        h = lax.axis_index("h")
        other = lax.dynamic_slice_in_dim(partial, (1 - h) * rows, rows)
        own = lax.dynamic_slice_in_dim(partial, h * rows, rows)
        other = lax.ppermute(other, "h", [(0, 1), (1, 0)])
        if late:
            own = after(own, *late)
        return own.astype(F32) + other.astype(F32)
    return lax.psum_scatter(partial, "h", scatter_dimension=0, tiled=True).astype(F32)


def column_block(blocks):
    four, rows, n = blocks.shape
    mine = plane_exchange(blocks)
    return half_gather(mine.reshape(four * rows, n))


def column_grad(scattered, rows, *late):
    mine = half_scatter(scattered, *late).astype(BF16)
    return plane_exchange(mine.reshape(4, rows, mine.shape[1]))


def to_line(tokens, rows):
    count = tokens.shape[0]
    blocks = tokens.reshape(count, 2, -1, 2, 2, 2, rows)
    return blocks.transpose(0, 4, 5, 2, 1, 3, 6).reshape(tokens.shape)


def from_line(tokens, rows):
    count = tokens.shape[0]
    blocks = tokens.reshape(count, 2, 2, -1, 2, 2, rows)
    return blocks.transpose(0, 4, 3, 5, 1, 2, 6).reshape(tokens.shape)


def head_order(flip):
    h = lax.axis_size("h")
    pairs = []
    for hi in range(h):
        for li in range(2):
            for xc in range(4):
                source = li * 4 * h + xc * h + hi
                pairs.append((source, ((hi ^ flip) * 2 + li) * 4 + xc))
    return pairs


def angle_tables(positions):
    inverse = 10000.0 ** (-jnp.arange(32, dtype=F32) / 32.0)
    phase = positions[:, None] * inverse[None, :]
    phase = jnp.concatenate([phase, phase], axis=-1)
    return jnp.cos(phase), jnp.sin(phase)


def rotate(tensor, cosine, sine):
    half = HEAD_DIM // 2
    turned = jnp.concatenate([-tensor[..., half:], tensor[..., :half]], axis=-1)
    return tensor * cosine[:, None, :] + turned * sine[:, None, :]


def rotate_back(grad, cosine, sine):
    half = HEAD_DIM // 2
    scaled = grad * sine[:, None, :]
    turned = jnp.concatenate([scaled[..., half:], -scaled[..., :half]], axis=-1)
    return grad * cosine[:, None, :] + turned


def norm_factor(values):
    return lax.rsqrt(jnp.mean(values * values, axis=-1, keepdims=True) + NORM_EPS)


def norm_back(values, factor, grad):
    mean = jnp.mean(values * grad, axis=-1, keepdims=True)
    return factor * (grad - values * (factor * factor) * mean)


def einsum(spec, left, right):
    return jnp.einsum(spec, left, right, preferred_element_type=F32)


def body(
    inputs,
    lengths,
    query_weight,
    key_weight,
    value_weight,
    out_weight,
    gate_weight,
    up_weight,
    down_weight,
    attn_gain,
    ffn_gain,
    cotangent,
):
    count, tokens, width = inputs.shape
    rows = query_weight.shape[0]
    units = down_weight.shape[0]
    halves = lax.axis_size("h")
    heads = HEADS // 4
    part = heads * HEAD_DIM
    padded = -(-units // 8) * 8
    hidden = padded * 4 * halves
    y = lax.axis_index("y")

    spare = -3 * part % 128
    spare = spare if spare >= 2 else spare + 128
    extra = jnp.concatenate(
        [attn_gain[:, None], ffn_gain[:, None], jnp.zeros((rows, spare - 2), BF16)], axis=1
    )
    extra = jnp.broadcast_to(extra[None], (4, rows, spare))

    def split_heads(weight):
        return weight.reshape(rows, 4, part).transpose(1, 0, 2)

    def split_units(weight):
        blocks = weight.reshape(rows, 2, halves, 2, 2, 2, units)
        blocks = jnp.pad(blocks, ((0, 0),) * 6 + ((0, padded - units),))
        return blocks.transpose(1, 3, 0, 4, 5, 2, 6).reshape(4, rows, hidden)

    def join_units(blocks):
        blocks = blocks.reshape(2, 2, rows, 2, 2, halves, padded)[..., :units]
        return blocks.transpose(2, 0, 5, 1, 3, 4, 6).reshape(rows, 16 * halves * units)

    HLXC = ("h", "l", "x", "c")
    if halves == 2:
        pair = [lax.ppermute(out_weight, HLXC, head_order(flip)) for flip in (0, 1)]
        out_block = in_order(*pair)
    else:
        out_block = half_gather(lax.ppermute(out_weight, HLXC, head_order(0)))
    other_lengths = lax.ppermute(lengths, "l", [(0, 1), (1, 0)])
    qkv_block = column_block(
        jnp.concatenate(
            [split_heads(w) for w in (query_weight, key_weight, value_weight)] + [extra], axis=2
        ),
    )
    gu_block = column_block(
        jnp.concatenate([split_units(gate_weight), split_units(up_weight)], axis=2)
    )
    down_own = jnp.pad(down_weight, ((0, padded - units), (0, 0)))
    if halves == 2:
        down_other = lax.ppermute(down_own, "h", [(0, 1), (1, 0)])
    gathered = [plane_gather(to_line(inputs[s], rows)) for s in range(count)]
    w_out = line_gather(out_block)
    w_qkv = line_gather(qkv_block)
    w_gu = line_gather(gu_block)
    step = jnp.arange(tokens, dtype=jnp.int32)
    place = jnp.concatenate([y * tokens + step, (1 - y) * tokens + step])
    local_place = place[:tokens]
    cosine, sine = angle_tables(place.astype(F32))
    lengths_two = jnp.stack([lengths, other_lengths], axis=1)

    x_float = [inputs[s].astype(F32) for s in range(count)]
    grad_y = []
    branch2 = []
    for s in range(count):
        live = (local_place < lengths[s]).astype(F32)
        grad_y.append(cotangent[s].astype(F32) * live[:, None])

    pick = (
        lax.broadcasted_iota(jnp.int32, (8, spare), 0)
        == lax.broadcasted_iota(jnp.int32, (8, spare), 1)
    ).astype(BF16)
    gains = dot(pick, w_qkv[:, 3 * part :], NT)
    gain_one_line = gains[0:1]
    gain_one = from_line(gain_one_line, rows)
    gain_two = from_line(gains[1:2], rows)

    kept = []
    mids = []
    normed = []
    for s in range(count):
        whole = gathered[s].astype(F32)
        normed.append((whole * norm_factor(whole) * gain_one_line).astype(BF16))
        visible = (place[None, :] <= place[:, None])[None] & (
            place[None, None, :] < lengths_two[s][:, None, None]
        )
        visible = visible[:, None, :, :]
        lin = after(dot(normed[s], w_qkv), gu_block)
        lin = lin[:, : 3 * part].reshape(2, 2 * tokens, 3, heads, HEAD_DIM)
        queries = rotate(lin[:, :, 0], cosine, sine).astype(BF16)
        keys = rotate(lin[:, :, 1], cosine, sine).astype(BF16)
        values = lin[:, :, 2].astype(BF16)
        scores = einsum("bqhe,bkhe->bhqk", queries, keys) * SCORE_SCALE
        scores = jnp.where(visible, scores, MASK_FILL)
        expo = jnp.exp(scores - jnp.max(scores, axis=-1, keepdims=True))
        probs = expo / jnp.sum(expo, axis=-1, keepdims=True)
        attended = einsum("bhqk,bkhe->bqhe", probs.astype(BF16), values)
        attended = attended.astype(BF16).reshape(4 * tokens, part)
        if s == 0:
            if halves == 2:
                down_block = in_order(down_own, after(down_other, attended))
            else:
                down_block = half_gather(down_own)
            w_down = line_gather(down_block)
        out_sum = dot(attended, w_out)
        out_sum = plane_scatter(out_sum)
        mid = x_float[s] + BRANCH_SCALE * out_sum
        kept.append((queries, keys, values, probs, attended))
        mids.append(mid)

    factor_two = [norm_factor(v) for v in mids]
    own_ffn = [
        to_line((v * f * gain_two).astype(BF16), rows) for v, f in zip(mids, factor_two)
    ]
    normed_ffn = [plane_gather(v) for v in own_ffn]
    for s in range(count):
        branch2.append(plane_gather((BRANCH_SCALE * grad_y[s]).astype(BF16), *own_ffn))
    mixes = []
    acts = []
    for s in range(count):
        both = dot(normed_ffn[s], w_gu)
        gate_pre, up_pre = both[:, :hidden], both[:, hidden:]
        sigmoid = 1.0 / (1.0 + jnp.exp(-gate_pre))
        mixes.append((gate_pre * sigmoid * up_pre).astype(BF16))
        acts.append((gate_pre, up_pre, sigmoid))
    all_mixed = jnp.concatenate(mixes, axis=0)
    all_branch2 = jnp.concatenate(branch2, axis=0)
    down_terms = dot(all_mixed, all_branch2, TN).astype(BF16)
    down_part = line_scatter(down_terms)

    grad_boths = []
    for s in range(count):
        gate_pre, up_pre, sigmoid = acts[s]
        grad_mixed = dot(after(branch2[s], down_terms), w_down, NT)
        grad_gate = grad_mixed * up_pre * (sigmoid + gate_pre * sigmoid * (1.0 - sigmoid))
        grad_up = grad_mixed * gate_pre * sigmoid
        grad_boths.append(jnp.concatenate([grad_gate.astype(BF16), grad_up.astype(BF16)], axis=1))
    norm_terms = [dot(g, w_gu, NT).astype(BF16) for g in grad_boths]
    all_ffn = after(jnp.concatenate(normed_ffn, axis=0), *norm_terms)
    all_boths = jnp.concatenate(grad_boths, axis=0)
    gu_terms = dot(all_ffn, all_boths, TN).astype(BF16)
    gu_part = line_scatter(gu_terms)

    grad_mids = []
    branch1 = []
    own_branch1 = []
    for s in range(count):
        grad_norm = plane_scatter(norm_terms[s])
        grad_norm = from_line(grad_norm, rows) * gain_two
        grad_mid = grad_y[s] + norm_back(mids[s], factor_two[s], grad_norm)
        grad_mids.append(grad_mid)
        own_branch1.append((BRANCH_SCALE * grad_mid).astype(BF16))
        branch1.append(plane_gather(own_branch1[s]))

    outputs = []
    for s in range(count):
        terms = dot(after(mixes[s], gu_terms, *own_branch1), w_down)
        outputs.append((mids[s] + BRANCH_SCALE * plane_scatter(terms)).astype(BF16))

    grad_qkv = []
    input_grads = []
    for s in range(count):
        queries, keys, values, probs, attended = kept[s]
        grad_att = dot(after(branch1[s], down_part), w_out, NT).astype(BF16)
        grad_att = grad_att.reshape(2, 2 * tokens, heads, HEAD_DIM)
        grad_probs = einsum("bqhe,bkhe->bhqk", grad_att, values)
        delta = jnp.sum(probs * grad_probs, axis=-1, keepdims=True)
        grad_scores = (probs * (grad_probs - delta)).astype(BF16)
        grad_q = einsum("bhqk,bkhe->bqhe", grad_scores, keys) * SCORE_SCALE
        grad_k = einsum("bhqk,bqhe->bkhe", grad_scores, queries) * SCORE_SCALE
        grad_v = einsum("bhqk,bqhe->bkhe", probs.astype(BF16), grad_att)
        grads = jnp.stack(
            [
                rotate_back(grad_q, cosine, sine).astype(BF16),
                rotate_back(grad_k, cosine, sine).astype(BF16),
                grad_v.astype(BF16),
            ],
            axis=2,
        ).reshape(4 * tokens, 3 * part)
        grad_qkv.append(jnp.pad(grads, ((0, 0), (0, spare))))
    all_normed = jnp.concatenate(normed, axis=0)
    all_grads = jnp.concatenate(grad_qkv, axis=0)
    v_terms = dot(all_normed, all_grads[:, 2 * part :], TN).astype(BF16)
    v_part = line_scatter(v_terms)
    qk_terms = dot(after(all_normed, v_terms), all_grads[:, : 2 * part], TN).astype(BF16)
    qk_part = line_scatter(qk_terms)
    all_attended = after(jnp.concatenate([k[4] for k in kept], axis=0), qk_terms)
    out_terms = dot(all_attended, jnp.concatenate(branch1, axis=0), TN).astype(BF16)
    out_part = line_scatter(out_terms)
    all_in_terms = [dot(after(g, out_terms), w_qkv, NT).astype(BF16) for g in grad_qkv]
    factor_one = [norm_factor(v) for v in x_float]
    for s in range(count):
        grad_norm = plane_scatter(all_in_terms[s])
        grad_norm = from_line(grad_norm, rows) * gain_one
        input_grads.append(
            (grad_mids[s] + norm_back(x_float[s], factor_one[s], grad_norm)).astype(BF16)
        )

    qk_part = after(qk_part, *input_grads)
    gu_raw = after(column_grad(gu_part, rows, *input_grads), qk_part)
    gate_grad, up_grad = lax.optimization_barrier(
        (join_units(gu_raw[:, :, :hidden]), join_units(gu_raw[:, :, hidden:]))
    )
    out_part = after(out_part, gate_grad, up_grad)
    own = out_part.shape[0] // halves
    if halves == 2:
        h = lax.axis_index("h")
        out_grad = sum(
            lax.ppermute(
                lax.dynamic_slice_in_dim(out_part, (h ^ flip) * own, own),
                HLXC,
                [(b, a) for a, b in head_order(flip)],
            ).astype(F32)
            for flip in (0, 1)
        )
    else:
        out_grad = lax.ppermute(half_scatter(out_part), HLXC, [(b, a) for a, b in head_order(0)])
    v_raw = column_grad(v_part, rows, qk_part)
    qk_raw = column_grad(qk_part, rows, gate_grad, up_grad)
    qkv_raw = jnp.concatenate([qk_raw, v_raw], axis=2)

    gate_grad, up_grad = gate_grad.astype(F32), up_grad.astype(F32)
    ffn_gain_grad = jnp.sum(
        gate_grad * gate_weight.astype(F32) + up_grad * up_weight.astype(F32), axis=1
    ) / ffn_gain.astype(F32)
    qkv_grads = [
        qkv_raw[:, :, i * part : (i + 1) * part].transpose(1, 0, 2).reshape(rows, width).astype(F32)
        for i in range(3)
    ]
    attn_gain_grad = jnp.sum(
        qkv_grads[0] * query_weight.astype(F32)
        + qkv_grads[1] * key_weight.astype(F32)
        + qkv_grads[2] * value_weight.astype(F32),
        axis=1,
    ) / attn_gain.astype(F32)
    return (
        jnp.stack(outputs, axis=0),
        jnp.stack(input_grads, axis=0),
        *qkv_grads,
        out_grad,
        gate_grad,
        up_grad,
        half_scatter(down_part, v_part)[:units],
        attn_gain_grad,
        ffn_gain_grad,
    )


def solution(mesh):
    seq, dp = mesh.devices.shape
    fine = Mesh(mesh.devices.reshape(seq, dp // 8, 2, 2, 2), ("y", "h", "l", "x", "c"))
    owners = ("y", "h", "l", "x", "c")
    acts = P(owners[1:], "y", None)
    weight = P(owners, None)
    gain = P(owners)
    return jax.shard_map(
        body,
        mesh=fine,
        in_specs=(acts, P(owners[1:])) + (weight,) * 7 + (gain, gain, acts),
        out_specs=(acts, acts) + (weight,) * 7 + (gain, gain),
        check_vma=False,
    )
```

```python
import math

import jax
import jax.numpy as jnp
from jax import lax
from jax.sharding import Mesh
from jax.sharding import PartitionSpec as P


HEADS = 36
HEAD_DIM = 64

NORM_EPS = 1e-05
BRANCH_SCALE = 1.4 / math.sqrt(40.0)
SCORE_SCALE = 0.125
MASK_FILL = -1e30

BF16 = jnp.bfloat16
F32 = jnp.float32


PLANE = ("y", "l")
LINE = ("x", "c")
FLIPS = (0, 2, 1, 3)


def dot(left, right, contract=((1,), (0,))):
    return lax.dot_general(left, right, (contract, ((), ())), preferred_element_type=F32)


NT = ((1,), (1,))
TN = ((0,), (0,))


def flip_send(block, flip):
    return lax.ppermute(block, PLANE, [(p, p ^ flip) for p in range(4)])


def plane_gather(block, *late):
    got = [flip_send(block, f) for f in FLIPS[1:]]
    if late:
        got = [after(g, *late) for g in got]
    return lax.optimization_barrier(jnp.concatenate([block] + got, axis=0))


def plane_scatter(partial):
    rows = partial.shape[0] // 4
    total = partial[:rows].astype(F32)
    for k, f in enumerate(FLIPS[1:], 1):
        total = total + flip_send(partial[k * rows : (k + 1) * rows].astype(BF16), f).astype(F32)
    return total


def reorder(blocks):
    pairs = blocks.reshape((2, 2) + blocks.shape[1:])
    pairs = jnp.where(lax.axis_index("y") == 1, pairs[::-1], pairs)
    pairs = jnp.where(lax.axis_index("l") == 1, pairs[:, ::-1], pairs)
    return pairs.reshape(blocks.shape)


def plane_exchange(blocks, *late):
    mine = reorder(blocks)
    got = [mine[0]] + [flip_send(mine[f], f) for f in (1, 2, 3)]
    if late:
        got = [after(g, *late) for g in got]
    return reorder(jnp.stack(got))


def after(value, *others):
    return lax.optimization_barrier((value,) + others)[0]


def line_gather(block):
    return lax.all_gather(block, LINE, axis=0, tiled=True)


def in_order(own, other):
    return jnp.where(
        lax.axis_index("h") == 0,
        jnp.concatenate([own, other], axis=0),
        jnp.concatenate([other, own], axis=0),
    )


def half_gather(block):
    if lax.axis_size("h") == 2:
        other = lax.ppermute(block, "h", [(0, 1), (1, 0)])
        return in_order(block, other)
    return lax.all_gather(block, "h", axis=0, tiled=True)


def line_scatter(partial):
    return lax.psum_scatter(partial, LINE, scatter_dimension=0, tiled=True)


def half_scatter(partial, *late):
    if lax.axis_size("h") == 2:
        rows = partial.shape[0] // 2
        h = lax.axis_index("h")
        other = lax.dynamic_slice_in_dim(partial, (1 - h) * rows, rows)
        own = lax.dynamic_slice_in_dim(partial, h * rows, rows)
        other = lax.ppermute(other, "h", [(0, 1), (1, 0)])
        if late:
            own = after(own, *late)
        return own.astype(F32) + other.astype(F32)
    return lax.psum_scatter(partial, "h", scatter_dimension=0, tiled=True).astype(F32)


def column_block(blocks, *late):
    four, rows, n = blocks.shape
    mine = plane_exchange(blocks, *late)
    return half_gather(mine.reshape(four * rows, n))


def column_grad(scattered, rows, *late):
    mine = half_scatter(scattered, *late).astype(BF16)
    return plane_exchange(mine.reshape(4, rows, mine.shape[1]))


def to_line(tokens, rows):
    count = tokens.shape[0]
    blocks = tokens.reshape(count, 2, -1, 2, 2, 2, rows)
    return blocks.transpose(0, 4, 5, 2, 1, 3, 6).reshape(tokens.shape)


def from_line(tokens, rows):
    count = tokens.shape[0]
    blocks = tokens.reshape(count, 2, 2, -1, 2, 2, rows)
    return blocks.transpose(0, 4, 3, 5, 1, 2, 6).reshape(tokens.shape)


def head_order(flip):
    h = lax.axis_size("h")
    pairs = []
    for hi in range(h):
        for li in range(2):
            for xc in range(4):
                source = li * 4 * h + xc * h + hi
                pairs.append((source, ((hi ^ flip) * 2 + li) * 4 + xc))
    return pairs


def angle_tables(positions):
    inverse = 10000.0 ** (-jnp.arange(32, dtype=F32) / 32.0)
    phase = positions[:, None] * inverse[None, :]
    phase = jnp.concatenate([phase, phase], axis=-1)
    return jnp.cos(phase), jnp.sin(phase)


def rotate(tensor, cosine, sine):
    half = HEAD_DIM // 2
    turned = jnp.concatenate([-tensor[..., half:], tensor[..., :half]], axis=-1)
    return tensor * cosine[:, None, :] + turned * sine[:, None, :]


def rotate_back(grad, cosine, sine):
    half = HEAD_DIM // 2
    scaled = grad * sine[:, None, :]
    turned = jnp.concatenate([scaled[..., half:], -scaled[..., :half]], axis=-1)
    return grad * cosine[:, None, :] + turned


def norm_factor(values):
    return lax.rsqrt(jnp.mean(values * values, axis=-1, keepdims=True) + NORM_EPS)


def norm_back(values, factor, grad):
    mean = jnp.mean(values * grad, axis=-1, keepdims=True)
    return factor * (grad - values * (factor * factor) * mean)


def einsum(spec, left, right):
    return jnp.einsum(spec, left, right, preferred_element_type=F32)


def body(
    inputs,
    lengths,
    query_weight,
    key_weight,
    value_weight,
    out_weight,
    gate_weight,
    up_weight,
    down_weight,
    attn_gain,
    ffn_gain,
    cotangent,
):
    count, tokens, width = inputs.shape
    rows = query_weight.shape[0]
    units = down_weight.shape[0]
    halves = lax.axis_size("h")
    heads = HEADS // 4
    part = heads * HEAD_DIM
    padded = -(-units // 8) * 8
    hidden = padded * 4 * halves
    y = lax.axis_index("y")

    spare = -3 * part % 128
    spare = spare if spare >= 2 else spare + 128
    extra = jnp.concatenate(
        [attn_gain[:, None], ffn_gain[:, None], jnp.zeros((rows, spare - 2), BF16)], axis=1
    )
    extra = jnp.broadcast_to(extra[None], (4, rows, spare))

    def split_heads(weight):
        return weight.reshape(rows, 4, part).transpose(1, 0, 2)

    def split_units(weight):
        blocks = weight.reshape(rows, 2, halves, 2, 2, 2, units)
        blocks = jnp.pad(blocks, ((0, 0),) * 6 + ((0, padded - units),))
        return blocks.transpose(1, 3, 0, 4, 5, 2, 6).reshape(4, rows, hidden)

    def join_units(blocks):
        blocks = blocks.reshape(2, 2, rows, 2, 2, halves, padded)[..., :units]
        return blocks.transpose(2, 0, 5, 1, 3, 4, 6).reshape(rows, 16 * halves * units)

    HLXC = ("h", "l", "x", "c")
    if halves == 2:
        pair = [lax.ppermute(out_weight, HLXC, head_order(flip)) for flip in (0, 1)]
        out_block = in_order(*pair)
    else:
        out_block = half_gather(lax.ppermute(out_weight, HLXC, head_order(0)))
    other_lengths = lax.ppermute(lengths, "l", [(0, 1), (1, 0)])
    down_block = half_gather(jnp.pad(down_weight, ((0, padded - units), (0, 0))))
    gu_columns = jnp.concatenate(
        [split_units(after(gate_weight, out_block)), split_units(after(up_weight, out_block))],
        axis=2,
    )
    qkv_block = column_block(
        jnp.concatenate(
            [split_heads(w) for w in (query_weight, key_weight, value_weight)] + [extra], axis=2
        ),
        gu_columns,
    )
    gu_block = column_block(gu_columns)
    gathered = [plane_gather(to_line(inputs[s], rows)) for s in range(count)]
    w_out = line_gather(out_block)
    first = width // 3
    w_down_a = line_gather(down_block[:, :first])
    w_qkv = line_gather(qkv_block)
    w_gu = line_gather(gu_block)
    w_down_b = line_gather(down_block[:, first:])
    step = jnp.arange(tokens, dtype=jnp.int32)
    place = jnp.concatenate([y * tokens + step, (1 - y) * tokens + step])
    local_place = place[:tokens]
    cosine, sine = angle_tables(place.astype(F32))
    lengths_two = jnp.stack([lengths, other_lengths], axis=1)

    x_float = [inputs[s].astype(F32) for s in range(count)]
    grad_y = []
    branch2 = []
    for s in range(count):
        live = (local_place < lengths[s]).astype(F32)
        grad_y.append(cotangent[s].astype(F32) * live[:, None])

    pick = (
        lax.broadcasted_iota(jnp.int32, (8, spare), 0)
        == lax.broadcasted_iota(jnp.int32, (8, spare), 1)
    ).astype(BF16)
    gains = dot(pick, w_qkv[:, 3 * part :], NT)
    gain_one_line = gains[0:1]
    gain_one = from_line(gain_one_line, rows)
    gain_two = from_line(gains[1:2], rows)

    kept = []
    mids = []
    normed = []
    for s in range(count):
        whole = gathered[s].astype(F32)
        normed.append((whole * norm_factor(whole) * gain_one_line).astype(BF16))
        visible = (place[None, :] <= place[:, None])[None] & (
            place[None, None, :] < lengths_two[s][:, None, None]
        )
        visible = visible[:, None, :, :]
        lin = after(dot(normed[s], w_qkv), gu_block)
        lin = lin[:, : 3 * part].reshape(2, 2 * tokens, 3, heads, HEAD_DIM)
        queries = rotate(lin[:, :, 0], cosine, sine).astype(BF16)
        keys = rotate(lin[:, :, 1], cosine, sine).astype(BF16)
        values = lin[:, :, 2].astype(BF16)
        scores = einsum("bqhe,bkhe->bhqk", queries, keys) * SCORE_SCALE
        scores = jnp.where(visible, scores, MASK_FILL)
        expo = jnp.exp(scores - jnp.max(scores, axis=-1, keepdims=True))
        probs = expo / jnp.sum(expo, axis=-1, keepdims=True)
        attended = einsum("bhqk,bkhe->bqhe", probs.astype(BF16), values)
        attended = attended.astype(BF16).reshape(4 * tokens, part)
        out_sum = dot(attended, w_out)
        out_sum = plane_scatter(out_sum)
        mid = x_float[s] + BRANCH_SCALE * out_sum
        kept.append((queries, keys, values, probs, attended))
        mids.append(mid)

    factor_two = [norm_factor(v) for v in mids]
    own_ffn = [
        to_line((v * f * gain_two).astype(BF16), rows) for v, f in zip(mids, factor_two)
    ]
    normed_ffn = [plane_gather(v) for v in own_ffn]
    for s in range(count):
        branch2.append(plane_gather((BRANCH_SCALE * grad_y[s]).astype(BF16), *own_ffn))
    mixes = []
    acts = []
    for s in range(count):
        both = dot(normed_ffn[s], w_gu)
        gate_pre, up_pre = both[:, :hidden], both[:, hidden:]
        sigmoid = 1.0 / (1.0 + jnp.exp(-gate_pre))
        mixes.append((gate_pre * sigmoid * up_pre).astype(BF16))
        acts.append((gate_pre, up_pre, sigmoid))
    all_mixed = jnp.concatenate(mixes, axis=0)
    all_branch2 = jnp.concatenate(branch2, axis=0)
    down_terms = dot(all_mixed, all_branch2, TN).astype(BF16)
    down_part = line_scatter(down_terms)

    grad_boths = []
    for s in range(count):
        gate_pre, up_pre, sigmoid = acts[s]
        late = after(branch2[s], down_terms)
        grad_mixed = dot(late[:, :first], w_down_a, NT) + dot(late[:, first:], w_down_b, NT)
        grad_gate = grad_mixed * up_pre * (sigmoid + gate_pre * sigmoid * (1.0 - sigmoid))
        grad_up = grad_mixed * gate_pre * sigmoid
        grad_boths.append(jnp.concatenate([grad_gate.astype(BF16), grad_up.astype(BF16)], axis=1))
    norm_terms = [dot(g, w_gu, NT).astype(BF16) for g in grad_boths]
    all_ffn = after(jnp.concatenate(normed_ffn, axis=0), *norm_terms)
    all_boths = jnp.concatenate(grad_boths, axis=0)
    gu_terms = dot(all_ffn, all_boths, TN).astype(BF16)
    gu_part = line_scatter(gu_terms)

    grad_mids = []
    branch1 = []
    own_branch1 = []
    for s in range(count):
        grad_norm = plane_scatter(norm_terms[s])
        grad_norm = from_line(grad_norm, rows) * gain_two
        grad_mid = grad_y[s] + norm_back(mids[s], factor_two[s], grad_norm)
        grad_mids.append(grad_mid)
        own_branch1.append((BRANCH_SCALE * grad_mid).astype(BF16))
        branch1.append(plane_gather(own_branch1[s]))

    grad_qkv = []
    input_grads = []
    for s in range(count):
        queries, keys, values, probs, attended = kept[s]
        grad_att = dot(after(branch1[s], down_part), w_out, NT).astype(BF16)
        grad_att = grad_att.reshape(2, 2 * tokens, heads, HEAD_DIM)
        grad_probs = einsum("bqhe,bkhe->bhqk", grad_att, values)
        delta = jnp.sum(probs * grad_probs, axis=-1, keepdims=True)
        grad_scores = (probs * (grad_probs - delta)).astype(BF16)
        grad_q = einsum("bhqk,bkhe->bqhe", grad_scores, keys) * SCORE_SCALE
        grad_k = einsum("bhqk,bqhe->bkhe", grad_scores, queries) * SCORE_SCALE
        grad_v = einsum("bhqk,bqhe->bkhe", probs.astype(BF16), grad_att)
        grads = jnp.stack(
            [
                rotate_back(grad_q, cosine, sine).astype(BF16),
                rotate_back(grad_k, cosine, sine).astype(BF16),
                grad_v.astype(BF16),
            ],
            axis=2,
        ).reshape(4 * tokens, 3 * part)
        grad_qkv.append(jnp.pad(grads, ((0, 0), (0, spare))))
    all_normed = jnp.concatenate(normed, axis=0)
    all_grads = jnp.concatenate(grad_qkv, axis=0)
    v_terms = dot(all_normed, all_grads[:, 2 * part :], TN).astype(BF16)
    v_part = line_scatter(v_terms)
    qk_terms = dot(after(all_normed, v_terms), all_grads[:, : 2 * part], TN).astype(BF16)
    qk_part = line_scatter(qk_terms)
    all_attended = after(jnp.concatenate([k[4] for k in kept], axis=0), qk_terms, gu_part)
    out_terms = dot(all_attended, jnp.concatenate(branch1, axis=0), TN).astype(BF16)
    out_part = line_scatter(out_terms)
    outputs = []
    for s in range(count):
        late = after(mixes[s], out_terms)
        terms = jnp.concatenate(
            [dot(late, w_down_a).astype(BF16), dot(late, w_down_b).astype(BF16)], axis=1
        )
        outputs.append((mids[s] + BRANCH_SCALE * plane_scatter(terms)).astype(BF16))

    all_in_terms = [dot(after(g, out_terms), w_qkv, NT).astype(BF16) for g in grad_qkv]
    factor_one = [norm_factor(v) for v in x_float]
    for s in range(count):
        grad_norm = plane_scatter(all_in_terms[s])
        grad_norm = from_line(grad_norm, rows) * gain_one
        input_grads.append(
            (grad_mids[s] + norm_back(x_float[s], factor_one[s], grad_norm)).astype(BF16)
        )

    qk_part = after(qk_part, *input_grads)
    gu_raw = after(column_grad(gu_part, rows, *input_grads), qk_part)
    gate_grad, up_grad = lax.optimization_barrier(
        (join_units(gu_raw[:, :, :hidden]), join_units(gu_raw[:, :, hidden:]))
    )
    out_part = after(out_part, gate_grad, up_grad)
    own = out_part.shape[0] // halves
    if halves == 2:
        h = lax.axis_index("h")
        out_grad = sum(
            lax.ppermute(
                lax.dynamic_slice_in_dim(out_part, (h ^ flip) * own, own),
                HLXC,
                [(b, a) for a, b in head_order(flip)],
            ).astype(F32)
            for flip in (0, 1)
        )
    else:
        out_grad = lax.ppermute(half_scatter(out_part), HLXC, [(b, a) for a, b in head_order(0)])
    v_raw = column_grad(v_part, rows, qk_part)
    qk_raw = column_grad(qk_part, rows, gate_grad, up_grad)
    qkv_raw = jnp.concatenate([qk_raw, v_raw], axis=2)

    gate_grad, up_grad = gate_grad.astype(F32), up_grad.astype(F32)
    ffn_gain_grad = jnp.sum(
        gate_grad * gate_weight.astype(F32) + up_grad * up_weight.astype(F32), axis=1
    ) / ffn_gain.astype(F32)
    qkv_grads = [
        qkv_raw[:, :, i * part : (i + 1) * part].transpose(1, 0, 2).reshape(rows, width).astype(F32)
        for i in range(3)
    ]
    attn_gain_grad = jnp.sum(
        qkv_grads[0] * query_weight.astype(F32)
        + qkv_grads[1] * key_weight.astype(F32)
        + qkv_grads[2] * value_weight.astype(F32),
        axis=1,
    ) / attn_gain.astype(F32)
    return (
        jnp.stack(outputs, axis=0),
        jnp.stack(input_grads, axis=0),
        *qkv_grads,
        out_grad,
        gate_grad,
        up_grad,
        half_scatter(down_part, v_part)[:units],
        attn_gain_grad,
        ffn_gain_grad,
    )


def solution(mesh):
    seq, dp = mesh.devices.shape
    fine = Mesh(mesh.devices.reshape(seq, dp // 8, 2, 2, 2), ("y", "h", "l", "x", "c"))
    owners = ("y", "h", "l", "x", "c")
    acts = P(owners[1:], "y", None)
    weight = P(owners, None)
    gain = P(owners)
    return jax.shard_map(
        body,
        mesh=fine,
        in_specs=(acts, P(owners[1:])) + (weight,) * 7 + (gain, gain, acts),
        out_specs=(acts, acts) + (weight,) * 7 + (gain, gain),
        check_vma=False,
    )
```

```python
import math

import jax
import jax.numpy as jnp
from jax import lax
from jax.sharding import Mesh
from jax.sharding import PartitionSpec as P


HEADS = 36
HEAD_DIM = 64

NORM_EPS = 1e-05
BRANCH_SCALE = 1.4 / math.sqrt(40.0)
SCORE_SCALE = 0.125
MASK_FILL = -1e30

BF16 = jnp.bfloat16
F32 = jnp.float32


PLANE = ("y", "l")
LINE = ("x", "c")
FLIPS = (0, 2, 1, 3)


def dot(left, right, contract=((1,), (0,))):
    return lax.dot_general(left, right, (contract, ((), ())), preferred_element_type=F32)


NT = ((1,), (1,))
TN = ((0,), (0,))


def flip_send(block, flip):
    return lax.ppermute(block, PLANE, [(p, p ^ flip) for p in range(4)])


def plane_gather(block, *late):
    got = [flip_send(block, f) for f in FLIPS[1:]]
    if late:
        got = [after(g, *late) for g in got]
    return lax.optimization_barrier(jnp.concatenate([block] + got, axis=0))


def plane_scatter(partial):
    rows = partial.shape[0] // 4
    total = partial[:rows].astype(F32)
    for k, f in enumerate(FLIPS[1:], 1):
        total = total + flip_send(partial[k * rows : (k + 1) * rows].astype(BF16), f).astype(F32)
    return total


def reorder(blocks):
    pairs = blocks.reshape((2, 2) + blocks.shape[1:])
    pairs = jnp.where(lax.axis_index("y") == 1, pairs[::-1], pairs)
    pairs = jnp.where(lax.axis_index("l") == 1, pairs[:, ::-1], pairs)
    return pairs.reshape(blocks.shape)


def plane_exchange(blocks):
    mine = reorder(blocks)
    got = [mine[0]] + [flip_send(mine[f], f) for f in (1, 2, 3)]
    return reorder(jnp.stack(got))


def after(value, *others):
    return lax.optimization_barrier((value,) + others)[0]


def line_gather(block):
    return lax.all_gather(block, LINE, axis=0, tiled=True)


def in_order(own, other):
    return jnp.where(
        lax.axis_index("h") == 0,
        jnp.concatenate([own, other], axis=0),
        jnp.concatenate([other, own], axis=0),
    )


def half_gather(block):
    if lax.axis_size("h") == 2:
        other = lax.ppermute(block, "h", [(0, 1), (1, 0)])
        return in_order(block, other)
    return lax.all_gather(block, "h", axis=0, tiled=True)


def line_scatter(partial):
    return lax.psum_scatter(partial, LINE, scatter_dimension=0, tiled=True)


def half_scatter(partial, *late):
    if lax.axis_size("h") == 2:
        rows = partial.shape[0] // 2
        h = lax.axis_index("h")
        other = lax.dynamic_slice_in_dim(partial, (1 - h) * rows, rows)
        own = lax.dynamic_slice_in_dim(partial, h * rows, rows)
        other = lax.ppermute(other, "h", [(0, 1), (1, 0)])
        if late:
            own = after(own, *late)
        return own.astype(F32) + other.astype(F32)
    return lax.psum_scatter(partial, "h", scatter_dimension=0, tiled=True).astype(F32)


def column_block(blocks):
    four, rows, n = blocks.shape
    mine = plane_exchange(blocks)
    return half_gather(mine.reshape(four * rows, n))


def column_grad(scattered, rows, *late):
    mine = half_scatter(scattered, *late).astype(BF16)
    return plane_exchange(mine.reshape(4, rows, mine.shape[1]))


def to_line(tokens, rows):
    count = tokens.shape[0]
    blocks = tokens.reshape(count, 2, -1, 2, 2, 2, rows)
    return blocks.transpose(0, 4, 5, 2, 1, 3, 6).reshape(tokens.shape)


def from_line(tokens, rows):
    count = tokens.shape[0]
    blocks = tokens.reshape(count, 2, 2, -1, 2, 2, rows)
    return blocks.transpose(0, 4, 3, 5, 1, 2, 6).reshape(tokens.shape)


def head_order(flip):
    h = lax.axis_size("h")
    pairs = []
    for hi in range(h):
        for li in range(2):
            for xc in range(4):
                source = li * 4 * h + xc * h + hi
                pairs.append((source, ((hi ^ flip) * 2 + li) * 4 + xc))
    return pairs


def angle_tables(positions):
    inverse = 10000.0 ** (-jnp.arange(32, dtype=F32) / 32.0)
    phase = positions[:, None] * inverse[None, :]
    phase = jnp.concatenate([phase, phase], axis=-1)
    return jnp.cos(phase), jnp.sin(phase)


def rotate(tensor, cosine, sine):
    half = HEAD_DIM // 2
    turned = jnp.concatenate([-tensor[..., half:], tensor[..., :half]], axis=-1)
    return tensor * cosine[:, None, :] + turned * sine[:, None, :]


def rotate_back(grad, cosine, sine):
    half = HEAD_DIM // 2
    scaled = grad * sine[:, None, :]
    turned = jnp.concatenate([scaled[..., half:], -scaled[..., :half]], axis=-1)
    return grad * cosine[:, None, :] + turned


def norm_factor(values):
    return lax.rsqrt(jnp.mean(values * values, axis=-1, keepdims=True) + NORM_EPS)


def norm_back(values, factor, grad):
    mean = jnp.mean(values * grad, axis=-1, keepdims=True)
    return factor * (grad - values * (factor * factor) * mean)


def einsum(spec, left, right):
    return jnp.einsum(spec, left, right, preferred_element_type=F32)


def body(
    inputs,
    lengths,
    query_weight,
    key_weight,
    value_weight,
    out_weight,
    gate_weight,
    up_weight,
    down_weight,
    attn_gain,
    ffn_gain,
    cotangent,
):
    count, tokens, width = inputs.shape
    rows = query_weight.shape[0]
    units = down_weight.shape[0]
    halves = lax.axis_size("h")
    heads = HEADS // 4
    part = heads * HEAD_DIM
    padded = -(-units // 8) * 8
    hidden = padded * 4 * halves
    y = lax.axis_index("y")

    spare = -3 * part % 128
    spare = spare if spare >= 2 else spare + 128
    extra = jnp.concatenate(
        [attn_gain[:, None], ffn_gain[:, None], jnp.zeros((rows, spare - 2), BF16)], axis=1
    )
    extra = jnp.broadcast_to(extra[None], (4, rows, spare))

    def split_heads(weight):
        return weight.reshape(rows, 4, part).transpose(1, 0, 2)

    def split_units(weight):
        blocks = weight.reshape(rows, 2, halves, 2, 2, 2, units)
        blocks = jnp.pad(blocks, ((0, 0),) * 6 + ((0, padded - units),))
        return blocks.transpose(1, 3, 0, 4, 5, 2, 6).reshape(4, rows, hidden)

    def join_units(blocks):
        blocks = blocks.reshape(2, 2, rows, 2, 2, halves, padded)[..., :units]
        return blocks.transpose(2, 0, 5, 1, 3, 4, 6).reshape(rows, 16 * halves * units)

    HLXC = ("h", "l", "x", "c")
    if halves == 2:
        pair = [lax.ppermute(out_weight, HLXC, head_order(flip)) for flip in (0, 1)]
        out_block = in_order(*pair)
    else:
        out_block = half_gather(lax.ppermute(out_weight, HLXC, head_order(0)))
    other_lengths = lax.ppermute(lengths, "l", [(0, 1), (1, 0)])
    qkv_block = column_block(
        jnp.concatenate(
            [split_heads(w) for w in (query_weight, key_weight, value_weight)] + [extra], axis=2
        ),
    )
    gu_block = column_block(
        jnp.concatenate([split_units(gate_weight), split_units(up_weight)], axis=2)
    )
    down_own = jnp.pad(down_weight, ((0, padded - units), (0, 0)))
    if halves == 2:
        down_other = lax.ppermute(down_own, "h", [(0, 1), (1, 0)])
    gathered = [plane_gather(to_line(inputs[s], rows)) for s in range(count)]
    w_out = line_gather(out_block)
    w_qkv = line_gather(qkv_block)
    w_gu = line_gather(gu_block)
    step = jnp.arange(tokens, dtype=jnp.int32)
    place = jnp.concatenate([y * tokens + step, (1 - y) * tokens + step])
    local_place = place[:tokens]
    cosine, sine = angle_tables(place.astype(F32))
    lengths_two = jnp.stack([lengths, other_lengths], axis=1)

    x_float = [inputs[s].astype(F32) for s in range(count)]
    grad_y = []
    branch2 = []
    for s in range(count):
        live = (local_place < lengths[s]).astype(F32)
        grad_y.append(cotangent[s].astype(F32) * live[:, None])

    pick = (
        lax.broadcasted_iota(jnp.int32, (8, spare), 0)
        == lax.broadcasted_iota(jnp.int32, (8, spare), 1)
    ).astype(BF16)
    gains = dot(pick, w_qkv[:, 3 * part :], NT)
    gain_one_line = gains[0:1]
    gain_one = from_line(gain_one_line, rows)
    gain_two = from_line(gains[1:2], rows)

    kept = []
    mids = []
    normed = []
    for s in range(count):
        whole = gathered[s].astype(F32)
        normed.append((whole * norm_factor(whole) * gain_one_line).astype(BF16))
        visible = (place[None, :] <= place[:, None])[None] & (
            place[None, None, :] < lengths_two[s][:, None, None]
        )
        visible = visible[:, None, :, :]
        lin = after(dot(normed[s], w_qkv), gu_block)
        lin = lin[:, : 3 * part].reshape(2, 2 * tokens, 3, heads, HEAD_DIM)
        queries = rotate(lin[:, :, 0], cosine, sine).astype(BF16)
        keys = rotate(lin[:, :, 1], cosine, sine).astype(BF16)
        values = lin[:, :, 2].astype(BF16)
        scores = einsum("bqhe,bkhe->bhqk", queries, keys) * SCORE_SCALE
        scores = jnp.where(visible, scores, MASK_FILL)
        expo = jnp.exp(scores - jnp.max(scores, axis=-1, keepdims=True))
        probs = expo / jnp.sum(expo, axis=-1, keepdims=True)
        attended = einsum("bhqk,bkhe->bqhe", probs.astype(BF16), values)
        attended = attended.astype(BF16).reshape(4 * tokens, part)
        if s == 0:
            if halves == 2:
                down_block = in_order(down_own, after(down_other, attended))
            else:
                down_block = half_gather(down_own)
            w_down = line_gather(down_block)
        out_sum = dot(attended, w_out)
        out_sum = plane_scatter(out_sum)
        mid = x_float[s] + BRANCH_SCALE * out_sum
        kept.append((queries, keys, values, probs, attended))
        mids.append(mid)

    factor_two = [norm_factor(v) for v in mids]
    own_ffn = [
        to_line((v * f * gain_two).astype(BF16), rows) for v, f in zip(mids, factor_two)
    ]
    normed_ffn = [plane_gather(v) for v in own_ffn]
    for s in range(count):
        branch2.append(plane_gather((BRANCH_SCALE * grad_y[s]).astype(BF16), *own_ffn))
    mixes = []
    acts = []
    for s in range(count):
        both = dot(normed_ffn[s], w_gu)
        gate_pre, up_pre = both[:, :hidden], both[:, hidden:]
        sigmoid = 1.0 / (1.0 + jnp.exp(-gate_pre))
        mixes.append((gate_pre * sigmoid * up_pre).astype(BF16))
        acts.append((gate_pre, up_pre, sigmoid))
    all_mixed = jnp.concatenate(mixes, axis=0)
    all_branch2 = jnp.concatenate(branch2, axis=0)
    down_terms = dot(all_mixed, all_branch2, TN).astype(BF16)
    down_part = line_scatter(down_terms)

    grad_boths = []
    for s in range(count):
        gate_pre, up_pre, sigmoid = acts[s]
        grad_mixed = dot(after(branch2[s], down_terms), w_down, NT)
        grad_gate = grad_mixed * up_pre * (sigmoid + gate_pre * sigmoid * (1.0 - sigmoid))
        grad_up = grad_mixed * gate_pre * sigmoid
        grad_boths.append(jnp.concatenate([grad_gate.astype(BF16), grad_up.astype(BF16)], axis=1))
    norm_terms = [dot(g, w_gu, NT).astype(BF16) for g in grad_boths]
    all_ffn = after(jnp.concatenate(normed_ffn, axis=0), *norm_terms)
    all_boths = jnp.concatenate(grad_boths, axis=0)
    gu_terms = dot(all_ffn, all_boths, TN).astype(BF16)
    gu_part = line_scatter(gu_terms)

    grad_mids = []
    branch1 = []
    own_branch1 = []
    for s in range(count):
        grad_norm = plane_scatter(norm_terms[s])
        grad_norm = from_line(grad_norm, rows) * gain_two
        grad_mid = grad_y[s] + norm_back(mids[s], factor_two[s], grad_norm)
        grad_mids.append(grad_mid)
        own_branch1.append((BRANCH_SCALE * grad_mid).astype(BF16))
        branch1.append(plane_gather(own_branch1[s]))

    outputs = []
    for s in range(count):
        terms = dot(after(mixes[s], gu_terms, *own_branch1), w_down)
        outputs.append((mids[s] + BRANCH_SCALE * plane_scatter(terms)).astype(BF16))

    grad_qkv = []
    input_grads = []
    for s in range(count):
        queries, keys, values, probs, attended = kept[s]
        grad_att = dot(after(branch1[s], down_part), w_out, NT).astype(BF16)
        grad_att = grad_att.reshape(2, 2 * tokens, heads, HEAD_DIM)
        grad_probs = einsum("bqhe,bkhe->bhqk", grad_att, values)
        delta = jnp.sum(probs * grad_probs, axis=-1, keepdims=True)
        grad_scores = (probs * (grad_probs - delta)).astype(BF16)
        grad_q = einsum("bhqk,bkhe->bqhe", grad_scores, keys) * SCORE_SCALE
        grad_k = einsum("bhqk,bqhe->bkhe", grad_scores, queries) * SCORE_SCALE
        grad_v = einsum("bhqk,bqhe->bkhe", probs.astype(BF16), grad_att)
        grads = jnp.stack(
            [
                rotate_back(grad_q, cosine, sine).astype(BF16),
                rotate_back(grad_k, cosine, sine).astype(BF16),
                grad_v.astype(BF16),
            ],
            axis=2,
        ).reshape(4 * tokens, 3 * part)
        grad_qkv.append(jnp.pad(grads, ((0, 0), (0, spare))))
    all_normed = jnp.concatenate(normed, axis=0)
    all_grads = jnp.concatenate(grad_qkv, axis=0)
    qkv_terms = dot(all_normed, all_grads, TN).astype(BF16)
    qkv_part = line_scatter(qkv_terms)
    all_attended = after(jnp.concatenate([k[4] for k in kept], axis=0), qkv_terms, gu_part)
    out_terms = dot(all_attended, jnp.concatenate(branch1, axis=0), TN).astype(BF16)
    out_part = line_scatter(out_terms)
    all_in_terms = [dot(after(g, out_terms), w_qkv, NT).astype(BF16) for g in grad_qkv]
    factor_one = [norm_factor(v) for v in x_float]
    for s in range(count):
        grad_norm = plane_scatter(all_in_terms[s])
        grad_norm = from_line(grad_norm, rows) * gain_one
        input_grads.append(
            (grad_mids[s] + norm_back(x_float[s], factor_one[s], grad_norm)).astype(BF16)
        )

    qkv_part = after(qkv_part, *input_grads)
    gu_raw = after(column_grad(gu_part, rows, *input_grads), qkv_part)
    gate_grad, up_grad = lax.optimization_barrier(
        (join_units(gu_raw[:, :, :hidden]), join_units(gu_raw[:, :, hidden:]))
    )
    out_part = after(out_part, gate_grad, up_grad)
    own = out_part.shape[0] // halves
    if halves == 2:
        h = lax.axis_index("h")
        out_grad = sum(
            lax.ppermute(
                lax.dynamic_slice_in_dim(out_part, (h ^ flip) * own, own),
                HLXC,
                [(b, a) for a, b in head_order(flip)],
            ).astype(F32)
            for flip in (0, 1)
        )
    else:
        out_grad = lax.ppermute(half_scatter(out_part), HLXC, [(b, a) for a, b in head_order(0)])
    qkv_raw = column_grad(qkv_part, rows, gate_grad, up_grad)

    gate_grad, up_grad = gate_grad.astype(F32), up_grad.astype(F32)
    ffn_gain_grad = jnp.sum(
        gate_grad * gate_weight.astype(F32) + up_grad * up_weight.astype(F32), axis=1
    ) / ffn_gain.astype(F32)
    qkv_grads = [
        qkv_raw[:, :, i * part : (i + 1) * part].transpose(1, 0, 2).reshape(rows, width).astype(F32)
        for i in range(3)
    ]
    attn_gain_grad = jnp.sum(
        qkv_grads[0] * query_weight.astype(F32)
        + qkv_grads[1] * key_weight.astype(F32)
        + qkv_grads[2] * value_weight.astype(F32),
        axis=1,
    ) / attn_gain.astype(F32)
    return (
        jnp.stack(outputs, axis=0),
        jnp.stack(input_grads, axis=0),
        *qkv_grads,
        out_grad,
        gate_grad,
        up_grad,
        half_scatter(down_part, qkv_part)[:units],
        attn_gain_grad,
        ffn_gain_grad,
    )


def solution(mesh):
    seq, dp = mesh.devices.shape
    fine = Mesh(mesh.devices.reshape(seq, dp // 8, 2, 2, 2), ("y", "h", "l", "x", "c"))
    owners = ("y", "h", "l", "x", "c")
    acts = P(owners[1:], "y", None)
    weight = P(owners, None)
    gain = P(owners)
    return jax.shard_map(
        body,
        mesh=fine,
        in_specs=(acts, P(owners[1:])) + (weight,) * 7 + (gain, gain, acts),
        out_specs=(acts, acts) + (weight,) * 7 + (gain, gain),
        check_vma=False,
    )
```

```python
import math

import jax
import jax.numpy as jnp
from jax import lax
from jax.sharding import Mesh
from jax.sharding import PartitionSpec as P


HEADS = 36
HEAD_DIM = 64

NORM_EPS = 1e-05
BRANCH_SCALE = 1.4 / math.sqrt(40.0)
SCORE_SCALE = 0.125
MASK_FILL = -1e30

BF16 = jnp.bfloat16
F32 = jnp.float32


PLANE = ("y", "l")
LINE = ("x", "c")
FLIPS = (0, 2, 1, 3)


def dot(left, right, contract=((1,), (0,))):
    return lax.dot_general(left, right, (contract, ((), ())), preferred_element_type=F32)


NT = ((1,), (1,))
TN = ((0,), (0,))


def flip_send(block, flip):
    return lax.ppermute(block, PLANE, [(p, p ^ flip) for p in range(4)])


def plane_gather(block, *late):
    got = [flip_send(block, f) for f in FLIPS[1:]]
    if late:
        got = [after(g, *late) for g in got]
    return lax.optimization_barrier(jnp.concatenate([block] + got, axis=0))


def plane_scatter(partial, *late):
    rows = partial.shape[0] // 4
    total = partial[:rows].astype(F32)
    for k, f in enumerate(FLIPS[1:], 1):
        got = flip_send(partial[k * rows : (k + 1) * rows].astype(BF16), f)
        if late:
            got = after(got, *late)
        total = total + got.astype(F32)
    return total


def reorder(blocks):
    pairs = blocks.reshape((2, 2) + blocks.shape[1:])
    pairs = jnp.where(lax.axis_index("y") == 1, pairs[::-1], pairs)
    pairs = jnp.where(lax.axis_index("l") == 1, pairs[:, ::-1], pairs)
    return pairs.reshape(blocks.shape)


def plane_exchange(blocks):
    mine = reorder(blocks)
    got = [mine[0]] + [flip_send(mine[f], f) for f in (1, 2, 3)]
    return reorder(jnp.stack(got))


def after(value, *others):
    return lax.optimization_barrier((value,) + others)[0]


def line_gather(block):
    return lax.all_gather(block, LINE, axis=0, tiled=True)


def in_order(own, other):
    return jnp.where(
        lax.axis_index("h") == 0,
        jnp.concatenate([own, other], axis=0),
        jnp.concatenate([other, own], axis=0),
    )


def half_gather(block):
    if lax.axis_size("h") == 2:
        other = lax.ppermute(block, "h", [(0, 1), (1, 0)])
        return in_order(block, other)
    return lax.all_gather(block, "h", axis=0, tiled=True)


def line_scatter(partial):
    return lax.psum_scatter(partial, LINE, scatter_dimension=0, tiled=True)


def half_scatter(partial, kind, *late):
    if lax.axis_size("h") == 2:
        rows = partial.shape[0] // 2
        h = lax.axis_index("h")
        other = lax.dynamic_slice_in_dim(partial, (1 - h) * rows, rows)
        own = lax.dynamic_slice_in_dim(partial, h * rows, rows)
        other = lax.ppermute(other, "h", [(0, 1), (1, 0)])
        if late:
            own = after(own, *late)
        return (own.astype(F32) + other.astype(F32)).astype(kind)
    return lax.psum_scatter(partial, "h", scatter_dimension=0, tiled=True).astype(kind)


def column_block(blocks):
    four, rows, n = blocks.shape
    mine = plane_exchange(blocks)
    return half_gather(mine.reshape(four * rows, n))


def to_line(tokens, rows):
    count = tokens.shape[0]
    blocks = tokens.reshape(count, 2, -1, 2, 2, 2, rows)
    return blocks.transpose(0, 4, 5, 2, 1, 3, 6).reshape(tokens.shape)


def from_line(tokens, rows):
    count = tokens.shape[0]
    blocks = tokens.reshape(count, 2, 2, -1, 2, 2, rows)
    return blocks.transpose(0, 4, 3, 5, 1, 2, 6).reshape(tokens.shape)


def head_order(flip):
    h = lax.axis_size("h")
    pairs = []
    for hi in range(h):
        for li in range(2):
            for xc in range(4):
                source = li * 4 * h + xc * h + hi
                pairs.append((source, ((hi ^ flip) * 2 + li) * 4 + xc))
    return pairs


def angle_tables(positions):
    inverse = 10000.0 ** (-jnp.arange(32, dtype=F32) / 32.0)
    phase = positions[:, None] * inverse[None, :]
    phase = jnp.concatenate([phase, phase], axis=-1)
    return jnp.cos(phase), jnp.sin(phase)


def rotate(tensor, cosine, sine):
    half = HEAD_DIM // 2
    turned = jnp.concatenate([-tensor[..., half:], tensor[..., :half]], axis=-1)
    return tensor * cosine[:, None, :] + turned * sine[:, None, :]


def rotate_back(grad, cosine, sine):
    half = HEAD_DIM // 2
    scaled = grad * sine[:, None, :]
    turned = jnp.concatenate([scaled[..., half:], -scaled[..., :half]], axis=-1)
    return grad * cosine[:, None, :] + turned


def norm_factor(values):
    return lax.rsqrt(jnp.mean(values * values, axis=-1, keepdims=True) + NORM_EPS)


def norm_back(values, factor, grad):
    mean = jnp.mean(values * grad, axis=-1, keepdims=True)
    return factor * (grad - values * (factor * factor) * mean)


def einsum(spec, left, right):
    return jnp.einsum(spec, left, right, preferred_element_type=F32)


def body(
    inputs,
    lengths,
    query_weight,
    key_weight,
    value_weight,
    out_weight,
    gate_weight,
    up_weight,
    down_weight,
    attn_gain,
    ffn_gain,
    cotangent,
):
    count, tokens, width = inputs.shape
    rows = query_weight.shape[0]
    units = down_weight.shape[0]
    halves = lax.axis_size("h")
    heads = HEADS // 4
    part = heads * HEAD_DIM
    padded = -(-units // 8) * 8
    hidden = padded * 4 * halves
    y = lax.axis_index("y")

    spare = -3 * part % 128
    spare = spare if spare >= 2 else spare + 128
    extra = jnp.concatenate(
        [attn_gain[:, None], ffn_gain[:, None], jnp.zeros((rows, spare - 2), BF16)], axis=1
    )
    extra = jnp.broadcast_to(extra[None], (4, rows, spare))

    def split_heads(weight):
        return weight.reshape(rows, 4, part).transpose(1, 0, 2)

    def split_units(weight):
        blocks = weight.reshape(rows, 2, halves, 2, 2, 2, units)
        blocks = jnp.pad(blocks, ((0, 0),) * 6 + ((0, padded - units),))
        return blocks.transpose(1, 3, 0, 4, 5, 2, 6).reshape(4, rows, hidden)

    def join_units(blocks):
        blocks = blocks.reshape(2, 2, rows, 2, 2, halves, padded)[..., :units]
        return blocks.transpose(2, 0, 5, 1, 3, 4, 6).reshape(rows, 16 * halves * units)

    HLXC = ("h", "l", "x", "c")
    if halves == 2:
        pair = [lax.ppermute(out_weight, HLXC, head_order(flip)) for flip in (0, 1)]
        out_block = in_order(*pair)
    else:
        out_block = half_gather(lax.ppermute(out_weight, HLXC, head_order(0)))
    other_lengths = lax.ppermute(lengths, "l", [(0, 1), (1, 0)])
    qkv_block = column_block(
        jnp.concatenate(
            [split_heads(w) for w in (query_weight, key_weight, value_weight)] + [extra], axis=2
        ),
    )
    gu_block = column_block(
        jnp.concatenate([split_units(gate_weight), split_units(up_weight)], axis=2)
    )
    down_own = jnp.pad(down_weight, ((0, padded - units), (0, 0)))
    if halves == 2:
        down_other = lax.ppermute(down_own, "h", [(0, 1), (1, 0)])
    gathered = [plane_gather(to_line(inputs[s], rows)) for s in range(count)]
    w_out = line_gather(out_block)
    w_qkv = line_gather(qkv_block)
    w_gu = line_gather(gu_block)
    step = jnp.arange(tokens, dtype=jnp.int32)
    place = jnp.concatenate([y * tokens + step, (1 - y) * tokens + step])
    local_place = place[:tokens]
    cosine, sine = angle_tables(place.astype(F32))
    lengths_two = jnp.stack([lengths, other_lengths], axis=1)

    x_float = [inputs[s].astype(F32) for s in range(count)]
    grad_y = []
    branch2 = []
    for s in range(count):
        live = (local_place < lengths[s]).astype(F32)
        grad_y.append(cotangent[s].astype(F32) * live[:, None])

    pick = (
        lax.broadcasted_iota(jnp.int32, (8, spare), 0)
        == lax.broadcasted_iota(jnp.int32, (8, spare), 1)
    ).astype(BF16)
    gains = dot(pick, w_qkv[:, 3 * part :], NT)
    gain_one_line = gains[0:1]
    gain_one = from_line(gain_one_line, rows)
    gain_two = from_line(gains[1:2], rows)

    kept = []
    mids = []
    normed = []
    for s in range(count):
        whole = gathered[s].astype(F32)
        normed.append((whole * norm_factor(whole) * gain_one_line).astype(BF16))
        visible = (place[None, :] <= place[:, None])[None] & (
            place[None, None, :] < lengths_two[s][:, None, None]
        )
        visible = visible[:, None, :, :]
        lin = after(dot(normed[s], w_qkv), gu_block)
        lin = lin[:, : 3 * part].reshape(2, 2 * tokens, 3, heads, HEAD_DIM)
        queries = rotate(lin[:, :, 0], cosine, sine).astype(BF16)
        keys = rotate(lin[:, :, 1], cosine, sine).astype(BF16)
        values = lin[:, :, 2].astype(BF16)
        scores = einsum("bqhe,bkhe->bhqk", queries, keys) * SCORE_SCALE
        scores = jnp.where(visible, scores, MASK_FILL)
        expo = jnp.exp(scores - jnp.max(scores, axis=-1, keepdims=True))
        probs = expo / jnp.sum(expo, axis=-1, keepdims=True)
        attended = einsum("bhqk,bkhe->bqhe", probs.astype(BF16), values)
        attended = attended.astype(BF16).reshape(4 * tokens, part)
        if s == 0:
            if halves == 2:
                down_block = in_order(down_own, after(down_other, attended))
            else:
                down_block = half_gather(down_own)
            w_down = line_gather(down_block)
        out_sum = dot(attended, w_out)
        out_sum = plane_scatter(out_sum)
        mid = x_float[s] + BRANCH_SCALE * out_sum
        kept.append((queries, keys, values, probs, attended))
        mids.append(mid)

    factor_two = [norm_factor(v) for v in mids]
    own_ffn = [
        to_line((v * f * gain_two).astype(BF16), rows) for v, f in zip(mids, factor_two)
    ]
    normed_ffn = [plane_gather(v) for v in own_ffn]
    for s in range(count):
        branch2.append(plane_gather((BRANCH_SCALE * grad_y[s]).astype(BF16), *own_ffn))
    mixes = []
    acts = []
    for s in range(count):
        both = dot(normed_ffn[s], w_gu)
        gate_pre, up_pre = both[:, :hidden], both[:, hidden:]
        sigmoid = 1.0 / (1.0 + jnp.exp(-gate_pre))
        mixes.append((gate_pre * sigmoid * up_pre).astype(BF16))
        acts.append((gate_pre, up_pre, sigmoid))
    all_mixed = jnp.concatenate(mixes, axis=0)
    all_branch2 = jnp.concatenate(branch2, axis=0)
    down_terms = dot(all_mixed, all_branch2, TN).astype(BF16)
    down_part = line_scatter(down_terms)

    grad_boths = []
    for s in range(count):
        gate_pre, up_pre, sigmoid = acts[s]
        grad_mixed = dot(after(branch2[s], down_terms), w_down, NT)
        grad_gate = grad_mixed * up_pre * (sigmoid + gate_pre * sigmoid * (1.0 - sigmoid))
        grad_up = grad_mixed * gate_pre * sigmoid
        grad_boths.append(jnp.concatenate([grad_gate.astype(BF16), grad_up.astype(BF16)], axis=1))
    norm_terms = [dot(g, w_gu, NT).astype(BF16) for g in grad_boths]
    all_ffn = after(jnp.concatenate(normed_ffn, axis=0), *norm_terms)
    all_boths = jnp.concatenate(grad_boths, axis=0)
    gu_terms = dot(all_ffn, all_boths, TN).astype(BF16)
    gu_part = line_scatter(gu_terms)

    grad_mids = []
    branch1 = []
    own_branch1 = []
    for s in range(count):
        grad_norm = plane_scatter(norm_terms[s])
        grad_norm = from_line(grad_norm, rows) * gain_two
        grad_mid = grad_y[s] + norm_back(mids[s], factor_two[s], grad_norm)
        grad_mids.append(grad_mid)
        own_branch1.append((BRANCH_SCALE * grad_mid).astype(BF16))
        branch1.append(plane_gather(own_branch1[s]))

    y_terms = [dot(after(mixes[s], gu_terms, *own_branch1), w_down).astype(BF16) for s in range(count)]

    grad_qkv = []
    input_grads = []
    for s in range(count):
        queries, keys, values, probs, attended = kept[s]
        grad_att = dot(after(branch1[s], down_part), w_out, NT).astype(BF16)
        grad_att = grad_att.reshape(2, 2 * tokens, heads, HEAD_DIM)
        grad_probs = einsum("bqhe,bkhe->bhqk", grad_att, values)
        delta = jnp.sum(probs * grad_probs, axis=-1, keepdims=True)
        grad_scores = (probs * (grad_probs - delta)).astype(BF16)
        grad_q = einsum("bhqk,bkhe->bqhe", grad_scores, keys) * SCORE_SCALE
        grad_k = einsum("bhqk,bqhe->bkhe", grad_scores, queries) * SCORE_SCALE
        grad_v = einsum("bhqk,bqhe->bkhe", probs.astype(BF16), grad_att)
        grads = jnp.stack(
            [
                rotate_back(grad_q, cosine, sine).astype(BF16),
                rotate_back(grad_k, cosine, sine).astype(BF16),
                grad_v.astype(BF16),
            ],
            axis=2,
        ).reshape(4 * tokens, 3 * part)
        grad_qkv.append(jnp.pad(grads, ((0, 0), (0, spare))))
    all_normed = jnp.concatenate(normed, axis=0)
    all_grads = jnp.concatenate(grad_qkv, axis=0)
    qkv_terms = dot(all_normed, all_grads, TN).astype(BF16)
    qkv_part = line_scatter(qkv_terms)
    all_attended = after(jnp.concatenate([k[4] for k in kept], axis=0), qkv_terms, gu_part)
    out_terms = dot(all_attended, jnp.concatenate(branch1, axis=0), TN).astype(BF16)
    out_part = line_scatter(out_terms)
    outputs = []
    for s in range(count):
        y_sum = plane_scatter(y_terms[s], out_terms)
        outputs.append((mids[s] + BRANCH_SCALE * y_sum).astype(BF16))

    all_in_terms = [dot(after(g, out_terms), w_qkv, NT).astype(BF16) for g in grad_qkv]
    factor_one = [norm_factor(v) for v in x_float]

    def input_grad_of(s, *late):
        grad_norm = plane_scatter(all_in_terms[s], *late)
        grad_norm = from_line(grad_norm, rows) * gain_one
        return (grad_mids[s] + norm_back(x_float[s], factor_one[s], grad_norm)).astype(BF16)

    input_grads = [input_grad_of(s) for s in range(count - 1)]
    gu_mine = half_scatter(gu_part, BF16, qkv_part, *input_grads)
    gu_raw = plane_exchange(gu_mine.reshape(4, rows, 2 * hidden))
    input_grads.append(input_grad_of(count - 1, gu_mine))
    qkv_mine = half_scatter(qkv_part, BF16, input_grads[-1])
    qkv_raw = plane_exchange(qkv_mine.reshape(4, rows, 3 * part + spare))
    out_part = after(out_part, input_grads[-1])
    own = out_part.shape[0] // halves
    if halves == 2:
        h = lax.axis_index("h")
        out_grad = sum(
            lax.ppermute(
                lax.dynamic_slice_in_dim(out_part, (h ^ flip) * own, own),
                HLXC,
                [(b, a) for a, b in head_order(flip)],
            ).astype(F32)
            for flip in (0, 1)
        )
    else:
        out_grad = lax.ppermute(
            half_scatter(out_part, F32), HLXC, [(b, a) for a, b in head_order(0)]
        )
    gu_raw = after(gu_raw, qkv_mine)
    gate_grad, up_grad = lax.optimization_barrier(
        (join_units(gu_raw[:, :, :hidden]), join_units(gu_raw[:, :, hidden:]))
    )

    gate_grad, up_grad = gate_grad.astype(F32), up_grad.astype(F32)
    ffn_gain_grad = jnp.sum(
        gate_grad * gate_weight.astype(F32) + up_grad * up_weight.astype(F32), axis=1
    ) / ffn_gain.astype(F32)
    qkv_grads = [
        qkv_raw[:, :, i * part : (i + 1) * part].transpose(1, 0, 2).reshape(rows, width).astype(F32)
        for i in range(3)
    ]
    attn_gain_grad = jnp.sum(
        qkv_grads[0] * query_weight.astype(F32)
        + qkv_grads[1] * key_weight.astype(F32)
        + qkv_grads[2] * value_weight.astype(F32),
        axis=1,
    ) / attn_gain.astype(F32)
    return (
        jnp.stack(outputs, axis=0),
        jnp.stack(input_grads, axis=0),
        *qkv_grads,
        out_grad,
        gate_grad,
        up_grad,
        half_scatter(down_part, F32, qkv_part)[:units],
        attn_gain_grad,
        ffn_gain_grad,
    )


def solution(mesh):
    seq, dp = mesh.devices.shape
    fine = Mesh(mesh.devices.reshape(seq, dp // 8, 2, 2, 2), ("y", "h", "l", "x", "c"))
    owners = ("y", "h", "l", "x", "c")
    acts = P(owners[1:], "y", None)
    weight = P(owners, None)
    gain = P(owners)
    return jax.shard_map(
        body,
        mesh=fine,
        in_specs=(acts, P(owners[1:])) + (weight,) * 7 + (gain, gain, acts),
        out_specs=(acts, acts) + (weight,) * 7 + (gain, gain),
        check_vma=False,
    )
```

```python
import math

import jax
import jax.numpy as jnp
from jax import lax
from jax.sharding import Mesh
from jax.sharding import PartitionSpec as P


HEADS = 36
HEAD_DIM = 64

NORM_EPS = 1e-05
BRANCH_SCALE = 1.4 / math.sqrt(40.0)
SCORE_SCALE = 0.125
MASK_FILL = -1e30

BF16 = jnp.bfloat16
F32 = jnp.float32


PLANE = ("y", "l")
LINE = ("x", "c")
FLIPS = (0, 2, 1, 3)


def dot(left, right, contract=((1,), (0,))):
    return lax.dot_general(left, right, (contract, ((), ())), preferred_element_type=F32)


NT = ((1,), (1,))
TN = ((0,), (0,))


def flip_send(block, flip):
    return lax.ppermute(block, PLANE, [(p, p ^ flip) for p in range(4)])


def plane_gather(block, *late):
    got = [flip_send(block, f) for f in FLIPS[1:]]
    if late:
        got = [after(g, *late) for g in got]
    return lax.optimization_barrier(jnp.concatenate([block] + got, axis=0))


def plane_scatter(partial, *late):
    rows = partial.shape[0] // 4
    total = partial[:rows].astype(F32)
    for k, f in enumerate(FLIPS[1:], 1):
        got = flip_send(partial[k * rows : (k + 1) * rows].astype(BF16), f)
        if late:
            got = after(got, *late)
        total = total + got.astype(F32)
    return total


def reorder(blocks):
    pairs = blocks.reshape((2, 2) + blocks.shape[1:])
    pairs = jnp.where(lax.axis_index("y") == 1, pairs[::-1], pairs)
    pairs = jnp.where(lax.axis_index("l") == 1, pairs[:, ::-1], pairs)
    return pairs.reshape(blocks.shape)


def plane_exchange(blocks):
    mine = reorder(blocks)
    got = [mine[0]] + [flip_send(mine[f], f) for f in (1, 2, 3)]
    return reorder(jnp.stack(got))


def after(value, *others):
    return lax.optimization_barrier((value,) + others)[0]


def line_gather(block):
    return lax.all_gather(block, LINE, axis=0, tiled=True)


def in_order(own, other):
    return jnp.where(
        lax.axis_index("h") == 0,
        jnp.concatenate([own, other], axis=0),
        jnp.concatenate([other, own], axis=0),
    )


def half_gather(block):
    if lax.axis_size("h") == 2:
        other = lax.ppermute(block, "h", [(0, 1), (1, 0)])
        return in_order(block, other)
    return lax.all_gather(block, "h", axis=0, tiled=True)


def line_scatter(partial):
    return lax.psum_scatter(partial, LINE, scatter_dimension=0, tiled=True)


def half_scatter(partial, kind, *late):
    if lax.axis_size("h") == 2:
        rows = partial.shape[0] // 2
        h = lax.axis_index("h")
        other = lax.dynamic_slice_in_dim(partial, (1 - h) * rows, rows)
        own = lax.dynamic_slice_in_dim(partial, h * rows, rows)
        other = lax.ppermute(other, "h", [(0, 1), (1, 0)])
        if late:
            own = after(own, *late)
        return (own.astype(F32) + other.astype(F32)).astype(kind)
    return lax.psum_scatter(partial, "h", scatter_dimension=0, tiled=True).astype(kind)


def column_block(blocks):
    four, rows, n = blocks.shape
    mine = plane_exchange(blocks)
    return half_gather(mine.reshape(four * rows, n))


def to_line(tokens, rows):
    count = tokens.shape[0]
    blocks = tokens.reshape(count, 2, -1, 2, 2, 2, rows)
    return blocks.transpose(0, 4, 5, 2, 1, 3, 6).reshape(tokens.shape)


def from_line(tokens, rows):
    count = tokens.shape[0]
    blocks = tokens.reshape(count, 2, 2, -1, 2, 2, rows)
    return blocks.transpose(0, 4, 3, 5, 1, 2, 6).reshape(tokens.shape)


def head_order(flip):
    h = lax.axis_size("h")
    pairs = []
    for hi in range(h):
        for li in range(2):
            for xc in range(4):
                source = li * 4 * h + xc * h + hi
                pairs.append((source, ((hi ^ flip) * 2 + li) * 4 + xc))
    return pairs


def angle_tables(positions):
    inverse = 10000.0 ** (-jnp.arange(32, dtype=F32) / 32.0)
    phase = positions[:, None] * inverse[None, :]
    phase = jnp.concatenate([phase, phase], axis=-1)
    return jnp.cos(phase), jnp.sin(phase)


def rotate(tensor, cosine, sine):
    half = HEAD_DIM // 2
    turned = jnp.concatenate([-tensor[..., half:], tensor[..., :half]], axis=-1)
    return tensor * cosine[:, None, :] + turned * sine[:, None, :]


def rotate_back(grad, cosine, sine):
    half = HEAD_DIM // 2
    scaled = grad * sine[:, None, :]
    turned = jnp.concatenate([scaled[..., half:], -scaled[..., :half]], axis=-1)
    return grad * cosine[:, None, :] + turned


def norm_factor(values):
    return lax.rsqrt(jnp.mean(values * values, axis=-1, keepdims=True) + NORM_EPS)


def norm_back(values, factor, grad):
    mean = jnp.mean(values * grad, axis=-1, keepdims=True)
    return factor * (grad - values * (factor * factor) * mean)


def einsum(spec, left, right):
    return jnp.einsum(spec, left, right, preferred_element_type=F32)


def body(
    inputs,
    lengths,
    query_weight,
    key_weight,
    value_weight,
    out_weight,
    gate_weight,
    up_weight,
    down_weight,
    attn_gain,
    ffn_gain,
    cotangent,
):
    count, tokens, width = inputs.shape
    rows = query_weight.shape[0]
    units = down_weight.shape[0]
    halves = lax.axis_size("h")
    heads = HEADS // 4
    part = heads * HEAD_DIM
    padded = -(-units // 8) * 8
    hidden = padded * 4 * halves
    y = lax.axis_index("y")

    spare = -3 * part % 128
    spare = spare if spare >= 2 else spare + 128
    extra = jnp.concatenate(
        [attn_gain[:, None], ffn_gain[:, None], jnp.zeros((rows, spare - 2), BF16)], axis=1
    )
    extra = jnp.broadcast_to(extra[None], (4, rows, spare))

    def split_heads(weight):
        return weight.reshape(rows, 4, part).transpose(1, 0, 2)

    def split_units(weight):
        blocks = weight.reshape(rows, 2, halves, 2, 2, 2, units)
        blocks = jnp.pad(blocks, ((0, 0),) * 6 + ((0, padded - units),))
        return blocks.transpose(1, 3, 0, 4, 5, 2, 6).reshape(4, rows, hidden)

    def join_units(blocks):
        blocks = blocks.reshape(2, 2, rows, 2, 2, halves, padded)[..., :units]
        return blocks.transpose(2, 0, 5, 1, 3, 4, 6).reshape(rows, 16 * halves * units)

    HLXC = ("h", "l", "x", "c")
    if halves == 2:
        pair = [lax.ppermute(out_weight, HLXC, head_order(flip)) for flip in (0, 1)]
        out_block = in_order(*pair)
    else:
        out_block = half_gather(lax.ppermute(out_weight, HLXC, head_order(0)))
    other_lengths = lax.ppermute(lengths, "l", [(0, 1), (1, 0)])
    qkv_block = column_block(
        jnp.concatenate(
            [split_heads(w) for w in (query_weight, key_weight, value_weight)] + [extra], axis=2
        ),
    )
    gu_block = column_block(
        jnp.concatenate([split_units(gate_weight), split_units(up_weight)], axis=2)
    )
    down_own = jnp.pad(down_weight, ((0, padded - units), (0, 0)))
    if halves == 2:
        down_other = lax.ppermute(down_own, "h", [(0, 1), (1, 0)])
    gathered = [plane_gather(to_line(inputs[s], rows)) for s in range(count)]
    w_out = line_gather(out_block)
    w_qkv = line_gather(qkv_block)
    w_gu = line_gather(gu_block)
    step = jnp.arange(tokens, dtype=jnp.int32)
    place = jnp.concatenate([y * tokens + step, (1 - y) * tokens + step])
    local_place = place[:tokens]
    cosine, sine = angle_tables(place.astype(F32))
    lengths_two = jnp.stack([lengths, other_lengths], axis=1)

    x_float = [inputs[s].astype(F32) for s in range(count)]
    grad_y = []
    branch2 = []
    for s in range(count):
        live = (local_place < lengths[s]).astype(F32)
        grad_y.append(cotangent[s].astype(F32) * live[:, None])

    pick = (
        lax.broadcasted_iota(jnp.int32, (8, spare), 0)
        == lax.broadcasted_iota(jnp.int32, (8, spare), 1)
    ).astype(BF16)
    gains = dot(pick, w_qkv[:, 3 * part :], NT)
    gain_one_line = gains[0:1]
    gain_one = from_line(gain_one_line, rows)
    gain_two = from_line(gains[1:2], rows)

    kept = []
    mids = []
    normed = []
    for s in range(count):
        whole = gathered[s].astype(F32)
        normed.append((whole * norm_factor(whole) * gain_one_line).astype(BF16))
        visible = (place[None, :] <= place[:, None])[None] & (
            place[None, None, :] < lengths_two[s][:, None, None]
        )
        visible = visible[:, None, :, :]
        lin = after(dot(normed[s], w_qkv), gu_block)
        lin = lin[:, : 3 * part].reshape(2, 2 * tokens, 3, heads, HEAD_DIM)
        queries = rotate(lin[:, :, 0], cosine, sine).astype(BF16)
        keys = rotate(lin[:, :, 1], cosine, sine).astype(BF16)
        values = lin[:, :, 2].astype(BF16)
        scores = einsum("bqhe,bkhe->bhqk", queries, keys) * SCORE_SCALE
        scores = jnp.where(visible, scores, MASK_FILL)
        expo = jnp.exp(scores - jnp.max(scores, axis=-1, keepdims=True))
        probs = expo / jnp.sum(expo, axis=-1, keepdims=True)
        attended = einsum("bhqk,bkhe->bqhe", probs.astype(BF16), values)
        attended = attended.astype(BF16).reshape(4 * tokens, part)
        if s == 0:
            if halves == 2:
                down_block = in_order(down_own, after(down_other, attended))
            else:
                down_block = half_gather(down_own)
            w_down = line_gather(down_block)
        out_sum = dot(attended, w_out)
        out_sum = plane_scatter(out_sum)
        mid = x_float[s] + BRANCH_SCALE * out_sum
        kept.append((queries, keys, values, probs, attended))
        mids.append(mid)

    factor_two = [norm_factor(v) for v in mids]
    own_ffn = [
        to_line((v * f * gain_two).astype(BF16), rows) for v, f in zip(mids, factor_two)
    ]
    normed_ffn = [plane_gather(v) for v in own_ffn]
    for s in range(count):
        branch2.append(plane_gather((BRANCH_SCALE * grad_y[s]).astype(BF16), *own_ffn))
    mixes = []
    acts = []
    for s in range(count):
        both = dot(normed_ffn[s], w_gu)
        gate_pre, up_pre = both[:, :hidden], both[:, hidden:]
        sigmoid = 1.0 / (1.0 + jnp.exp(-gate_pre))
        mixes.append((gate_pre * sigmoid * up_pre).astype(BF16))
        acts.append((gate_pre, up_pre, sigmoid))
    all_mixed = jnp.concatenate(mixes, axis=0)
    all_branch2 = jnp.concatenate(branch2, axis=0)
    down_terms = dot(all_mixed, all_branch2, TN).astype(BF16)
    down_part = line_scatter(down_terms)

    grad_boths = []
    for s in range(count):
        gate_pre, up_pre, sigmoid = acts[s]
        grad_mixed = dot(after(branch2[s], down_terms), w_down, NT)
        grad_gate = grad_mixed * up_pre * (sigmoid + gate_pre * sigmoid * (1.0 - sigmoid))
        grad_up = grad_mixed * gate_pre * sigmoid
        grad_boths.append(jnp.concatenate([grad_gate.astype(BF16), grad_up.astype(BF16)], axis=1))
    norm_terms = [dot(g, w_gu, NT).astype(BF16) for g in grad_boths]
    all_ffn = after(jnp.concatenate(normed_ffn, axis=0), *norm_terms)
    all_boths = jnp.concatenate(grad_boths, axis=0)
    gu_terms = dot(all_ffn, all_boths, TN).astype(BF16)
    gu_part = line_scatter(gu_terms)

    grad_mids = []
    branch1 = []
    own_branch1 = []
    for s in range(count):
        grad_norm = plane_scatter(norm_terms[s])
        grad_norm = from_line(grad_norm, rows) * gain_two
        grad_mid = grad_y[s] + norm_back(mids[s], factor_two[s], grad_norm)
        grad_mids.append(grad_mid)
        own_branch1.append((BRANCH_SCALE * grad_mid).astype(BF16))
        branch1.append(plane_gather(own_branch1[s]))

    grad_qkv = []
    input_grads = []
    for s in range(count):
        queries, keys, values, probs, attended = kept[s]
        grad_att = dot(after(branch1[s], down_part), w_out, NT).astype(BF16)
        grad_att = grad_att.reshape(2, 2 * tokens, heads, HEAD_DIM)
        grad_probs = einsum("bqhe,bkhe->bhqk", grad_att, values)
        delta = jnp.sum(probs * grad_probs, axis=-1, keepdims=True)
        grad_scores = (probs * (grad_probs - delta)).astype(BF16)
        grad_q = einsum("bhqk,bkhe->bqhe", grad_scores, keys) * SCORE_SCALE
        grad_k = einsum("bhqk,bqhe->bkhe", grad_scores, queries) * SCORE_SCALE
        grad_v = einsum("bhqk,bqhe->bkhe", probs.astype(BF16), grad_att)
        grads = jnp.stack(
            [
                rotate_back(grad_q, cosine, sine).astype(BF16),
                rotate_back(grad_k, cosine, sine).astype(BF16),
                grad_v.astype(BF16),
            ],
            axis=2,
        ).reshape(4 * tokens, 3 * part)
        grad_qkv.append(jnp.pad(grads, ((0, 0), (0, spare))))
    all_normed = jnp.concatenate(normed, axis=0)
    all_grads = jnp.concatenate(grad_qkv, axis=0)
    qkv_terms = dot(all_normed, all_grads, TN).astype(BF16)
    qkv_part = line_scatter(qkv_terms)
    all_in_terms = [dot(after(g, qkv_terms), w_qkv, NT).astype(BF16) for g in grad_qkv]
    all_attended = after(jnp.concatenate([k[4] for k in kept], axis=0), qkv_terms, gu_part)
    out_terms = dot(all_attended, jnp.concatenate(branch1, axis=0), TN).astype(BF16)
    out_part = line_scatter(out_terms)
    factor_one = [norm_factor(v) for v in x_float]

    input_grads = []
    for s in range(count):
        grad_norm = plane_scatter(all_in_terms[s], gu_part)
        grad_norm = from_line(grad_norm, rows) * gain_one
        input_grads.append(
            (grad_mids[s] + norm_back(x_float[s], factor_one[s], grad_norm)).astype(BF16)
        )
    y_terms = [dot(after(m, out_terms), w_down).astype(BF16) for m in mixes]
    gu_mine = half_scatter(gu_part, BF16, qkv_part, *input_grads)
    gu_raw = plane_exchange(gu_mine.reshape(4, rows, 2 * hidden))
    outputs = []
    for s in range(count):
        y_sum = plane_scatter(y_terms[s], gu_raw)
        outputs.append((mids[s] + BRANCH_SCALE * y_sum).astype(BF16))
    qkv_mine = half_scatter(qkv_part, BF16, gu_mine)
    qkv_raw = plane_exchange(qkv_mine.reshape(4, rows, 3 * part + spare))
    out_part = after(out_part, gu_mine)
    own = out_part.shape[0] // halves
    if halves == 2:
        h = lax.axis_index("h")
        out_grad = sum(
            lax.ppermute(
                lax.dynamic_slice_in_dim(out_part, (h ^ flip) * own, own),
                HLXC,
                [(b, a) for a, b in head_order(flip)],
            ).astype(F32)
            for flip in (0, 1)
        )
    else:
        out_grad = lax.ppermute(
            half_scatter(out_part, F32), HLXC, [(b, a) for a, b in head_order(0)]
        )
    gu_raw = after(gu_raw, qkv_mine)
    gate_grad, up_grad = lax.optimization_barrier(
        (join_units(gu_raw[:, :, :hidden]), join_units(gu_raw[:, :, hidden:]))
    )

    gate_grad, up_grad = gate_grad.astype(F32), up_grad.astype(F32)
    ffn_gain_grad = jnp.sum(
        gate_grad * gate_weight.astype(F32) + up_grad * up_weight.astype(F32), axis=1
    ) / ffn_gain.astype(F32)
    qkv_grads = [
        qkv_raw[:, :, i * part : (i + 1) * part].transpose(1, 0, 2).reshape(rows, width).astype(F32)
        for i in range(3)
    ]
    attn_gain_grad = jnp.sum(
        qkv_grads[0] * query_weight.astype(F32)
        + qkv_grads[1] * key_weight.astype(F32)
        + qkv_grads[2] * value_weight.astype(F32),
        axis=1,
    ) / attn_gain.astype(F32)
    return (
        jnp.stack(outputs, axis=0),
        jnp.stack(input_grads, axis=0),
        *qkv_grads,
        out_grad,
        gate_grad,
        up_grad,
        half_scatter(down_part, F32, qkv_part)[:units],
        attn_gain_grad,
        ffn_gain_grad,
    )


def solution(mesh):
    seq, dp = mesh.devices.shape
    fine = Mesh(mesh.devices.reshape(seq, dp // 8, 2, 2, 2), ("y", "h", "l", "x", "c"))
    owners = ("y", "h", "l", "x", "c")
    acts = P(owners[1:], "y", None)
    weight = P(owners, None)
    gain = P(owners)
    return jax.shard_map(
        body,
        mesh=fine,
        in_specs=(acts, P(owners[1:])) + (weight,) * 7 + (gain, gain, acts),
        out_specs=(acts, acts) + (weight,) * 7 + (gain, gain),
        check_vma=False,
    )
```

```python
import math

import jax
import jax.numpy as jnp
from jax import lax
from jax.sharding import Mesh
from jax.sharding import PartitionSpec as P


HEADS = 36
HEAD_DIM = 64

NORM_EPS = 1e-05
BRANCH_SCALE = 1.4 / math.sqrt(40.0)
SCORE_SCALE = 0.125
MASK_FILL = -1e30

BF16 = jnp.bfloat16
F32 = jnp.float32


PLANE = ("y", "l")
LINE = ("x", "c")
FLIPS = (0, 2, 1, 3)


def dot(left, right, contract=((1,), (0,))):
    return lax.dot_general(left, right, (contract, ((), ())), preferred_element_type=F32)


NT = ((1,), (1,))
TN = ((0,), (0,))


def flip_send(block, flip):
    return lax.ppermute(block, PLANE, [(p, p ^ flip) for p in range(4)])


def plane_gather(block, *late):
    got = [flip_send(block, f) for f in FLIPS[1:]]
    if late:
        got = [after(g, *late) for g in got]
    return lax.optimization_barrier(jnp.concatenate([block] + got, axis=0))


def plane_scatter(partial, *late):
    rows = partial.shape[0] // 4
    total = partial[:rows].astype(F32)
    for k, f in enumerate(FLIPS[1:], 1):
        got = flip_send(partial[k * rows : (k + 1) * rows].astype(BF16), f)
        if late:
            got = after(got, *late)
        total = total + got.astype(F32)
    return total


def reorder(blocks):
    pairs = blocks.reshape((2, 2) + blocks.shape[1:])
    pairs = jnp.where(lax.axis_index("y") == 1, pairs[::-1], pairs)
    pairs = jnp.where(lax.axis_index("l") == 1, pairs[:, ::-1], pairs)
    return pairs.reshape(blocks.shape)


def plane_exchange(blocks):
    mine = reorder(blocks)
    got = [mine[0]] + [flip_send(mine[f], f) for f in (1, 2, 3)]
    return reorder(jnp.stack(got))


def after(value, *others):
    return lax.optimization_barrier((value,) + others)[0]


def line_gather(block):
    return lax.all_gather(block, LINE, axis=0, tiled=True)


def in_order(own, other):
    return jnp.where(
        lax.axis_index("h") == 0,
        jnp.concatenate([own, other], axis=0),
        jnp.concatenate([other, own], axis=0),
    )


def half_gather(block):
    if lax.axis_size("h") == 2:
        other = lax.ppermute(block, "h", [(0, 1), (1, 0)])
        return in_order(block, other)
    return lax.all_gather(block, "h", axis=0, tiled=True)


def line_scatter(partial):
    return lax.psum_scatter(partial, LINE, scatter_dimension=0, tiled=True)


def half_scatter(partial, kind, *late):
    if lax.axis_size("h") == 2:
        rows = partial.shape[0] // 2
        h = lax.axis_index("h")
        other = lax.dynamic_slice_in_dim(partial, (1 - h) * rows, rows)
        own = lax.dynamic_slice_in_dim(partial, h * rows, rows)
        other = lax.ppermute(other, "h", [(0, 1), (1, 0)])
        if late:
            own = after(own, *late)
        return (own.astype(F32) + other.astype(F32)).astype(kind)
    return lax.psum_scatter(partial, "h", scatter_dimension=0, tiled=True).astype(kind)


def column_block(blocks):
    four, rows, n = blocks.shape
    mine = plane_exchange(blocks)
    return half_gather(mine.reshape(four * rows, n))


def to_line(tokens, rows):
    count = tokens.shape[0]
    blocks = tokens.reshape(count, 2, -1, 2, 2, 2, rows)
    return blocks.transpose(0, 4, 5, 2, 1, 3, 6).reshape(tokens.shape)


def from_line(tokens, rows):
    count = tokens.shape[0]
    blocks = tokens.reshape(count, 2, 2, -1, 2, 2, rows)
    return blocks.transpose(0, 4, 3, 5, 1, 2, 6).reshape(tokens.shape)


def head_order(flip):
    h = lax.axis_size("h")
    pairs = []
    for hi in range(h):
        for li in range(2):
            for xc in range(4):
                source = li * 4 * h + xc * h + hi
                pairs.append((source, ((hi ^ flip) * 2 + li) * 4 + xc))
    return pairs


def angle_tables(positions):
    inverse = 10000.0 ** (-jnp.arange(32, dtype=F32) / 32.0)
    phase = positions[:, None] * inverse[None, :]
    phase = jnp.concatenate([phase, phase], axis=-1)
    return jnp.cos(phase), jnp.sin(phase)


def rotate(tensor, cosine, sine):
    half = HEAD_DIM // 2
    turned = jnp.concatenate([-tensor[..., half:], tensor[..., :half]], axis=-1)
    return tensor * cosine[:, None, :] + turned * sine[:, None, :]


def rotate_back(grad, cosine, sine):
    half = HEAD_DIM // 2
    scaled = grad * sine[:, None, :]
    turned = jnp.concatenate([scaled[..., half:], -scaled[..., :half]], axis=-1)
    return grad * cosine[:, None, :] + turned


def norm_factor(values):
    return lax.rsqrt(jnp.mean(values * values, axis=-1, keepdims=True) + NORM_EPS)


def norm_back(values, factor, grad):
    mean = jnp.mean(values * grad, axis=-1, keepdims=True)
    return factor * (grad - values * (factor * factor) * mean)


def einsum(spec, left, right):
    return jnp.einsum(spec, left, right, preferred_element_type=F32)


def body(
    inputs,
    lengths,
    query_weight,
    key_weight,
    value_weight,
    out_weight,
    gate_weight,
    up_weight,
    down_weight,
    attn_gain,
    ffn_gain,
    cotangent,
):
    count, tokens, width = inputs.shape
    rows = query_weight.shape[0]
    units = down_weight.shape[0]
    halves = lax.axis_size("h")
    heads = HEADS // 4
    part = heads * HEAD_DIM
    padded = -(-units // 8) * 8
    hidden = padded * 4 * halves
    y = lax.axis_index("y")

    spare = -3 * part % 128
    spare = spare if spare >= 2 else spare + 128
    extra = jnp.concatenate(
        [attn_gain[:, None], ffn_gain[:, None], jnp.zeros((rows, spare - 2), BF16)], axis=1
    )
    extra = jnp.broadcast_to(extra[None], (4, rows, spare))

    def split_heads(weight):
        return weight.reshape(rows, 4, part).transpose(1, 0, 2)

    def split_units(weight):
        blocks = weight.reshape(rows, 2, halves, 2, 2, 2, units)
        blocks = jnp.pad(blocks, ((0, 0),) * 6 + ((0, padded - units),))
        return blocks.transpose(1, 3, 0, 4, 5, 2, 6).reshape(4, rows, hidden)

    def join_units(blocks):
        blocks = blocks.reshape(2, 2, rows, 2, 2, halves, padded)[..., :units]
        return blocks.transpose(2, 0, 5, 1, 3, 4, 6).reshape(rows, 16 * halves * units)

    HLXC = ("h", "l", "x", "c")
    if halves == 2:
        pair = [lax.ppermute(out_weight, HLXC, head_order(flip)) for flip in (0, 1)]
        out_block = in_order(*pair)
    else:
        out_block = half_gather(lax.ppermute(out_weight, HLXC, head_order(0)))
    other_lengths = lax.ppermute(lengths, "l", [(0, 1), (1, 0)])
    qkv_block = column_block(
        jnp.concatenate(
            [split_heads(w) for w in (query_weight, key_weight, value_weight)] + [extra], axis=2
        ),
    )
    gu_block = column_block(
        jnp.concatenate([split_units(gate_weight), split_units(up_weight)], axis=2)
    )
    down_own = jnp.pad(down_weight, ((0, padded - units), (0, 0)))
    if halves == 2:
        down_other = lax.ppermute(down_own, "h", [(0, 1), (1, 0)])
    gathered = [plane_gather(to_line(inputs[s], rows)) for s in range(count)]
    w_out = line_gather(out_block)
    w_qkv = line_gather(qkv_block)
    w_gu = line_gather(gu_block)
    step = jnp.arange(tokens, dtype=jnp.int32)
    place = jnp.concatenate([y * tokens + step, (1 - y) * tokens + step])
    local_place = place[:tokens]
    cosine, sine = angle_tables(place.astype(F32))
    lengths_two = jnp.stack([lengths, other_lengths], axis=1)

    x_float = [inputs[s].astype(F32) for s in range(count)]
    grad_y = []
    branch2 = []
    for s in range(count):
        live = (local_place < lengths[s]).astype(F32)
        grad_y.append(cotangent[s].astype(F32) * live[:, None])

    pick = (
        lax.broadcasted_iota(jnp.int32, (8, spare), 0)
        == lax.broadcasted_iota(jnp.int32, (8, spare), 1)
    ).astype(BF16)
    gains = dot(pick, w_qkv[:, 3 * part :], NT)
    gain_one_line = gains[0:1]
    gain_one = from_line(gain_one_line, rows)
    gain_two = from_line(gains[1:2], rows)

    kept = []
    mids = []
    normed = []
    for s in range(count):
        whole = gathered[s].astype(F32)
        normed.append((whole * norm_factor(whole) * gain_one_line).astype(BF16))
        visible = (place[None, :] <= place[:, None])[None] & (
            place[None, None, :] < lengths_two[s][:, None, None]
        )
        visible = visible[:, None, :, :]
        lin = after(dot(normed[s], w_qkv), gu_block)
        lin = lin[:, : 3 * part].reshape(2, 2 * tokens, 3, heads, HEAD_DIM)
        queries = rotate(lin[:, :, 0], cosine, sine).astype(BF16)
        keys = rotate(lin[:, :, 1], cosine, sine).astype(BF16)
        values = lin[:, :, 2].astype(BF16)
        scores = einsum("bqhe,bkhe->bhqk", queries, keys) * SCORE_SCALE
        scores = jnp.where(visible, scores, MASK_FILL)
        expo = jnp.exp(scores - jnp.max(scores, axis=-1, keepdims=True))
        probs = expo / jnp.sum(expo, axis=-1, keepdims=True)
        attended = einsum("bhqk,bkhe->bqhe", probs.astype(BF16), values)
        attended = attended.astype(BF16).reshape(4 * tokens, part)
        if s == 0:
            if halves == 2:
                down_block = in_order(down_own, after(down_other, attended))
            else:
                down_block = half_gather(down_own)
            w_down = line_gather(down_block)
        out_sum = dot(attended, w_out)
        out_sum = plane_scatter(out_sum)
        mid = x_float[s] + BRANCH_SCALE * out_sum
        kept.append((queries, keys, values, probs, attended))
        mids.append(mid)

    factor_two = [norm_factor(v) for v in mids]
    own_ffn = [
        to_line((v * f * gain_two).astype(BF16), rows) for v, f in zip(mids, factor_two)
    ]
    normed_ffn = [plane_gather(v) for v in own_ffn]
    for s in range(count):
        branch2.append(plane_gather((BRANCH_SCALE * grad_y[s]).astype(BF16), *own_ffn))
    mixes = []
    acts = []
    for s in range(count):
        both = dot(normed_ffn[s], w_gu)
        gate_pre, up_pre = both[:, :hidden], both[:, hidden:]
        sigmoid = 1.0 / (1.0 + jnp.exp(-gate_pre))
        mixes.append((gate_pre * sigmoid * up_pre).astype(BF16))
        acts.append((gate_pre, up_pre, sigmoid))
    all_mixed = jnp.concatenate(mixes, axis=0)
    all_branch2 = jnp.concatenate(branch2, axis=0)
    down_terms = dot(all_mixed, all_branch2, TN).astype(BF16)
    down_part = line_scatter(down_terms)

    grad_boths = []
    for s in range(count):
        gate_pre, up_pre, sigmoid = acts[s]
        grad_mixed = dot(after(branch2[s], down_terms), w_down, NT)
        grad_gate = grad_mixed * up_pre * (sigmoid + gate_pre * sigmoid * (1.0 - sigmoid))
        grad_up = grad_mixed * gate_pre * sigmoid
        grad_boths.append(jnp.concatenate([grad_gate.astype(BF16), grad_up.astype(BF16)], axis=1))
    norm_terms = [dot(g, w_gu, NT).astype(BF16) for g in grad_boths]
    all_ffn = after(jnp.concatenate(normed_ffn, axis=0), *norm_terms)
    all_boths = jnp.concatenate(grad_boths, axis=0)
    gu_terms = dot(all_ffn, all_boths, TN).astype(BF16)
    gu_part = line_scatter(gu_terms)

    grad_mids = []
    branch1 = []
    own_branch1 = []
    for s in range(count):
        grad_norm = plane_scatter(norm_terms[s])
        grad_norm = from_line(grad_norm, rows) * gain_two
        grad_mid = grad_y[s] + norm_back(mids[s], factor_two[s], grad_norm)
        grad_mids.append(grad_mid)
        own_branch1.append((BRANCH_SCALE * grad_mid).astype(BF16))
        branch1.append(plane_gather(own_branch1[s]))

    y_terms = [dot(after(m, gu_terms, *own_branch1), w_down).astype(BF16) for m in mixes]

    grad_qkv = []
    for s in range(count):
        queries, keys, values, probs, attended = kept[s]
        grad_att = dot(after(branch1[s], down_part), w_out, NT).astype(BF16)
        grad_att = grad_att.reshape(2, 2 * tokens, heads, HEAD_DIM)
        grad_probs = einsum("bqhe,bkhe->bhqk", grad_att, values)
        delta = jnp.sum(probs * grad_probs, axis=-1, keepdims=True)
        grad_scores = (probs * (grad_probs - delta)).astype(BF16)
        grad_q = einsum("bhqk,bkhe->bqhe", grad_scores, keys) * SCORE_SCALE
        grad_k = einsum("bhqk,bqhe->bkhe", grad_scores, queries) * SCORE_SCALE
        grad_v = einsum("bhqk,bqhe->bkhe", probs.astype(BF16), grad_att)
        grads = jnp.stack(
            [
                rotate_back(grad_q, cosine, sine).astype(BF16),
                rotate_back(grad_k, cosine, sine).astype(BF16),
                grad_v.astype(BF16),
            ],
            axis=2,
        ).reshape(4 * tokens, 3 * part)
        grad_qkv.append(jnp.pad(grads, ((0, 0), (0, spare))))
    all_normed = jnp.concatenate(normed, axis=0)
    all_grads = jnp.concatenate(grad_qkv, axis=0)
    qkv_terms = dot(all_normed, all_grads, TN).astype(BF16)
    qkv_part = line_scatter(qkv_terms)
    all_in_terms = [dot(after(g, qkv_terms), w_qkv, NT).astype(BF16) for g in grad_qkv]
    all_attended = after(jnp.concatenate([k[4] for k in kept], axis=0), qkv_terms, gu_part)
    out_terms = dot(all_attended, jnp.concatenate(branch1, axis=0), TN).astype(BF16)
    out_part = line_scatter(out_terms)
    factor_one = [norm_factor(v) for v in x_float]

    outputs = []
    for s in range(count):
        y_sum = plane_scatter(y_terms[s], out_terms)
        outputs.append((mids[s] + BRANCH_SCALE * y_sum).astype(BF16))
    input_grads = []
    for s in range(count):
        grad_norm = plane_scatter(all_in_terms[s], gu_part)
        grad_norm = from_line(grad_norm, rows) * gain_one
        input_grads.append(
            (grad_mids[s] + norm_back(x_float[s], factor_one[s], grad_norm)).astype(BF16)
        )
    gu_mine = half_scatter(gu_part, BF16, qkv_part, *input_grads)
    gu_raw = plane_exchange(gu_mine.reshape(4, rows, 2 * hidden))
    qkv_mine = half_scatter(qkv_part, BF16, gu_mine)
    qkv_raw = plane_exchange(qkv_mine.reshape(4, rows, 3 * part + spare))
    out_part = after(out_part, gu_mine)
    own = out_part.shape[0] // halves
    if halves == 2:
        h = lax.axis_index("h")
        out_grad = sum(
            lax.ppermute(
                lax.dynamic_slice_in_dim(out_part, (h ^ flip) * own, own),
                HLXC,
                [(b, a) for a, b in head_order(flip)],
            ).astype(F32)
            for flip in (0, 1)
        )
    else:
        out_grad = lax.ppermute(
            half_scatter(out_part, F32), HLXC, [(b, a) for a, b in head_order(0)]
        )
    gu_raw = after(gu_raw, qkv_mine)
    gate_grad, up_grad = lax.optimization_barrier(
        (join_units(gu_raw[:, :, :hidden]), join_units(gu_raw[:, :, hidden:]))
    )

    gate_grad, up_grad = gate_grad.astype(F32), up_grad.astype(F32)
    ffn_gain_grad = jnp.sum(
        gate_grad * gate_weight.astype(F32) + up_grad * up_weight.astype(F32), axis=1
    ) / ffn_gain.astype(F32)
    qkv_grads = [
        qkv_raw[:, :, i * part : (i + 1) * part].transpose(1, 0, 2).reshape(rows, width).astype(F32)
        for i in range(3)
    ]
    attn_gain_grad = jnp.sum(
        qkv_grads[0] * query_weight.astype(F32)
        + qkv_grads[1] * key_weight.astype(F32)
        + qkv_grads[2] * value_weight.astype(F32),
        axis=1,
    ) / attn_gain.astype(F32)
    return (
        jnp.stack(outputs, axis=0),
        jnp.stack(input_grads, axis=0),
        *qkv_grads,
        out_grad,
        gate_grad,
        up_grad,
        half_scatter(down_part, F32, qkv_part)[:units],
        attn_gain_grad,
        ffn_gain_grad,
    )


def solution(mesh):
    seq, dp = mesh.devices.shape
    fine = Mesh(mesh.devices.reshape(seq, dp // 8, 2, 2, 2), ("y", "h", "l", "x", "c"))
    owners = ("y", "h", "l", "x", "c")
    acts = P(owners[1:], "y", None)
    weight = P(owners, None)
    gain = P(owners)
    return jax.shard_map(
        body,
        mesh=fine,
        in_specs=(acts, P(owners[1:])) + (weight,) * 7 + (gain, gain, acts),
        out_specs=(acts, acts) + (weight,) * 7 + (gain, gain),
        check_vma=False,
    )
```
